16 devices in a mesh: dp: 2 (over z), sp: 8 (over y, x, core).
Axes of the slice: x: 2, y: 2, z: 2, core: 2. Of those that a mesh axis runs over, the one named last changes fastest.
Arguments:
- images: float32 [12, 256, 256, 3], P('dp', 'sp'), parts along dimension 0
- w_patch: bfloat16 [16, 16, 3, 1024], replicated
- b_patch: float32 [1024], replicated
- pos_embed: bfloat16 [256, 1024], P('sp')
- ln1_gain: float32 [1024], replicated
- ln1_bias: float32 [1024], replicated
- w_qkv: bfloat16 [1024, 3, 16, 64], replicated
- b_qkv: float32 [3, 16, 64], replicated
- w_out: bfloat16 [16, 64, 1024], replicated
- b_out: float32 [1024], replicated
- ln2_gain: float32 [1024], replicated
- ln2_bias: float32 [1024], replicated
- w_fc1: bfloat16 [1024, 4096], replicated
- b_fc1: float32 [4096], replicated
- w_fc2: bfloat16 [4096, 1024], replicated
- b_fc2: float32 [1024], replicated
Outputs:
- output: bfloat16 [12, 256, 1024], P('dp', 'sp'), parts along dimension 0
There are 2 independent parts. The reference program is written for one: setup_inputs(seed, part) draws one part's arguments, and reference() takes and returns one part's arrays. A program takes and returns all parts, laid end to end along the dimension named above; an argument that names none is the same for every part.
All inputs are finite; a program needn't handle non-finite values.
Results may differ from the reference program's by a relative error of at most 0.0125094.
Values are sent between devices in bfloat16 or wider.
A program may use at most 1 GiB of HBM per device.

```python
import jax
import jax.numpy as jnp
from jax import lax

B = 6
IMG = 256
PATCH = 16
D = 1024
HEADS = 16
HEAD = 64
FF = 4096

GRID = IMG // PATCH
TOKENS = GRID * GRID
PATCH_DIM = PATCH * PATCH * 3
LN_EPS = 1e-6


def draw_normal(rng_key, arr_shape, std_dev):
    return jax.random.normal(rng_key, arr_shape, jnp.float32) * std_dev


def smooth_images(base_key, num_images):
    key_freq, key_phase, key_amp, key_noise = jax.random.split(base_key, 4)
    wave_freq = jax.random.uniform(key_freq, (num_images, 8, 2), jnp.float32, -4.0, 4.0) * (2.0 * jnp.pi / IMG)
    wave_phase = jax.random.uniform(key_phase, (num_images, 8, 3), jnp.float32, 0.0, 2.0 * jnp.pi)
    wave_amp = draw_normal(key_amp, (num_images, 8, 3), 0.5)
    coords = jnp.arange(IMG, dtype=jnp.float32)
    row_angle = wave_freq[:, :, 0, None] * coords
    col_angle = wave_freq[:, :, 1, None, None] * coords[:, None] + wave_phase[:, :, None, :]
    waves = (jnp.einsum('nky,nkxc->nyxc', jnp.cos(row_angle), wave_amp[:, :, None, :] * jnp.cos(col_angle))
             - jnp.einsum('nky,nkxc->nyxc', jnp.sin(row_angle), wave_amp[:, :, None, :] * jnp.sin(col_angle)))
    return waves + draw_normal(key_noise, (num_images, IMG, IMG, 3), 0.2)


def setup_inputs(seed: int = 0, part: int = 0) -> dict:
    sub_keys = jax.random.split(jax.random.key(seed), 16)
    qk_gain = jnp.array([1.5, 1.5, 1.0], jnp.float32)[None, :, None, None]
    return {
        'images': smooth_images(jax.random.fold_in(sub_keys[0], part), B),
        'w_patch': draw_normal(sub_keys[1], (PATCH, PATCH, 3, D), PATCH_DIM ** -0.5).astype(jnp.bfloat16),
        'b_patch': draw_normal(sub_keys[2], (D,), 0.5),
        'pos_embed': draw_normal(sub_keys[3], (TOKENS, D), 1.0).astype(jnp.bfloat16),
        'ln1_gain': 1.0 + draw_normal(sub_keys[4], (D,), 0.2),
        'ln1_bias': draw_normal(sub_keys[5], (D,), 0.5),
        'w_qkv': (draw_normal(sub_keys[6], (D, 3, HEADS, HEAD), D ** -0.5) * qk_gain).astype(jnp.bfloat16),
        'b_qkv': draw_normal(sub_keys[7], (3, HEADS, HEAD), 0.5),
        'w_out': draw_normal(sub_keys[8], (HEADS, HEAD, D), 2.0 * D ** -0.5).astype(jnp.bfloat16),
        'b_out': draw_normal(sub_keys[9], (D,), 0.5),
        'ln2_gain': 1.0 + draw_normal(sub_keys[10], (D,), 0.2),
        'ln2_bias': draw_normal(sub_keys[11], (D,), 0.5),
        'w_fc1': draw_normal(sub_keys[12], (D, FF), D ** -0.5).astype(jnp.bfloat16),
        'b_fc1': draw_normal(sub_keys[13], (FF,), 0.5),
        'w_fc2': draw_normal(sub_keys[14], (FF, D), 1.5 * FF ** -0.5).astype(jnp.bfloat16),
        'b_fc2': draw_normal(sub_keys[15], (D,), 0.5),
    }


def layer_norm(x_in, ln_gain, ln_bias):
    row_mean = jnp.mean(x_in, axis=-1, keepdims=True)
    centered = x_in - row_mean
    variance = jnp.mean(centered * centered, axis=-1, keepdims=True)
    return centered * lax.rsqrt(variance + LN_EPS) * ln_gain + ln_bias


def reference(images, w_patch, b_patch, pos_embed, ln1_gain, ln1_bias, w_qkv, b_qkv, w_out, b_out, ln2_gain, ln2_bias, w_fc1, b_fc1, w_fc2, b_fc2):
    w_patch_flat = w_patch.reshape(PATCH_DIM, D)
    w_qkv_flat = w_qkv.reshape(D, 3 * D)
    b_qkv_flat = b_qkv.reshape(3 * D)
    w_out_flat = w_out.reshape(D, D)
    pos_f32 = pos_embed.astype(jnp.float32)

    def encode_image(single_image):
        pixels = single_image.astype(jnp.bfloat16).reshape(GRID, PATCH, GRID, PATCH, 3)
        patches = jnp.transpose(pixels, (0, 2, 1, 3, 4)).reshape(TOKENS, PATCH_DIM)
        patch_embed = jnp.dot(patches, w_patch_flat, preferred_element_type=jnp.float32)
        x_zero = (patch_embed + b_patch + pos_f32).astype(jnp.bfloat16)
        normed = layer_norm(x_zero.astype(jnp.float32), ln1_gain, ln1_bias).astype(jnp.bfloat16)
        qkv_proj = (jnp.dot(normed, w_qkv_flat, preferred_element_type=jnp.float32) + b_qkv_flat).astype(jnp.bfloat16)
        queries = qkv_proj[:, :D].reshape(GRID, GRID, HEADS, HEAD)
        keys_all = qkv_proj[:, D:2 * D].reshape(TOKENS, HEADS, HEAD).astype(jnp.float32)
        values_all = qkv_proj[:, 2 * D:].reshape(TOKENS, HEADS, HEAD).astype(jnp.float32)

        def attend_row(row_queries):
            scores = jnp.einsum('qhe,khe->hqk', row_queries.astype(jnp.float32), keys_all) * HEAD ** -0.5
            weights = jax.nn.softmax(scores, axis=-1).astype(jnp.bfloat16).astype(jnp.float32)
            return jnp.einsum('hqk,khe->qhe', weights, values_all).astype(jnp.bfloat16)

        attended = lax.map(attend_row, queries).reshape(TOKENS, D)
        residual = x_zero.astype(jnp.float32) + jnp.dot(attended, w_out_flat, preferred_element_type=jnp.float32) + b_out
        normed_two = layer_norm(residual, ln2_gain, ln2_bias).astype(jnp.bfloat16)
        hidden = jax.nn.gelu(jnp.dot(normed_two, w_fc1, preferred_element_type=jnp.float32) + b_fc1, approximate=True).astype(jnp.bfloat16)
        return (residual + jnp.dot(hidden, w_fc2, preferred_element_type=jnp.float32) + b_fc2).astype(jnp.bfloat16)

    return lax.map(encode_image, images)
```

```python
import functools
import math
import jax
import jax.numpy as jnp
from jax import lax
from jax.experimental import pallas as pl
from jax.experimental.pallas import tpu as pltpu
from jax.sharding import PartitionSpec as P

LN_EPS = 1e-6
F32 = jnp.float32
BF16 = jnp.bfloat16
D = 1024
FF = 4096
IMAGES = 6
BLOCK = 32
TOKENS = 256
OWN = 192
N_FC1, W_FC1 = 8, 512
N_FC2, W_FC2 = 4, 256
EXP_SCALE = math.log2(math.e) / 8.0
MESH = pl.DeviceIdType.MESH
NT = (((1,), (1,)), ((), ()))


def as_row(vec):
    return jnp.concatenate([vec[i:i + 1, :] for i in range(vec.shape[0])], axis=1)


def norm_rows(x_in, gain, bias):
    centered = x_in - jnp.mean(x_in, axis=-1, keepdims=True)
    variance = jnp.mean(centered * centered, axis=-1, keepdims=True)
    return centered * lax.rsqrt(variance + LN_EPS) * gain + bias


def layer_kernel(
        img_hbm, wp_hbm, bp_hbm, pos_hbm, g1_hbm, c1_hbm, wqkv_hbm, bqkv_hbm, wo_hbm, bo_hbm, g2_hbm, c2_hbm,
        w1_hbm, b1_hbm, w2_hbm, b2_hbm,
        out_hbm,
        img, wp, pos, vecs, b1, bqkv, wqkv, wo, w1, w2,
        lhs, sel, pix, xs, xg, y1, qh, kh, vh, og, op, res, y2, hid, outs, b1row,
        in_sem, wqkv_sem, wo_sem, w1_sem, w2_sem,
        xsend, xrecv, fsend, frecv, osend, orecv, rsend, rrecv):
    dp = lax.axis_index("dp")
    me = lax.axis_index("sp")
    chip = me // 2
    core = me % 2
    mate = chip * 2 + (1 - core)
    cx = chip % 2
    cy = chip // 2

    def remote(src, dst, ssem, rsem, dev):
        return pltpu.make_async_remote_copy(
            src_ref=src, dst_ref=dst, send_sem=ssem, recv_sem=rsem, device_id=(dp, dev), device_id_type=MESH)

    def chip_at(k):
        return ((cy + k // 2) % 2) * 2 + (cx + k % 2) % 2

    barrier = pltpu.get_barrier_semaphore()
    for k in range(1, 8):
        pl.semaphore_signal(barrier, inc=1, device_id=(dp, (me + k) % 8), device_id_type=MESH)

    small = [(img_hbm, img), (wp_hbm, wp), (pos_hbm, pos)]
    for i, v in enumerate((bp_hbm, g1_hbm, c1_hbm, bo_hbm, g2_hbm, c2_hbm, b2_hbm)):
        small.append((v, vecs.at[i]))
    small.append((b1_hbm, b1))
    small_copies = [pltpu.make_async_copy(s, d, in_sem.at[i]) for i, (s, d) in enumerate(small)]
    for c in small_copies:
        c.start()
    bq_copy = pltpu.make_async_copy(bqkv_hbm.at[:, pl.ds(pl.multiple_of(core * 8, 8), 8), :], bqkv, in_sem.at[len(small)])
    bq_copy.start()
    wq_copies = [
        pltpu.make_async_copy(wqkv_hbm.at[pl.ds(pl.multiple_of(t * D + core * 512, 512), 512), :], wqkv.at[t], wqkv_sem.at[t])
        for t in range(3)]
    wo_copies = [
        pltpu.make_async_copy(wo_hbm.at[pl.ds(pl.multiple_of(((core + i) % 2) * 512, 512), 512), :], wo.at[i], wo_sem.at[i])
        for i in range(2)]
    w1_copies = [pltpu.make_async_copy(w1_hbm.at[:, pl.ds(i * W_FC1, W_FC1)], w1.at[i], w1_sem.at[i]) for i in range(N_FC1)]
    w2_copies = [pltpu.make_async_copy(w2_hbm.at[:, pl.ds(i * W_FC2, W_FC2)], w2.at[i], w2_sem.at[i]) for i in range(N_FC2)]

    rows128 = lax.broadcasted_iota(jnp.int32, (128, 256), 0)
    cols256 = lax.broadcasted_iota(jnp.int32, (128, 256), 1)
    diff = cols256 - rows128 % 16

    def build_sel(i, carry):
        sel[pl.ds(pl.multiple_of(i * 128, 128), 128), :] = jnp.where(diff == i * 16, 1.0, 0.0).astype(BF16)
        return carry
    lax.fori_loop(0, 16, build_sel, 0)

    small_copies[0].wait()
    keep = lax.broadcasted_iota(jnp.int32, (8, 128), 1) // 16 == lax.broadcasted_iota(jnp.int32, (8, 128), 0)

    def spread(n, carry):
        base = pl.multiple_of(n * BLOCK, BLOCK)
        for g in range(48):
            p, c = g // 3, g % 3
            t, col = g // 16, (g % 16) * 128
            for py in range(2):
                row = img[n, c, pl.ds(py * 16 + p, 1), :]
                halves = [jnp.where(keep, jnp.broadcast_to(row[:, i * 128:(i + 1) * 128], (8, 128)), 0.0) for i in range(2)]
                lhs[t, pl.ds(base + py * 16, 16), pl.ds(col, 128)] = jnp.concatenate(halves, axis=0).astype(BF16)
        return carry
    lax.fori_loop(0, IMAGES, spread, 0)
    for t in range(3):
        pix[:, t * 256:(t + 1) * 256] = jnp.dot(lhs[t], sel[...], preferred_element_type=F32).astype(BF16)

    for c in small_copies[1:]:
        c.wait()
    bq_copy.wait()
    for c in wq_copies + wo_copies + w1_copies + w2_copies:
        c.start()

    bp_row = as_row(vecs[0])
    for n in range(4):
        cols = slice(n * 256, (n + 1) * 256)
        emb = jnp.dot(pix[...], wp[:, cols], preferred_element_type=F32) + bp_row[:, cols]
        emb = emb.reshape(IMAGES, BLOCK, 256) + pos[:, cols].astype(F32)[None]
        xs[:, cols] = emb.reshape(OWN, 256).astype(BF16)

    pl.semaphore_wait(barrier, 7)

    def block_rows(slot, k, other):
        if slot == 0:
            first = k + 4 * other
        else:
            first = 8 + (k // 2) + 2 * other + 4 * (k % 2)
        return pl.ds(first * BLOCK, BLOCK)

    def x_block(chip_to, slot):
        image = chip_to if slot == 0 else 4 + chip_to // 2
        return xs.at[pl.ds(pl.multiple_of(image * BLOCK, BLOCK), BLOCK), :]

    sends = []
    for k in (3, 1, 2):
        to = chip_at(k)
        for slot in range(2):
            sends.append(remote(x_block(to, slot), xg.at[block_rows(slot, k, 0), :], xsend.at[k - 1, slot], xrecv.at[k - 1, slot], to * 2 + core))
            sends[-1].start()
    for slot in range(2):
        sends.append(remote(x_block(chip, slot), xg.at[block_rows(slot, 0, 1), :], fsend.at[0, slot], frecv.at[0, slot], mate))
        sends[-1].start()
    xg[block_rows(0, 0, 0), :] = xs[pl.ds(pl.multiple_of(chip * BLOCK, BLOCK), BLOCK), :]
    xg[block_rows(1, 0, 0), :] = xs[pl.ds(pl.multiple_of((4 + cy) * BLOCK, BLOCK), BLOCK), :]

    g1_row, c1_row = as_row(vecs[1]), as_row(vecs[2])

    def norm_block(rows):
        y1[rows, :] = norm_rows(xg[rows, :].astype(F32), g1_row, c1_row).astype(BF16)

    def forwarded(slot, k):
        ref = xg.at[block_rows(slot, k, 1), :]
        return remote(ref, ref, fsend.at[k, slot], frecv.at[k, slot], mate)

    for slot in range(2):
        norm_block(block_rows(slot, 0, 0))
    for slot in range(2):
        forwarded(slot, 0).wait_recv()
        norm_block(block_rows(slot, 0, 1))
    for k in (1, 2, 3):
        for slot in range(2):
            ref = xg.at[block_rows(slot, k, 0), :]
            remote(ref, ref, xsend.at[k - 1, slot], xrecv.at[k - 1, slot], chip_at(k) * 2 + core).wait_recv()
            sends.append(remote(ref, xg.at[block_rows(slot, k, 1), :], fsend.at[k, slot], frecv.at[k, slot], mate))
            sends[-1].start()
        for slot in range(2):
            norm_block(block_rows(slot, k, 0))
    for k in (1, 2, 3):
        for slot in range(2):
            forwarded(slot, k).wait_recv()
            norm_block(block_rows(slot, k, 1))

    for c in wq_copies:
        c.wait()
    brow = [as_row(bqkv[t]) for t in range(3)]
    for n in range(2):
        cols = slice(n * 256, (n + 1) * 256)
        qh[:, cols] = (lax.dot_general(y1[0:384, :], wqkv[0, cols, :], NT, preferred_element_type=F32) + brow[0][:, cols]).astype(BF16)
        kh[:, cols] = (lax.dot_general(y1[...], wqkv[1, cols, :], NT, preferred_element_type=F32) + brow[1][:, cols]).astype(BF16)
        vh[:, cols] = (lax.dot_general(y1[...], wqkv[2, cols, :], NT, preferred_element_type=F32) + brow[2][:, cols]).astype(BF16)

    def attend(q0, rows, k0):
        low = lax.broadcasted_iota(jnp.int32, (rows, 128), 1) < 64
        for pair in range(4):
            cols = slice(pair * 128, (pair + 1) * 128)
            q_pair = qh[q0:q0 + rows, cols]
            k_pair = kh[k0:k0 + 256, cols]
            v_pair = vh[k0:k0 + 256, cols]
            heads = []
            for h in range(2):
                q_one = jnp.where(low == (h == 0), q_pair, jnp.zeros_like(q_pair))
                s = lax.dot_general(q_one, k_pair, NT, preferred_element_type=F32)
                e = jnp.exp2((s - jnp.max(s, axis=-1, keepdims=True)) * EXP_SCALE)
                w = (e * (1.0 / jnp.sum(e, axis=-1, keepdims=True))).astype(BF16)
                heads.append(jnp.dot(w, v_pair, preferred_element_type=F32))
            og[q0:q0 + rows, cols] = jnp.where(low, heads[0], heads[1]).astype(BF16)

    o_parts = ((128, 0, 128), (320, 128, 64))

    def o_send(i):
        src, dst, rows = o_parts[i]
        return remote(og.at[pl.ds(src, rows), :], op.at[pl.ds(dst, rows), :], osend.at[i], orecv.at[i], mate)

    attend(128, 128, 0)
    sends.append(o_send(0))
    sends[-1].start()
    attend(256, 128, 256)
    sends.append(o_send(1))
    sends[-1].start()
    attend(0, 128, 0)

    for c in wo_copies:
        c.wait()
    bo_row = as_row(vecs[3])
    res[0:128, :] = xg[0:128, :].astype(F32) + jnp.dot(og[0:128, :], wo[0], preferred_element_type=F32)
    res[128:192, :] = xg[256:320, :].astype(F32) + jnp.dot(og[256:320, :], wo[0], preferred_element_type=F32)
    for i in range(2):
        o_send(i).wait_recv()
    res[...] = res[...] + jnp.dot(op[...], wo[1], preferred_element_type=F32) + bo_row

    g2_row, c2_row = as_row(vecs[4]), as_row(vecs[5])
    for i in range(6):
        rows = slice(i * BLOCK, (i + 1) * BLOCK)
        y2[rows, :] = norm_rows(res[rows, :], g2_row, c2_row).astype(BF16)

    for i in range(N_FC1):
        b1row[i] = as_row(b1[i * 4:(i + 1) * 4, :])
    for c in w1_copies:
        c.wait()

    def fc1_step(i, carry):
        hid[i] = jax.nn.gelu(jnp.dot(y2[...], w1[i], preferred_element_type=F32) + b1row[i], approximate=True).astype(BF16)
        return carry
    lax.fori_loop(0, N_FC1, fc1_step, 0)

    for c in w2_copies:
        c.wait()
    b2_row = as_row(vecs[6])

    homes = ((0, 0), (0, 1), (0, 2), (0, 3), (1, 0), (1, 2))

    def home_copy(j, b, recv):
        slot, k = homes[b]
        other = chip_at(k)
        owner = other if recv else chip
        image = owner if slot == 0 else 4 + owner // 2
        src = outs.at[j, pl.ds(b * BLOCK, BLOCK), :]
        dst = out_hbm.at[image, :, pl.ds(j * W_FC2, W_FC2)]
        if k == 0:
            return pltpu.make_async_copy(src, dst, rsend.at[j, b])
        return remote(src, dst, rsend.at[j, b], rrecv.at[j, b], other * 2 + core)

    keeps = []
    for j in range(N_FC2):
        cols = slice(j * W_FC2, (j + 1) * W_FC2)
        acc = res[:, cols] + b2_row[:, cols]
        for i in range(N_FC1):
            acc = acc + jnp.dot(hid[i], w2[j, i * W_FC1:(i + 1) * W_FC1, :], preferred_element_type=F32)
        outs[j] = acc.astype(BF16)
        for b in (3, 1, 2, 5, 0, 4):
            copy = home_copy(j, b, False)
            copy.start()
            (keeps if homes[b][1] == 0 else sends).append(copy)

    for j in range(N_FC2):
        for b in (1, 2, 5, 3):
            home_copy(j, b, True).wait_recv()
    for c in keeps:
        c.wait()
    for c in sends:
        c.wait_send()


def solution(mesh):
    def device_step(images, w_patch, b_patch, pos_embed, ln1_gain, ln1_bias, w_qkv, b_qkv, w_out, b_out, ln2_gain, ln2_bias, w_fc1, b_fc1, w_fc2, b_fc2):
        tile = lambda v: v.reshape(-1, 128)
        args = (
            jnp.transpose(images, (0, 3, 1, 2)),
            jnp.transpose(w_patch, (0, 2, 1, 3)).reshape(768, D),
            tile(b_patch), pos_embed, tile(ln1_gain), tile(ln1_bias),
            jnp.transpose(w_qkv, (1, 2, 3, 0)).reshape(3 * D, D),
            b_qkv, w_out.reshape(D, D), tile(b_out), tile(ln2_gain), tile(ln2_bias),
            w_fc1, tile(b_fc1), w_fc2, tile(b_fc2))
        vm = pltpu.VMEM
        dma = pltpu.SemaphoreType.DMA
        return pl.pallas_call(
            layer_kernel,
            out_shape=jax.ShapeDtypeStruct((IMAGES, BLOCK, D), BF16),
            in_specs=[pl.BlockSpec(memory_space=pl.ANY)] * len(args),
            out_specs=pl.BlockSpec(memory_space=pl.ANY),
            scratch_shapes=[
                vm((IMAGES, 3, BLOCK, 256), F32), vm((768, D), BF16), vm((BLOCK, D), BF16), vm((7, 8, 128), F32),
                vm((32, 128), F32), vm((3, 8, 64), F32), vm((3, 512, D), BF16), vm((2, 512, D), BF16),
                vm((N_FC1, D, W_FC1), BF16), vm((N_FC2, FF, W_FC2), BF16),
                vm((3, OWN, 2048), BF16), vm((2048, 256), BF16), vm((OWN, 768), BF16), vm((OWN, D), BF16),
                vm((2 * TOKENS, D), BF16), vm((2 * TOKENS, D), BF16),
                vm((384, 512), BF16), vm((512, 512), BF16), vm((512, 512), BF16), vm((384, 512), BF16), vm((OWN, 512), BF16),
                vm((OWN, D), F32), vm((OWN, D), BF16), vm((N_FC1, OWN, W_FC1), BF16), vm((N_FC2, OWN, W_FC2), BF16),
                vm((N_FC1, 1, W_FC1), F32),
                dma((12,)), dma((3,)), dma((2,)), dma((N_FC1,)), dma((N_FC2,)),
                dma((3, 2)), dma((3, 2)), dma((4, 2)), dma((4, 2)), dma((2,)), dma((2,)), dma((N_FC2, 6)), dma((N_FC2, 6)),
            ],
            compiler_params=pltpu.CompilerParams(
                collective_id=0, has_side_effects=True, vmem_limit_bytes=60 * 1024 * 1024),
        )(*args)

    in_specs = (P('dp', 'sp', None, None), P(), P(), P('sp', None), P(), P(), P(), P(), P(), P(), P(), P(), P(), P(), P(), P())
    return jax.shard_map(device_step, mesh=mesh, in_specs=in_specs, out_specs=P('dp', 'sp', None), check_vma=False)
```

```python
import functools
import math
import jax
import jax.numpy as jnp
from jax import lax
from jax.experimental import pallas as pl
from jax.experimental.pallas import tpu as pltpu
from jax.sharding import PartitionSpec as P

LN_EPS = 1e-6
F32 = jnp.float32
BF16 = jnp.bfloat16
D = 1024
FF = 4096
IMAGES = 6
BLOCK = 32
TOKENS = 256
OWN = 192
N_FC1, W_FC1 = 8, 512
N_FC2, W_FC2 = 4, 256
EXP_SCALE = math.log2(math.e) / 8.0
MESH = pl.DeviceIdType.MESH
NT = (((1,), (1,)), ((), ()))


def as_row(vec):
    return jnp.concatenate([vec[i:i + 1, :] for i in range(vec.shape[0])], axis=1)


def norm_rows(x_in, gain, bias):
    centered = x_in - jnp.mean(x_in, axis=-1, keepdims=True)
    variance = jnp.mean(centered * centered, axis=-1, keepdims=True)
    return centered * lax.rsqrt(variance + LN_EPS) * gain + bias


def layer_kernel(
        img_hbm, wp_hbm, bp_hbm, pos_hbm, g1_hbm, c1_hbm, wqkv_hbm, bqkv_hbm, wo_hbm, bo_hbm, g2_hbm, c2_hbm,
        w1_hbm, b1_hbm, w2_hbm, b2_hbm,
        out_hbm,
        img, wp, pos, vecs, b1, bqkv, wqkv, wo, w1, w2,
        lhs, sel, pix, xs, xg, y1, qh, kh, vh, og, op, res, y2, hid, outs, b1row, pre,
        in_sem, wqkv_sem, wo_sem, w1_sem, w2_sem,
        xsend, xrecv, fsend, frecv, osend, orecv, rsend, rrecv):
    dp = lax.axis_index("dp")
    me = lax.axis_index("sp")
    chip = me // 2
    core = me % 2
    mate = chip * 2 + (1 - core)
    cx = chip % 2
    cy = chip // 2

    def remote(src, dst, ssem, rsem, dev):
        return pltpu.make_async_remote_copy(
            src_ref=src, dst_ref=dst, send_sem=ssem, recv_sem=rsem, device_id=(dp, dev), device_id_type=MESH)

    def chip_at(k):
        return ((cy + k // 2) % 2) * 2 + (cx + k % 2) % 2

    barrier = pltpu.get_barrier_semaphore()
    for k in range(1, 8):
        pl.semaphore_signal(barrier, inc=1, device_id=(dp, (me + k) % 8), device_id_type=MESH)

    small = [(img_hbm, img), (wp_hbm, wp), (pos_hbm, pos)]
    for i, v in enumerate((bp_hbm, g1_hbm, c1_hbm, bo_hbm, g2_hbm, c2_hbm, b2_hbm)):
        small.append((v, vecs.at[i]))
    small.append((b1_hbm, b1))
    small_copies = [pltpu.make_async_copy(s, d, in_sem.at[i]) for i, (s, d) in enumerate(small)]
    for c in small_copies:
        c.start()
    bq_copy = pltpu.make_async_copy(bqkv_hbm.at[:, pl.ds(pl.multiple_of(core * 8, 8), 8), :], bqkv, in_sem.at[len(small)])
    bq_copy.start()
    wq_copies = [
        pltpu.make_async_copy(wqkv_hbm.at[pl.ds(pl.multiple_of(t * D + core * 512, 512), 512), :], wqkv.at[t], wqkv_sem.at[t])
        for t in range(3)]
    wo_copies = [
        pltpu.make_async_copy(wo_hbm.at[pl.ds(pl.multiple_of(((core + i) % 2) * 512, 512), 512), :], wo.at[i], wo_sem.at[i])
        for i in range(2)]
    w1_copies = [pltpu.make_async_copy(w1_hbm.at[:, pl.ds(i * W_FC1, W_FC1)], w1.at[i], w1_sem.at[i]) for i in range(N_FC1)]
    w2_copies = [pltpu.make_async_copy(w2_hbm.at[:, pl.ds(i * W_FC2, W_FC2)], w2.at[i], w2_sem.at[i]) for i in range(N_FC2)]

    rows128 = lax.broadcasted_iota(jnp.int32, (128, 256), 0)
    cols256 = lax.broadcasted_iota(jnp.int32, (128, 256), 1)
    diff = cols256 - rows128 % 16

    def build_sel(i, carry):
        sel[pl.ds(pl.multiple_of(i * 128, 128), 128), :] = jnp.where(diff == i * 16, 1.0, 0.0).astype(BF16)
        return carry
    lax.fori_loop(0, 16, build_sel, 0)

    small_copies[0].wait()
    keep = lax.broadcasted_iota(jnp.int32, (8, 128), 1) // 16 == lax.broadcasted_iota(jnp.int32, (8, 128), 0)

    def spread(n, carry):
        base = pl.multiple_of(n * BLOCK, BLOCK)
        for g in range(48):
            p, c = g // 3, g % 3
            t, col = g // 16, (g % 16) * 128
            for py in range(2):
                row = img[n, c, pl.ds(py * 16 + p, 1), :]
                halves = [jnp.where(keep, jnp.broadcast_to(row[:, i * 128:(i + 1) * 128], (8, 128)), 0.0) for i in range(2)]
                lhs[t, pl.ds(base + py * 16, 16), pl.ds(col, 128)] = jnp.concatenate(halves, axis=0).astype(BF16)
        return carry
    lax.fori_loop(0, IMAGES, spread, 0)
    for t in range(3):
        pix[:, t * 256:(t + 1) * 256] = jnp.dot(lhs[t], sel[...], preferred_element_type=F32).astype(BF16)

    for c in small_copies[1:]:
        c.wait()
    bq_copy.wait()
    for c in wq_copies + wo_copies + w1_copies + w2_copies:
        c.start()

    bp_row = as_row(vecs[0])
    for n in range(4):
        cols = slice(n * 256, (n + 1) * 256)
        emb = jnp.dot(pix[...], wp[:, cols], preferred_element_type=F32) + bp_row[:, cols]
        emb = emb.reshape(IMAGES, BLOCK, 256) + pos[:, cols].astype(F32)[None]
        xs[:, cols] = emb.reshape(OWN, 256).astype(BF16)

    pl.semaphore_wait(barrier, 7)

    def block_rows(slot, k, other):
        if slot == 0:
            first = k + 4 * other
        else:
            first = 8 + (k // 2) + 2 * other + 4 * (k % 2)
        return pl.ds(first * BLOCK, BLOCK)

    def x_block(chip_to, slot):
        image = chip_to if slot == 0 else 4 + chip_to // 2
        return xs.at[pl.ds(pl.multiple_of(image * BLOCK, BLOCK), BLOCK), :]

    sends = []
    for k in (3, 1, 2):
        to = chip_at(k)
        for slot in range(2):
            sends.append(remote(x_block(to, slot), xg.at[block_rows(slot, k, 0), :], xsend.at[k - 1, slot], xrecv.at[k - 1, slot], to * 2 + core))
            sends[-1].start()
    for slot in range(2):
        sends.append(remote(x_block(chip, slot), xg.at[block_rows(slot, 0, 1), :], fsend.at[0, slot], frecv.at[0, slot], mate))
        sends[-1].start()
    xg[block_rows(0, 0, 0), :] = xs[pl.ds(pl.multiple_of(chip * BLOCK, BLOCK), BLOCK), :]
    xg[block_rows(1, 0, 0), :] = xs[pl.ds(pl.multiple_of((4 + cy) * BLOCK, BLOCK), BLOCK), :]

    g1_row, c1_row = as_row(vecs[1]), as_row(vecs[2])

    def norm_block(rows):
        y1[rows, :] = norm_rows(xg[rows, :].astype(F32), g1_row, c1_row).astype(BF16)

    def forwarded(slot, k):
        ref = xg.at[block_rows(slot, k, 1), :]
        return remote(ref, ref, fsend.at[k, slot], frecv.at[k, slot], mate)

    for slot in range(2):
        norm_block(block_rows(slot, 0, 0))
    for slot in range(2):
        forwarded(slot, 0).wait_recv()
        norm_block(block_rows(slot, 0, 1))
    for k in (1, 2, 3):
        for slot in range(2):
            ref = xg.at[block_rows(slot, k, 0), :]
            remote(ref, ref, xsend.at[k - 1, slot], xrecv.at[k - 1, slot], chip_at(k) * 2 + core).wait_recv()
            sends.append(remote(ref, xg.at[block_rows(slot, k, 1), :], fsend.at[k, slot], frecv.at[k, slot], mate))
            sends[-1].start()
        for slot in range(2):
            norm_block(block_rows(slot, k, 0))
    for k in (1, 2, 3):
        for slot in range(2):
            forwarded(slot, k).wait_recv()
            norm_block(block_rows(slot, k, 1))

    for c in wq_copies:
        c.wait()
    brow = [as_row(bqkv[t]) for t in range(3)]
    qh[...] = (lax.dot_general(y1[0:384, :], wqkv[0], NT, preferred_element_type=F32) + brow[0]).astype(BF16)
    kh[...] = (lax.dot_general(y1[...], wqkv[1], NT, preferred_element_type=F32) + brow[1]).astype(BF16)
    vh[...] = (lax.dot_general(y1[...], wqkv[2], NT, preferred_element_type=F32) + brow[2]).astype(BF16)

    def attend(q0, rows, k0):
        low = lax.broadcasted_iota(jnp.int32, (rows, 128), 1) < 64
        for pair in range(4):
            cols = slice(pair * 128, (pair + 1) * 128)
            q_pair = qh[q0:q0 + rows, cols]
            k_pair = kh[k0:k0 + 256, cols]
            v_pair = vh[k0:k0 + 256, cols]
            heads = []
            for h in range(2):
                q_one = jnp.where(low == (h == 0), q_pair, jnp.zeros_like(q_pair))
                s = lax.dot_general(q_one, k_pair, NT, preferred_element_type=F32)
                e = jnp.exp2((s - jnp.max(s, axis=-1, keepdims=True)) * EXP_SCALE)
                w = (e * (1.0 / jnp.sum(e, axis=-1, keepdims=True))).astype(BF16)
                heads.append(jnp.dot(w, v_pair, preferred_element_type=F32))
            og[q0:q0 + rows, cols] = jnp.where(low, heads[0], heads[1]).astype(BF16)

    o_parts = ((128, 0, 128), (320, 128, 64))

    def o_send(i):
        src, dst, rows = o_parts[i]
        return remote(og.at[pl.ds(src, rows), :], op.at[pl.ds(dst, rows), :], osend.at[i], orecv.at[i], mate)

    attend(128, 128, 0)
    sends.append(o_send(0))
    sends[-1].start()
    attend(256, 128, 256)
    sends.append(o_send(1))
    sends[-1].start()
    attend(0, 128, 0)

    for c in wo_copies:
        c.wait()
    bo_row = as_row(vecs[3])
    res[0:128, :] = xg[0:128, :].astype(F32) + jnp.dot(og[0:128, :], wo[0], preferred_element_type=F32)
    res[128:192, :] = xg[256:320, :].astype(F32) + jnp.dot(og[256:320, :], wo[0], preferred_element_type=F32)
    for i in range(2):
        o_send(i).wait_recv()
    res[...] = res[...] + jnp.dot(op[...], wo[1], preferred_element_type=F32) + bo_row

    g2_row, c2_row = as_row(vecs[4]), as_row(vecs[5])
    for i in range(6):
        rows = slice(i * BLOCK, (i + 1) * BLOCK)
        y2[rows, :] = norm_rows(res[rows, :], g2_row, c2_row).astype(BF16)

    for i in range(N_FC1):
        b1row[i] = as_row(b1[i * 4:(i + 1) * 4, :])
    for c in w1_copies:
        c.wait()

    def activate(i):
        hid[:, i * W_FC1:(i + 1) * W_FC1] = jax.nn.gelu(pre[i % 2], approximate=True).astype(BF16)

    for i in range(N_FC1):
        pre[i % 2] = jnp.dot(y2[...], w1[i], preferred_element_type=F32) + b1row[i]
        if i:
            activate(i - 1)
    activate(N_FC1 - 1)

    for c in w2_copies:
        c.wait()
    b2_row = as_row(vecs[6])

    homes = ((0, 0), (0, 1), (0, 2), (0, 3), (1, 0), (1, 2))

    def home_copy(j, b, recv):
        slot, k = homes[b]
        other = chip_at(k)
        owner = other if recv else chip
        image = owner if slot == 0 else 4 + owner // 2
        src = outs.at[j, pl.ds(b * BLOCK, BLOCK), :]
        dst = out_hbm.at[image, :, pl.ds(j * W_FC2, W_FC2)]
        if k == 0:
            return pltpu.make_async_copy(src, dst, rsend.at[j, b])
        return remote(src, dst, rsend.at[j, b], rrecv.at[j, b], other * 2 + core)

    keeps = []
    for j in range(N_FC2):
        cols = slice(j * W_FC2, (j + 1) * W_FC2)
        parts = [jnp.dot(hid[:, i:i + FF // 2], w2[j, i:i + FF // 2, :], preferred_element_type=F32) for i in (0, FF // 2)]
        outs[j] = (parts[0] + parts[1] + (res[:, cols] + b2_row[:, cols])).astype(BF16)
        for b in (3, 1, 2, 5, 0, 4):
            copy = home_copy(j, b, False)
            copy.start()
            (keeps if homes[b][1] == 0 else sends).append(copy)

    for j in range(N_FC2):
        for b in (1, 2, 5, 3):
            home_copy(j, b, True).wait_recv()
    for c in keeps:
        c.wait()
    for c in sends:
        c.wait_send()


def solution(mesh):
    def device_step(images, w_patch, b_patch, pos_embed, ln1_gain, ln1_bias, w_qkv, b_qkv, w_out, b_out, ln2_gain, ln2_bias, w_fc1, b_fc1, w_fc2, b_fc2):
        tile = lambda v: v.reshape(-1, 128)
        args = (
            jnp.transpose(images, (0, 3, 1, 2)),
            jnp.transpose(w_patch, (0, 2, 1, 3)).reshape(768, D),
            tile(b_patch), pos_embed, tile(ln1_gain), tile(ln1_bias),
            jnp.transpose(w_qkv, (1, 2, 3, 0)).reshape(3 * D, D),
            b_qkv, w_out.reshape(D, D), tile(b_out), tile(ln2_gain), tile(ln2_bias),
            w_fc1, tile(b_fc1), w_fc2, tile(b_fc2))
        vm = pltpu.VMEM
        dma = pltpu.SemaphoreType.DMA
        return pl.pallas_call(
            layer_kernel,
            out_shape=jax.ShapeDtypeStruct((IMAGES, BLOCK, D), BF16),
            in_specs=[pl.BlockSpec(memory_space=pl.ANY)] * len(args),
            out_specs=pl.BlockSpec(memory_space=pl.ANY),
            scratch_shapes=[
                vm((IMAGES, 3, BLOCK, 256), F32), vm((768, D), BF16), vm((BLOCK, D), BF16), vm((7, 8, 128), F32),
                vm((32, 128), F32), vm((3, 8, 64), F32), vm((3, 512, D), BF16), vm((2, 512, D), BF16),
                vm((N_FC1, D, W_FC1), BF16), vm((N_FC2, FF, W_FC2), BF16),
                vm((3, OWN, 2048), BF16), vm((2048, 256), BF16), vm((OWN, 768), BF16), vm((OWN, D), BF16),
                vm((2 * TOKENS, D), BF16), vm((2 * TOKENS, D), BF16),
                vm((384, 512), BF16), vm((512, 512), BF16), vm((512, 512), BF16), vm((384, 512), BF16), vm((OWN, 512), BF16),
                vm((OWN, D), F32), vm((OWN, D), BF16), vm((OWN, FF), BF16), vm((N_FC2, OWN, W_FC2), BF16),
                vm((N_FC1, 1, W_FC1), F32), vm((2, OWN, W_FC1), F32),
                dma((12,)), dma((3,)), dma((2,)), dma((N_FC1,)), dma((N_FC2,)),
                dma((3, 2)), dma((3, 2)), dma((4, 2)), dma((4, 2)), dma((2,)), dma((2,)), dma((N_FC2, 6)), dma((N_FC2, 6)),
            ],
            compiler_params=pltpu.CompilerParams(
                collective_id=0, has_side_effects=True, vmem_limit_bytes=60 * 1024 * 1024),
        )(*args)

    in_specs = (P('dp', 'sp', None, None), P(), P(), P('sp', None), P(), P(), P(), P(), P(), P(), P(), P(), P(), P(), P(), P())
    return jax.shard_map(device_step, mesh=mesh, in_specs=in_specs, out_specs=P('dp', 'sp', None), check_vma=False)
```

```python
import functools
import math
import jax
import jax.numpy as jnp
from jax import lax
from jax.experimental import pallas as pl
from jax.experimental.pallas import tpu as pltpu
from jax.sharding import PartitionSpec as P

LN_EPS = 1e-6
F32 = jnp.float32
BF16 = jnp.bfloat16
D = 1024
FF = 4096
IMAGES = 6
BLOCK = 32
TOKENS = 256
OWN = 192
HALF = 96
N_FC1, W_FC1 = 8, 512
N_FC2, W_FC2 = 2, 512
EXP_SCALE = math.log2(math.e) / 8.0
MESH = pl.DeviceIdType.MESH
NT = (((1,), (1,)), ((), ()))


def as_row(vec):
    return jnp.concatenate([vec[i:i + 1, :] for i in range(vec.shape[0])], axis=1)


def norm_rows(x_in, gain, bias):
    centered = x_in - jnp.mean(x_in, axis=-1, keepdims=True)
    variance = jnp.mean(centered * centered, axis=-1, keepdims=True)
    return centered * lax.rsqrt(variance + LN_EPS) * gain + bias


def layer_kernel(
        img_hbm, wp_hbm, bp_hbm, pos_hbm, g1_hbm, c1_hbm, wqkv_hbm, bqkv_hbm, wo_hbm, bo_hbm, g2_hbm, c2_hbm,
        w1_hbm, b1_hbm, w2_hbm, b2_hbm,
        out_hbm,
        img, wp, pos, vecs, b1, bqkv, wqkv, wo, w1, w2,
        lhs, sel, pix, xs, xg, y1, qh, kh, vh, og, op, oh, res, y2, hid, outs, b1row, pre,
        in_sem, wqkv_sem, wo_sem, w1_sem, w2_sem,
        xsend, xrecv, fsend, frecv, osend, orecv, hsend, hrecv, rsend, rrecv, keep_sem):
    dp = lax.axis_index("dp")
    me = lax.axis_index("sp")
    chip = me // 2
    core = me % 2
    mate = chip * 2 + (1 - core)
    cx = chip % 2
    cy = chip // 2

    def remote(src, dst, ssem, rsem, dev):
        return pltpu.make_async_remote_copy(
            src_ref=src, dst_ref=dst, send_sem=ssem, recv_sem=rsem, device_id=(dp, dev), device_id_type=MESH)

    def chip_at(k):
        return ((cy + k // 2) % 2) * 2 + (cx + k % 2) % 2

    barrier = pltpu.get_barrier_semaphore()
    for k in range(1, 8):
        pl.semaphore_signal(barrier, inc=1, device_id=(dp, (me + k) % 8), device_id_type=MESH)

    groups = ((4, 2), (0, 4))
    small = [(img_hbm.at[pl.ds(n0, n), :, :, :], img.at[pl.ds(n0, n), :, :, :]) for n0, n in groups] + [(wp_hbm, wp), (pos_hbm, pos)]
    for i, v in enumerate((bp_hbm, g1_hbm, c1_hbm, bo_hbm, g2_hbm, c2_hbm, b2_hbm)):
        small.append((v, vecs.at[i]))
    small.append((b1_hbm, b1))
    small.append((bqkv_hbm.at[:, pl.ds(pl.multiple_of(core * 8, 8), 8), :], bqkv))
    small_copies = [pltpu.make_async_copy(s, d, in_sem.at[i]) for i, (s, d) in enumerate(small)]
    for i in (0, 2, 1) + tuple(range(3, len(small))):
        small_copies[i].start()
    wq_copies = [
        pltpu.make_async_copy(wqkv_hbm.at[pl.ds(pl.multiple_of(t * D + core * 512, 512), 512), :], wqkv.at[t], wqkv_sem.at[t])
        for t in range(3)]
    wo_copies = [
        pltpu.make_async_copy(wo_hbm.at[pl.ds(pl.multiple_of(((core + i) % 2) * 512, 512), 512), :], wo.at[i], wo_sem.at[i])
        for i in range(2)]
    w1_copies = [pltpu.make_async_copy(w1_hbm.at[:, pl.ds(i * W_FC1, W_FC1)], w1.at[i], w1_sem.at[i]) for i in range(N_FC1)]
    w2_copies = [pltpu.make_async_copy(w2_hbm.at[:, pl.ds(i * W_FC2, W_FC2)], w2.at[i], w2_sem.at[i]) for i in range(N_FC2)]

    rows128 = lax.broadcasted_iota(jnp.int32, (128, 256), 0)
    cols256 = lax.broadcasted_iota(jnp.int32, (128, 256), 1)
    diff = cols256 - rows128 % 16

    def build_sel(i, carry):
        sel[pl.ds(pl.multiple_of(i * 128, 128), 128), :] = jnp.where(diff == i * 16, 1.0, 0.0).astype(BF16)
        return carry
    lax.fori_loop(0, 16, build_sel, 0)

    keep = lax.broadcasted_iota(jnp.int32, (8, 128), 1) // 16 == lax.broadcasted_iota(jnp.int32, (8, 128), 0)

    def embed(group):
        n0, count = groups[group]
        m = count * BLOCK
        top = n0 * BLOCK * 3

        def spread(i, carry):
            for g in range(48):
                p, c = g // 3, g % 3
                t, col = g // 16, (g % 16) * 128
                for py in range(2):
                    row = img[n0 + i, c, pl.ds(py * 16 + p, 1), :]
                    halves = [jnp.where(keep, jnp.broadcast_to(row[:, j * 128:(j + 1) * 128], (8, 128)), 0.0) for j in range(2)]
                    at = pl.multiple_of(top + t * m + i * BLOCK + py * 16, 16)
                    lhs[pl.ds(at, 16), pl.ds(col, 128)] = jnp.concatenate(halves, axis=0).astype(BF16)
            return carry
        lax.fori_loop(0, count, spread, 0)
        h = 3 * m // 2
        both = [jnp.dot(lhs[top + i * h:top + (i + 1) * h, :], sel[...], preferred_element_type=F32).astype(BF16) for i in range(2)]
        rows = slice(n0 * BLOCK, n0 * BLOCK + m)
        pix[rows, 0:256] = both[0][0:m]
        pix[rows, 256:512] = jnp.concatenate([both[0][m:], both[1][0:m // 2]], axis=0)
        pix[rows, 512:768] = both[1][m // 2:]
        return rows, count

    def project(rows, count):
        for n in range(2):
            cols = slice(n * 512, (n + 1) * 512)
            emb = jnp.dot(pix[rows, :], wp[:, cols], preferred_element_type=F32) + bp_row[:, cols]
            emb = emb.reshape(count, BLOCK, 512) + pos[:, cols].astype(F32)[None]
            xs[rows, cols] = emb.reshape(count * BLOCK, 512).astype(BF16)

    slot1_first = {3: 8, 1: 10, 0: 12, 2: 13}

    def block(slot, k, other):
        first = 2 * k + other if slot == 0 else slot1_first[k] + other * (2 if k in (0, 2) else 1)
        return pl.ds(first * BLOCK, BLOCK)

    def x_block(chip_to, slot):
        image = chip_to if slot == 0 else 4 + chip_to // 2
        return pl.ds(pl.multiple_of(image * BLOCK, BLOCK), BLOCK)

    sends = []

    def start(copy):
        copy.start()
        sends.append(copy)

    def send_slot(slot):
        for k in (2, 1, 3):
            to = chip_at(k)
            start(remote(xs.at[x_block(to, slot), :], xg.at[block(slot, k, 0), :], xsend.at[k - 1, slot], xrecv.at[k - 1, slot], to * 2 + core))
        start(remote(xs.at[x_block(chip, slot), :], xg.at[block(slot, 0, 1), :], fsend.at[0, slot], frecv.at[0, slot], mate))
        xg[block(slot, 0, 0), :] = xs[x_block(chip, slot), :]

    small_copies[0].wait()
    part = embed(0)
    for c in small_copies[2:]:
        c.wait()
    small_copies[1].wait()
    for c in wq_copies + wo_copies + w1_copies + w2_copies:
        c.start()
    bp_row = as_row(vecs[0])
    project(*part)
    pl.semaphore_wait(barrier, 7)
    send_slot(1)
    project(*embed(1))
    send_slot(0)

    g1_row, c1_row = as_row(vecs[1]), as_row(vecs[2])

    def norm_blocks(blocks):
        for rows in blocks:
            y1[rows, :] = norm_rows(xg[rows, :].astype(F32), g1_row, c1_row).astype(BF16)

    def arrive(slot, k):
        ref = xg.at[block(slot, k, 0), :]
        remote(ref, ref, xsend.at[k - 1, slot], xrecv.at[k - 1, slot], chip_at(k) * 2 + core).wait_recv()
        start(remote(ref, xg.at[block(slot, k, 1), :], fsend.at[k, slot], frecv.at[k, slot], mate))

    def forwarded(slot, k):
        ref = xg.at[block(slot, k, 1), :]
        remote(ref, ref, fsend.at[k, slot], frecv.at[k, slot], mate).wait_recv()

    norm_blocks([block(1, 0, 0), block(0, 0, 0)])
    for slot in (1, 0):
        forwarded(slot, 0)
    norm_blocks([block(1, 0, 1), block(0, 0, 1)])
    for slot in (1, 0):
        for k in (2, 1):
            arrive(slot, k)
        norm_blocks([block(slot, k, 0) for k in (2, 1)])
    for c in wq_copies:
        c.wait()
    brow = [as_row(bqkv[t]) for t in range(3)]
    for slot in (1, 0):
        for k in (2, 1):
            forwarded(slot, k)
    norm_blocks([block(slot, k, 1) for slot in (1, 0) for k in (2, 1)])

    early_q, early_kv = ((0, 192), (384, 512)), ((0, 192), (320, 512))

    def heads_of(t, dst, pieces):
        rows = jnp.concatenate([y1[a:b, :] for a, b in pieces], axis=0)
        got = (lax.dot_general(rows, wqkv[t], NT, preferred_element_type=F32) + brow[t]).astype(BF16)
        at = 0
        for a, b in pieces:
            dst[a:b, :] = got[at:at + b - a]
            at += b - a

    heads_of(0, qh, early_q)
    heads_of(1, kh, early_kv)
    for slot in (1, 0):
        arrive(slot, 3)
    heads_of(2, vh, early_kv)
    norm_blocks([block(slot, 3, 0) for slot in (1, 0)])
    for slot in (1, 0):
        forwarded(slot, 3)
    norm_blocks([block(slot, 3, 1) for slot in (1, 0)])
    heads_of(0, qh, ((192, 256),))
    heads_of(1, kh, ((192, 320),))
    heads_of(2, vh, ((192, 320),))

    def attend(q0, rows, k0):
        low = lax.broadcasted_iota(jnp.int32, (rows, 128), 1) < 64
        for pair in range(4):
            cols = slice(pair * 128, (pair + 1) * 128)
            q_pair = qh[q0:q0 + rows, cols]
            k_pair = kh[k0:k0 + 256, cols]
            v_pair = vh[k0:k0 + 256, cols]
            heads = []
            for h in range(2):
                q_one = jnp.where(low == (h == 0), q_pair, jnp.zeros_like(q_pair))
                s = lax.dot_general(q_one, k_pair, NT, preferred_element_type=F32)
                e = jnp.exp2((s - jnp.max(s, axis=-1, keepdims=True)) * EXP_SCALE)
                w = (e * (1.0 / jnp.sum(e, axis=-1, keepdims=True))).astype(BF16)
                heads.append(jnp.dot(w, v_pair, preferred_element_type=F32))
            og[q0:q0 + rows, cols] = jnp.where(low, heads[0], heads[1]).astype(BF16)

    def o_home(k, other, recv):
        dev = chip_at(k) * 2 + (core if other == 0 else 1 - core)
        return remote(og.at[block(0, k, other), :], oh.at[other, pl.ds((k - 1) * BLOCK, BLOCK), :],
                      hsend.at[k - 1, other], hrecv.at[k - 1, other], dev)

    o_parts = ((32, 0, 32), (448, 32, 64))

    def o_send(i):
        src, dst, rows = o_parts[i]
        return remote(og.at[pl.ds(src, rows), :], op.at[pl.ds(dst, rows), :], osend.at[i], orecv.at[i], mate)

    attend(128, 128, 0)
    for k, other in ((3, 0), (3, 1), (2, 0), (2, 1)):
        start(o_home(k, other, False))
    attend(0, 128, 0)
    start(o_send(0))
    for other in range(2):
        start(o_home(1, other, False))
    attend(384, 128, 256)
    start(o_send(1))

    for c in wo_copies + w1_copies + w2_copies:
        c.wait()
    bo_row, g2_row, c2_row, b2_row = [as_row(vecs[i]) for i in (3, 4, 5, 6)]
    for i in range(N_FC1):
        b1row[i] = as_row(b1[i * 4:(i + 1) * 4, :])

    def finish(x_in, near, far, ready):
        res[...] = x_in.astype(F32) + jnp.dot(near(), wo[0], preferred_element_type=F32)
        ready()
        res[...] = res[...] + jnp.dot(far(), wo[1], preferred_element_type=F32) + bo_row
        for i in range(3):
            rows = slice(i * BLOCK, (i + 1) * BLOCK)
            y2[rows, :] = norm_rows(res[rows, :], g2_row, c2_row).astype(BF16)

        def activate(i):
            hid[:, i * W_FC1:(i + 1) * W_FC1] = jax.nn.gelu(pre[i % 2], approximate=True).astype(BF16)

        for i in range(N_FC1):
            pre[i % 2] = jnp.dot(y2[...], w1[i], preferred_element_type=F32) + b1row[i]
            if i:
                activate(i - 1)
        activate(N_FC1 - 1)

    def second(j):
        cols = slice(j * W_FC2, (j + 1) * W_FC2)
        return (jnp.dot(hid[...], w2[j], preferred_element_type=F32) + (res[:, cols] + b2_row[:, cols])).astype(BF16)

    def mate_ready():
        for i in range(2):
            o_send(i).wait_recv()

    finish(jnp.concatenate([xg[0:32, :], xg[384:448, :]], axis=0),
           lambda: jnp.concatenate([og[0:32, :], og[384:448, :]], axis=0), lambda: op[...], mate_ready)

    def shared_home(j, recv):
        other = chip_at(2)
        image = 4 + (other if recv else chip) // 2
        return remote(outs.at[0, j, pl.ds(64, BLOCK), :], out_hbm.at[image, :, pl.ds(j * W_FC2, W_FC2)],
                      rsend.at[j], rrecv.at[j], other * 2 + core)

    keeps = []

    def keep_rows(half, j, b, image):
        copy = pltpu.make_async_copy(outs.at[half, j, pl.ds(b * BLOCK, BLOCK), :], out_hbm.at[image, :, pl.ds(j * W_FC2, W_FC2)],
                                     keep_sem.at[half, j, b])
        copy.start()
        keeps.append(copy)

    for j in range(N_FC2):
        outs[0, j] = second(j)
        start(shared_home(j, False))
        keep_rows(0, j, 0, chip)
        keep_rows(0, j, 1, 4 + cy)

    def home_ready():
        for k in (1, 2, 3):
            o_home(k, 1, True).wait_recv()

    for k in (1, 2, 3):
        o_home(k, 0, True).wait_recv()
    finish(jnp.concatenate([xs[x_block(chip_at(k), 0), :] for k in (1, 2, 3)], axis=0), lambda: oh[0], lambda: oh[1], home_ready)
    for j in range(N_FC2):
        outs[1, j] = second(j)
        for k in (1, 2, 3):
            keep_rows(1, j, k - 1, chip_at(k))

    for j in range(N_FC2):
        shared_home(j, True).wait_recv()
    for c in keeps:
        c.wait()
    for c in sends:
        c.wait_send()


def solution(mesh):
    def device_step(images, w_patch, b_patch, pos_embed, ln1_gain, ln1_bias, w_qkv, b_qkv, w_out, b_out, ln2_gain, ln2_bias, w_fc1, b_fc1, w_fc2, b_fc2):
        tile = lambda v: v.reshape(-1, 128)
        args = (
            jnp.transpose(images, (0, 3, 1, 2)),
            jnp.transpose(w_patch, (0, 2, 1, 3)).reshape(768, D),
            tile(b_patch), pos_embed, tile(ln1_gain), tile(ln1_bias),
            jnp.transpose(w_qkv, (1, 2, 3, 0)).reshape(3 * D, D),
            b_qkv, w_out.reshape(D, D), tile(b_out), tile(ln2_gain), tile(ln2_bias),
            w_fc1, tile(b_fc1), w_fc2, tile(b_fc2))
        vm = pltpu.VMEM
        dma = pltpu.SemaphoreType.DMA
        return pl.pallas_call(
            layer_kernel,
            out_shape=jax.ShapeDtypeStruct((IMAGES, BLOCK, D), BF16),
            in_specs=[pl.BlockSpec(memory_space=pl.ANY)] * len(args),
            out_specs=pl.BlockSpec(memory_space=pl.ANY),
            scratch_shapes=[
                vm((IMAGES, 3, BLOCK, 256), F32), vm((768, D), BF16), vm((BLOCK, D), BF16), vm((7, 8, 128), F32),
                vm((32, 128), F32), vm((3, 8, 64), F32), vm((3, 512, D), BF16), vm((2, 512, D), BF16),
                vm((N_FC1, D, W_FC1), BF16), vm((N_FC2, FF, W_FC2), BF16),
                vm((3 * OWN, 2048), BF16), vm((2048, 256), BF16), vm((OWN, 768), BF16), vm((OWN, D), BF16),
                vm((2 * TOKENS, D), BF16), vm((2 * TOKENS, D), BF16),
                vm((512, 512), BF16), vm((512, 512), BF16), vm((512, 512), BF16), vm((512, 512), BF16),
                vm((HALF, 512), BF16), vm((2, HALF, 512), BF16),
                vm((HALF, D), F32), vm((HALF, D), BF16), vm((HALF, FF), BF16), vm((2, N_FC2, HALF, W_FC2), BF16),
                vm((N_FC1, 1, W_FC1), F32), vm((2, HALF, W_FC1), F32),
                dma((13,)), dma((3,)), dma((2,)), dma((N_FC1,)), dma((N_FC2,)),
                dma((3, 2)), dma((3, 2)), dma((4, 2)), dma((4, 2)), dma((2,)), dma((2,)), dma((3, 2)), dma((3, 2)),
                dma((N_FC2,)), dma((N_FC2,)), dma((2, N_FC2, 3)),
            ],
            compiler_params=pltpu.CompilerParams(
                collective_id=0, has_side_effects=True, vmem_limit_bytes=60 * 1024 * 1024),
        )(*args)

    in_specs = (P('dp', 'sp', None, None), P(), P(), P('sp', None), P(), P(), P(), P(), P(), P(), P(), P(), P(), P(), P(), P())
    return jax.shard_map(device_step, mesh=mesh, in_specs=in_specs, out_specs=P('dp', 'sp', None), check_vma=False)
```

```python
import functools
import math
import jax
import jax.numpy as jnp
from jax import lax
from jax.experimental import pallas as pl
from jax.experimental.pallas import tpu as pltpu
from jax.sharding import PartitionSpec as P

LN_EPS = 1e-6
F32 = jnp.float32
BF16 = jnp.bfloat16
D = 1024
FF = 4096
IMAGES = 6
BLOCK = 32
TOKENS = 256
OWN = 192
HALF = 128
N_FC1, W_FC1 = 8, 512
N_FC2, W_FC2 = 2, 512
EXP_SCALE = math.log2(math.e) / 8.0
MESH = pl.DeviceIdType.MESH
NT = (((1,), (1,)), ((), ()))


def as_row(vec):
    return jnp.concatenate([vec[i:i + 1, :] for i in range(vec.shape[0])], axis=1)


def norm_rows(x_in, gain, bias):
    centered = x_in - jnp.mean(x_in, axis=-1, keepdims=True)
    variance = jnp.mean(centered * centered, axis=-1, keepdims=True)
    return centered * lax.rsqrt(variance + LN_EPS) * gain + bias


def layer_kernel(
        img_hbm, wp_hbm, bp_hbm, pos_hbm, g1_hbm, c1_hbm, wqkv_hbm, bqkv_hbm, wo_hbm, bo_hbm, g2_hbm, c2_hbm,
        w1_hbm, b1_hbm, w2_hbm, b2_hbm,
        out,
        img, wp, pos, vecs, b1, bqkv, wqkv, wo, w1, w2,
        lhs, sel, pix, xs, xg, y1, qh, kh, vh, og, op, oh, res, y2, hid, back, b1row, pre,
        in_sem, wqkv_sem, wo_sem, w1_sem, w2_sem,
        xsend, xrecv, fsend, frecv, osend, orecv, hsend, hrecv, rsend, rrecv):
    dp = lax.axis_index("dp")
    me = lax.axis_index("sp")
    chip = me // 2
    core = me % 2
    mate = chip * 2 + (1 - core)
    cx = chip % 2
    cy = chip // 2

    def remote(src, dst, ssem, rsem, dev):
        return pltpu.make_async_remote_copy(
            src_ref=src, dst_ref=dst, send_sem=ssem, recv_sem=rsem, device_id=(dp, dev), device_id_type=MESH)

    def chip_at(k):
        return ((cy + k // 2) % 2) * 2 + (cx + k % 2) % 2

    barrier = pltpu.get_barrier_semaphore()
    for k in range(1, 8):
        pl.semaphore_signal(barrier, inc=1, device_id=(dp, (me + k) % 8), device_id_type=MESH)

    groups = ((4, 2), (0, 4))
    small = [(img_hbm.at[pl.ds(n0, n), :, :, :], img.at[pl.ds(n0, n), :, :, :]) for n0, n in groups] + [(wp_hbm, wp), (pos_hbm, pos)]
    for i, v in enumerate((bp_hbm, g1_hbm, c1_hbm, bo_hbm, g2_hbm, c2_hbm, b2_hbm)):
        small.append((v, vecs.at[i]))
    small.append((b1_hbm, b1))
    small.append((bqkv_hbm.at[:, pl.ds(pl.multiple_of(core * 8, 8), 8), :], bqkv))
    small_copies = [pltpu.make_async_copy(s, d, in_sem.at[i]) for i, (s, d) in enumerate(small)]
    for i in (0, 2, 1) + tuple(range(3, len(small))):
        small_copies[i].start()
    wq_copies = [
        pltpu.make_async_copy(wqkv_hbm.at[pl.ds(pl.multiple_of(t * D + core * 512, 512), 512), :], wqkv.at[t], wqkv_sem.at[t])
        for t in range(3)]
    wo_copies = [
        pltpu.make_async_copy(wo_hbm.at[pl.ds(pl.multiple_of(((core + i) % 2) * 512, 512), 512), :], wo.at[i], wo_sem.at[i])
        for i in range(2)]
    w1_copies = [pltpu.make_async_copy(w1_hbm.at[:, pl.ds(i * W_FC1, W_FC1)], w1.at[i], w1_sem.at[i]) for i in range(N_FC1)]
    w2_copies = [pltpu.make_async_copy(w2_hbm.at[:, pl.ds(i * W_FC2, W_FC2)], w2.at[i], w2_sem.at[i]) for i in range(N_FC2)]

    rows128 = lax.broadcasted_iota(jnp.int32, (128, 256), 0)
    cols256 = lax.broadcasted_iota(jnp.int32, (128, 256), 1)
    diff = cols256 - rows128 % 16

    def build_sel(i, carry):
        sel[pl.ds(pl.multiple_of(i * 128, 128), 128), :] = jnp.where(diff == i * 16, 1.0, 0.0).astype(BF16)
        return carry
    lax.fori_loop(0, 16, build_sel, 0)

    keep = lax.broadcasted_iota(jnp.int32, (8, 128), 1) // 16 == lax.broadcasted_iota(jnp.int32, (8, 128), 0)

    def embed(group):
        n0, count = groups[group]
        m = count * BLOCK
        top = n0 * BLOCK * 3

        def spread(i, carry):
            for g in range(48):
                p, c = g // 3, g % 3
                t, col = g // 16, (g % 16) * 128
                for py in range(2):
                    row = img[n0 + i, c, pl.ds(py * 16 + p, 1), :]
                    halves = [jnp.where(keep, jnp.broadcast_to(row[:, j * 128:(j + 1) * 128], (8, 128)), 0.0) for j in range(2)]
                    at = pl.multiple_of(top + t * m + i * BLOCK + py * 16, 16)
                    lhs[pl.ds(at, 16), pl.ds(col, 128)] = jnp.concatenate(halves, axis=0).astype(BF16)
            return carry
        lax.fori_loop(0, count, spread, 0)
        h = 3 * m // 2
        both = [jnp.dot(lhs[top + i * h:top + (i + 1) * h, :], sel[...], preferred_element_type=F32).astype(BF16) for i in range(2)]
        rows = slice(n0 * BLOCK, n0 * BLOCK + m)
        pix[rows, 0:256] = both[0][0:m]
        pix[rows, 256:512] = jnp.concatenate([both[0][m:], both[1][0:m // 2]], axis=0)
        pix[rows, 512:768] = both[1][m // 2:]
        return rows, count

    def project(rows, count):
        for n in range(2):
            cols = slice(n * 512, (n + 1) * 512)
            emb = jnp.dot(pix[rows, :], wp[:, cols], preferred_element_type=F32) + bp_row[:, cols]
            emb = emb.reshape(count, BLOCK, 512) + pos[:, cols].astype(F32)[None]
            xs[rows, cols] = emb.reshape(count * BLOCK, 512).astype(BF16)

    slot1_first = {3: 8, 1: 10, 0: 12, 2: 13}

    def block(slot, k, other):
        first = 2 * k + other if slot == 0 else slot1_first[k] + other * (2 if k in (0, 2) else 1)
        return pl.ds(first * BLOCK, BLOCK)

    def x_block(chip_to, slot):
        image = chip_to if slot == 0 else 4 + chip_to // 2
        return pl.ds(pl.multiple_of(image * BLOCK, BLOCK), BLOCK)

    sends = []

    def start(copy):
        copy.start()
        sends.append(copy)

    def send_slot(slot):
        for k in (2, 1, 3):
            to = chip_at(k)
            start(remote(xs.at[x_block(to, slot), :], xg.at[block(slot, k, 0), :], xsend.at[k - 1, slot], xrecv.at[k - 1, slot], to * 2 + core))
        start(remote(xs.at[x_block(chip, slot), :], xg.at[block(slot, 0, 1), :], fsend.at[0, slot], frecv.at[0, slot], mate))
        xg[block(slot, 0, 0), :] = xs[x_block(chip, slot), :]

    small_copies[0].wait()
    part = embed(0)
    for c in small_copies[2:]:
        c.wait()
    small_copies[1].wait()
    for c in wq_copies + wo_copies + w1_copies + w2_copies:
        c.start()
    bp_row = as_row(vecs[0])
    project(*part)
    pl.semaphore_wait(barrier, 7)
    send_slot(1)
    project(*embed(1))
    send_slot(0)

    g1_row, c1_row = as_row(vecs[1]), as_row(vecs[2])

    def norm_blocks(blocks):
        for rows in blocks:
            y1[rows, :] = norm_rows(xg[rows, :].astype(F32), g1_row, c1_row).astype(BF16)

    def arrive(slot, k):
        ref = xg.at[block(slot, k, 0), :]
        remote(ref, ref, xsend.at[k - 1, slot], xrecv.at[k - 1, slot], chip_at(k) * 2 + core).wait_recv()
        start(remote(ref, xg.at[block(slot, k, 1), :], fsend.at[k, slot], frecv.at[k, slot], mate))

    def forwarded(slot, k):
        ref = xg.at[block(slot, k, 1), :]
        remote(ref, ref, fsend.at[k, slot], frecv.at[k, slot], mate).wait_recv()

    norm_blocks([block(1, 0, 0), block(0, 0, 0)])
    for slot in (1, 0):
        forwarded(slot, 0)
    norm_blocks([block(1, 0, 1), block(0, 0, 1)])
    for slot in (1, 0):
        for k in (2, 1):
            arrive(slot, k)
        norm_blocks([block(slot, k, 0) for k in (2, 1)])
    for c in wq_copies:
        c.wait()
    brow = [as_row(bqkv[t]) for t in range(3)]
    for slot in (1, 0):
        for k in (2, 1):
            forwarded(slot, k)
    norm_blocks([block(slot, k, 1) for slot in (1, 0) for k in (2, 1)])

    early_q, early_kv = ((0, 192), (384, 512)), ((0, 192), (320, 512))

    def heads_of(t, dst, pieces):
        rows = jnp.concatenate([y1[a:b, :] for a, b in pieces], axis=0)
        got = (lax.dot_general(rows, wqkv[t], NT, preferred_element_type=F32) + brow[t]).astype(BF16)
        at = 0
        for a, b in pieces:
            dst[a:b, :] = got[at:at + b - a]
            at += b - a

    heads_of(0, qh, early_q)
    heads_of(1, kh, early_kv)
    for slot in (1, 0):
        arrive(slot, 3)
    heads_of(2, vh, early_kv)
    norm_blocks([block(slot, 3, 0) for slot in (1, 0)])
    for slot in (1, 0):
        forwarded(slot, 3)
    norm_blocks([block(slot, 3, 1) for slot in (1, 0)])
    heads_of(0, qh, ((192, 256),))
    heads_of(1, kh, ((192, 320),))
    heads_of(2, vh, ((192, 320),))

    def attend(q0, rows, k0):
        low = lax.broadcasted_iota(jnp.int32, (rows, 128), 1) < 64
        for pair in range(4):
            cols = slice(pair * 128, (pair + 1) * 128)
            q_pair = qh[q0:q0 + rows, cols]
            k_pair = kh[k0:k0 + 256, cols]
            v_pair = vh[k0:k0 + 256, cols]
            heads = []
            for h in range(2):
                q_one = jnp.where(low == (h == 0), q_pair, jnp.zeros_like(q_pair))
                s = lax.dot_general(q_one, k_pair, NT, preferred_element_type=F32)
                e = jnp.exp2((s - jnp.max(s, axis=-1, keepdims=True)) * EXP_SCALE)
                w = (e * (1.0 / jnp.sum(e, axis=-1, keepdims=True))).astype(BF16)
                heads.append(jnp.dot(w, v_pair, preferred_element_type=F32))
            og[q0:q0 + rows, cols] = jnp.where(low, heads[0], heads[1]).astype(BF16)

    def o_home(k, other):
        dev = chip_at(k) * 2 + (core if other == 0 else 1 - core)
        return remote(og.at[block(0, k, other), :], oh.at[other, pl.ds(k * BLOCK, BLOCK), :],
                      hsend.at[k, other], hrecv.at[k, other], dev)

    o_mate = remote(og.at[pl.ds(448, 64), :], op, osend, orecv, mate)

    attend(128, 128, 0)
    for k in (3, 2):
        for other in range(2):
            start(o_home(k, other))
    attend(384, 128, 256)
    start(o_mate)
    attend(0, 128, 0)
    for k, other in ((1, 0), (1, 1), (0, 1)):
        start(o_home(k, other))

    for c in wo_copies + w1_copies + w2_copies:
        c.wait()
    bo_row, g2_row, c2_row, b2_row = [as_row(vecs[i]) for i in (3, 4, 5, 6)]
    for i in range(N_FC1):
        b1row[i] = as_row(b1[i * 4:(i + 1) * 4, :])

    def finish(m, x_in, near, far, ready):
        res[0:m, :] = x_in.astype(F32) + jnp.dot(near, wo[0], preferred_element_type=F32)
        ready()
        res[0:m, :] = res[0:m, :] + jnp.dot(far[...], wo[1], preferred_element_type=F32) + bo_row
        for i in range(m // BLOCK):
            rows = slice(i * BLOCK, (i + 1) * BLOCK)
            y2[rows, :] = norm_rows(res[rows, :], g2_row, c2_row).astype(BF16)

        def activate(i):
            hid[0:m, i * W_FC1:(i + 1) * W_FC1] = jax.nn.gelu(pre[i % 2, 0:m], approximate=True).astype(BF16)

        for i in range(N_FC1):
            pre[i % 2, 0:m] = jnp.dot(y2[0:m, :], w1[i], preferred_element_type=F32) + b1row[i]
            if i:
                activate(i - 1)
        activate(N_FC1 - 1)

    def second(m, j):
        cols = slice(j * W_FC2, (j + 1) * W_FC2)
        return (jnp.dot(hid[0:m, :], w2[j], preferred_element_type=F32) + (res[0:m, cols] + b2_row[:, cols])).astype(BF16)

    def shared_home(j, recv):
        other = chip_at(2)
        image = 4 + (other if recv else chip) // 2
        return remote(back.at[j], out.at[image, :, pl.ds(j * W_FC2, W_FC2)], rsend.at[j], rrecv.at[j], other * 2 + core)

    finish(64, xg[384:448, :], og[384:448, :], op, o_mate.wait_recv)
    for j in range(N_FC2):
        rows = second(64, j)
        back[j] = rows[BLOCK:]
        start(shared_home(j, False))
        out[4 + cy, :, j * W_FC2:(j + 1) * W_FC2] = rows[0:BLOCK]

    def home_ready():
        for k in range(4):
            o_home(k, 1).wait_recv()

    for k in (1, 2, 3):
        o_home(k, 0).wait_recv()
    finish(128, jnp.concatenate([xg[0:32, :]] + [xs[x_block(chip_at(k), 0), :] for k in (1, 2, 3)], axis=0),
           jnp.concatenate([og[0:32, :], oh[0, 32:128, :]], axis=0), oh.at[1], home_ready)
    for j in range(N_FC2):
        rows = second(128, j)
        for k in range(4):
            out[chip_at(k), :, j * W_FC2:(j + 1) * W_FC2] = rows[k * BLOCK:(k + 1) * BLOCK]

    for j in range(N_FC2):
        shared_home(j, True).wait_recv()
    for c in sends:
        c.wait_send()


def solution(mesh):
    def device_step(images, w_patch, b_patch, pos_embed, ln1_gain, ln1_bias, w_qkv, b_qkv, w_out, b_out, ln2_gain, ln2_bias, w_fc1, b_fc1, w_fc2, b_fc2):
        tile = lambda v: v.reshape(-1, 128)
        args = (
            jnp.transpose(images, (0, 3, 1, 2)),
            jnp.transpose(w_patch, (0, 2, 1, 3)).reshape(768, D),
            tile(b_patch), pos_embed, tile(ln1_gain), tile(ln1_bias),
            jnp.transpose(w_qkv, (1, 2, 3, 0)).reshape(3 * D, D),
            b_qkv, w_out.reshape(D, D), tile(b_out), tile(ln2_gain), tile(ln2_bias),
            w_fc1, tile(b_fc1), w_fc2, tile(b_fc2))
        vm = pltpu.VMEM
        dma = pltpu.SemaphoreType.DMA
        return pl.pallas_call(
            layer_kernel,
            out_shape=pltpu.VMEM((IMAGES, BLOCK, D), BF16),
            in_specs=[pl.BlockSpec(memory_space=pl.ANY)] * len(args),
            out_specs=pl.BlockSpec(memory_space=pltpu.VMEM),
            scratch_shapes=[
                vm((IMAGES, 3, BLOCK, 256), F32), vm((768, D), BF16), vm((BLOCK, D), BF16), vm((7, 8, 128), F32),
                vm((32, 128), F32), vm((3, 8, 64), F32), vm((3, 512, D), BF16), vm((2, 512, D), BF16),
                vm((N_FC1, D, W_FC1), BF16), vm((N_FC2, FF, W_FC2), BF16),
                vm((3 * OWN, 2048), BF16), vm((2048, 256), BF16), vm((OWN, 768), BF16), vm((OWN, D), BF16),
                vm((2 * TOKENS, D), BF16), vm((2 * TOKENS, D), BF16),
                vm((512, 512), BF16), vm((512, 512), BF16), vm((512, 512), BF16), vm((512, 512), BF16),
                vm((64, 512), BF16), vm((2, HALF, 512), BF16),
                vm((HALF, D), F32), vm((HALF, D), BF16), vm((HALF, FF), BF16), vm((N_FC2, BLOCK, W_FC2), BF16),
                vm((N_FC1, 1, W_FC1), F32), vm((2, HALF, W_FC1), F32),
                dma((13,)), dma((3,)), dma((2,)), dma((N_FC1,)), dma((N_FC2,)),
                dma((3, 2)), dma((3, 2)), dma((4, 2)), dma((4, 2)), dma, dma, dma((4, 2)), dma((4, 2)),
                dma((N_FC2,)), dma((N_FC2,)),
            ],
            compiler_params=pltpu.CompilerParams(
                collective_id=0, has_side_effects=True, vmem_limit_bytes=60 * 1024 * 1024),
        )(*args)

    in_specs = (P('dp', 'sp', None, None), P(), P(), P('sp', None), P(), P(), P(), P(), P(), P(), P(), P(), P(), P(), P(), P())
    return jax.shard_map(device_step, mesh=mesh, in_specs=in_specs, out_specs=P('dp', 'sp', None), check_vma=False)
```

```python
import functools
import math
import jax
import jax.numpy as jnp
from jax import lax
from jax.experimental import pallas as pl
from jax.experimental.pallas import tpu as pltpu
from jax.sharding import PartitionSpec as P

LN_EPS = 1e-6
F32 = jnp.float32
BF16 = jnp.bfloat16
D = 1024
FF = 4096
IMAGES = 6
BLOCK = 32
TOKENS = 256
OWN = 192
HALF = 128
N_FC1, W_FC1 = 8, 512
N_FC2, W_FC2 = 2, 512
EXP_SCALE = math.log2(math.e) / 8.0
MESH = pl.DeviceIdType.MESH
NT = (((1,), (1,)), ((), ()))


def as_row(vec):
    return jnp.concatenate([vec[i:i + 1, :] for i in range(vec.shape[0])], axis=1)


def norm_rows(x_in, gain, bias):
    centered = x_in - jnp.mean(x_in, axis=-1, keepdims=True)
    variance = jnp.mean(centered * centered, axis=-1, keepdims=True)
    return centered * lax.rsqrt(variance + LN_EPS) * gain + bias


def layer_kernel(
        img_hbm, wp_hbm, bp_hbm, pos_hbm, g1_hbm, c1_hbm, wqkv_hbm, bqkv_hbm, wo_hbm, bo_hbm, g2_hbm, c2_hbm,
        w1_hbm, b1_hbm, w2_hbm, b2_hbm,
        out,
        img, wp, pos, vecs, b1, bqkv, wqkv, wo, w1, w2,
        lhs, sel, pix, xs, xg, y1, qh, kh, vh, og, op, oh, res, y2, hid, back, b1row, pre,
        in_sem, wqkv_sem, wo_sem, w1_sem, w2_sem,
        xsend, xrecv, fsend, frecv, osend, orecv, hsend, hrecv, rsend, rrecv):
    dp = lax.axis_index("dp")
    me = lax.axis_index("sp")
    chip = me // 2
    core = me % 2
    mate = chip * 2 + (1 - core)
    cx = chip % 2
    cy = chip // 2

    def remote(src, dst, ssem, rsem, dev):
        return pltpu.make_async_remote_copy(
            src_ref=src, dst_ref=dst, send_sem=ssem, recv_sem=rsem, device_id=(dp, dev), device_id_type=MESH)

    def chip_at(k):
        return ((cy + k // 2) % 2) * 2 + (cx + k % 2) % 2

    barrier = pltpu.get_barrier_semaphore()
    for k in range(1, 8):
        pl.semaphore_signal(barrier, inc=1, device_id=(dp, (me + k) % 8), device_id_type=MESH)

    groups = ((4, 2), (0, 4))
    small = [(img_hbm.at[pl.ds(n0, n), :, :, :], img.at[pl.ds(n0, n), :, :, :]) for n0, n in groups] + [(wp_hbm, wp), (pos_hbm, pos)]
    for i, v in enumerate((bp_hbm, g1_hbm, c1_hbm, bo_hbm, g2_hbm, c2_hbm, b2_hbm)):
        small.append((v, vecs.at[i]))
    small.append((b1_hbm, b1))
    small.append((bqkv_hbm.at[:, pl.ds(pl.multiple_of(core * 8, 8), 8), :], bqkv))
    small_copies = [pltpu.make_async_copy(s, d, in_sem.at[i]) for i, (s, d) in enumerate(small)]
    for i in (0, 2, 1) + tuple(range(3, len(small))):
        small_copies[i].start()
    wq_copies = [
        pltpu.make_async_copy(wqkv_hbm.at[pl.ds(pl.multiple_of(t * D + core * 512, 512), 512), :], wqkv.at[t], wqkv_sem.at[t])
        for t in range(3)]
    wo_copies = [
        pltpu.make_async_copy(wo_hbm.at[pl.ds(pl.multiple_of(((core + i) % 2) * 512, 512), 512), :], wo.at[i], wo_sem.at[i])
        for i in range(2)]
    w1_copies = [pltpu.make_async_copy(w1_hbm.at[:, pl.ds(i * W_FC1, W_FC1)], w1.at[i], w1_sem.at[i]) for i in range(N_FC1)]
    w2_copies = [pltpu.make_async_copy(w2_hbm.at[:, pl.ds(i * W_FC2, W_FC2)], w2.at[i], w2_sem.at[i]) for i in range(N_FC2)]

    rows128 = lax.broadcasted_iota(jnp.int32, (128, 256), 0)
    cols256 = lax.broadcasted_iota(jnp.int32, (128, 256), 1)
    diff = cols256 - rows128 % 16

    def build_sel(i, carry):
        sel[pl.ds(pl.multiple_of(i * 128, 128), 128), :] = jnp.where(diff == i * 16, 1.0, 0.0).astype(BF16)
        return carry
    lax.fori_loop(0, 16, build_sel, 0)

    keep = lax.broadcasted_iota(jnp.int32, (8, 128), 1) // 16 == lax.broadcasted_iota(jnp.int32, (8, 128), 0)

    def embed(group):
        n0, count = groups[group]
        m = count * BLOCK
        top = n0 * BLOCK * 3

        def spread(i, carry):
            for g in range(48):
                p, c = g // 3, g % 3
                t, col = g // 16, (g % 16) * 128
                for py in range(2):
                    row = img[n0 + i, c, pl.ds(py * 16 + p, 1), :]
                    halves = [jnp.where(keep, jnp.broadcast_to(row[:, j * 128:(j + 1) * 128], (8, 128)), 0.0) for j in range(2)]
                    at = pl.multiple_of(top + t * m + i * BLOCK + py * 16, 16)
                    lhs[pl.ds(at, 16), pl.ds(col, 128)] = jnp.concatenate(halves, axis=0).astype(BF16)
            return carry
        lax.fori_loop(0, count, spread, 0)
        h = 3 * m // 2
        both = [jnp.dot(lhs[top + i * h:top + (i + 1) * h, :], sel[...], preferred_element_type=F32).astype(BF16) for i in range(2)]
        rows = slice(n0 * BLOCK, n0 * BLOCK + m)
        pix[rows, 0:256] = both[0][0:m]
        pix[rows, 256:512] = jnp.concatenate([both[0][m:], both[1][0:m // 2]], axis=0)
        pix[rows, 512:768] = both[1][m // 2:]
        return rows, count

    def project(rows, count):
        for n in range(2):
            cols = slice(n * 512, (n + 1) * 512)
            emb = jnp.dot(pix[rows, :], wp[:, cols], preferred_element_type=F32) + bp_row[:, cols]
            emb = emb.reshape(count, BLOCK, 512) + pos[:, cols].astype(F32)[None]
            xs[rows, cols] = emb.reshape(count * BLOCK, 512).astype(BF16)

    slot1_first = {3: 8, 1: 10, 0: 12, 2: 13}

    def block(slot, k, other):
        first = 2 * k + other if slot == 0 else slot1_first[k] + other * (2 if k in (0, 2) else 1)
        return pl.ds(first * BLOCK, BLOCK)

    def x_block(chip_to, slot):
        image = chip_to if slot == 0 else 4 + chip_to // 2
        return pl.ds(pl.multiple_of(image * BLOCK, BLOCK), BLOCK)

    sends = []

    def start(copy):
        copy.start()
        sends.append(copy)

    def send_slot(slot, where):
        for k in where:
            to = chip_at(k)
            start(remote(xs.at[x_block(to, slot), :], xg.at[block(slot, k, 0), :], xsend.at[k - 1, slot], xrecv.at[k - 1, slot], to * 2 + core))

    def share_own(slot):
        start(remote(xs.at[x_block(chip, slot), :], xg.at[block(slot, 0, 1), :], fsend.at[0, slot], frecv.at[0, slot], mate))
        xg[block(slot, 0, 0), :] = xs[x_block(chip, slot), :]

    small_copies[0].wait()
    part = embed(0)
    for c in small_copies[2:]:
        c.wait()
    small_copies[1].wait()
    for c in wq_copies + wo_copies + w1_copies + w2_copies:
        c.start()
    bp_row = as_row(vecs[0])
    project(*part)
    pl.semaphore_wait(barrier, 7)
    send_slot(1, (2, 1))
    share_own(1)
    project(*embed(1))
    send_slot(0, (2, 1))
    send_slot(1, (3,))
    send_slot(0, (3,))
    share_own(0)

    g1_row, c1_row = as_row(vecs[1]), as_row(vecs[2])

    def norm_blocks(blocks):
        for rows in blocks:
            y1[rows, :] = norm_rows(xg[rows, :].astype(F32), g1_row, c1_row).astype(BF16)

    def arrive(slot, k):
        ref = xg.at[block(slot, k, 0), :]
        remote(ref, ref, xsend.at[k - 1, slot], xrecv.at[k - 1, slot], chip_at(k) * 2 + core).wait_recv()
        start(remote(ref, xg.at[block(slot, k, 1), :], fsend.at[k, slot], frecv.at[k, slot], mate))

    def forwarded(slot, k):
        ref = xg.at[block(slot, k, 1), :]
        remote(ref, ref, fsend.at[k, slot], frecv.at[k, slot], mate).wait_recv()

    norm_blocks([block(1, 0, 0), block(0, 0, 0)])
    for slot in (1, 0):
        forwarded(slot, 0)
    norm_blocks([block(1, 0, 1), block(0, 0, 1)])
    for c in wq_copies:
        c.wait()
    brow = [as_row(bqkv[t]) for t in range(3)]

    def heads_of(t, dst, pieces):
        rows = jnp.concatenate([y1[a:b, :] for a, b in pieces], axis=0)
        got = (lax.dot_general(rows, wqkv[t], NT, preferred_element_type=F32) + brow[t]).astype(BF16)
        at = 0
        for a, b in pieces:
            dst[a:b, :] = got[at:at + b - a]
            at += b - a

    own = ((0, 64), (384, 416), (448, 480))
    heads_of(0, qh, own)
    heads_of(1, kh, own)
    heads_of(2, vh, own)

    for slot in (1, 0):
        for k in (2, 1):
            arrive(slot, k)
        norm_blocks([block(slot, k, 0) for k in (2, 1)])
    for slot in (1, 0):
        for k in (2, 1):
            forwarded(slot, k)
    norm_blocks([block(slot, k, 1) for slot in (1, 0) for k in (2, 1)])
    near_q = ((64, 192), (416, 448), (480, 512))
    near_kv = ((64, 192), (320, 384), (416, 448), (480, 512))
    heads_of(0, qh, near_q)
    heads_of(1, kh, near_kv)
    for slot in (1, 0):
        arrive(slot, 3)
    heads_of(2, vh, near_kv)
    norm_blocks([block(slot, 3, 0) for slot in (1, 0)])
    for slot in (1, 0):
        forwarded(slot, 3)
    norm_blocks([block(slot, 3, 1) for slot in (1, 0)])
    heads_of(0, qh, ((192, 256),))
    heads_of(1, kh, ((192, 320),))
    heads_of(2, vh, ((192, 320),))

    def attend(q0, rows, k0):
        low = lax.broadcasted_iota(jnp.int32, (rows, 128), 1) < 64
        for pair in range(4):
            cols = slice(pair * 128, (pair + 1) * 128)
            q_pair = qh[q0:q0 + rows, cols]
            k_pair = kh[k0:k0 + 256, cols]
            v_pair = vh[k0:k0 + 256, cols]
            heads = []
            for h in range(2):
                q_one = jnp.where(low == (h == 0), q_pair, jnp.zeros_like(q_pair))
                s = lax.dot_general(q_one, k_pair, NT, preferred_element_type=F32)
                e = jnp.exp2((s - jnp.max(s, axis=-1, keepdims=True)) * EXP_SCALE)
                w = (e * (1.0 / jnp.sum(e, axis=-1, keepdims=True))).astype(BF16)
                heads.append(jnp.dot(w, v_pair, preferred_element_type=F32))
            og[q0:q0 + rows, cols] = jnp.where(low, heads[0], heads[1]).astype(BF16)

    def o_home(k, other):
        dev = chip_at(k) * 2 + (core if other == 0 else 1 - core)
        return remote(og.at[block(0, k, other), :], oh.at[other, pl.ds(k * BLOCK, BLOCK), :],
                      hsend.at[k, other], hrecv.at[k, other], dev)

    o_mate = remote(og.at[pl.ds(448, 64), :], op, osend, orecv, mate)

    attend(128, 128, 0)
    for k in (3, 2):
        for other in range(2):
            start(o_home(k, other))
    attend(384, 128, 256)
    start(o_mate)
    attend(0, 128, 0)
    for k, other in ((1, 0), (1, 1), (0, 1)):
        start(o_home(k, other))

    for c in wo_copies + w1_copies + w2_copies:
        c.wait()
    bo_row, g2_row, c2_row, b2_row = [as_row(vecs[i]) for i in (3, 4, 5, 6)]
    for i in range(N_FC1):
        b1row[i] = as_row(b1[i * 4:(i + 1) * 4, :])

    def finish(m, x_in, near, far, ready):
        res[0:m, :] = x_in.astype(F32) + jnp.dot(near, wo[0], preferred_element_type=F32)
        ready()
        res[0:m, :] = res[0:m, :] + jnp.dot(far[...], wo[1], preferred_element_type=F32) + bo_row
        for i in range(m // BLOCK):
            rows = slice(i * BLOCK, (i + 1) * BLOCK)
            y2[rows, :] = norm_rows(res[rows, :], g2_row, c2_row).astype(BF16)

        def activate(i):
            hid[0:m, i * W_FC1:(i + 1) * W_FC1] = jax.nn.gelu(pre[i % 2, 0:m], approximate=True).astype(BF16)

        for i in range(N_FC1):
            pre[i % 2, 0:m] = jnp.dot(y2[0:m, :], w1[i], preferred_element_type=F32) + b1row[i]
            if i:
                activate(i - 1)
        activate(N_FC1 - 1)

    def second(m, j):
        cols = slice(j * W_FC2, (j + 1) * W_FC2)
        return (jnp.dot(hid[0:m, :], w2[j], preferred_element_type=F32) + (res[0:m, cols] + b2_row[:, cols])).astype(BF16)

    def shared_home(j, recv):
        other = chip_at(2)
        image = 4 + (other if recv else chip) // 2
        return remote(back.at[j], out.at[image, :, pl.ds(j * W_FC2, W_FC2)], rsend.at[j], rrecv.at[j], other * 2 + core)

    finish(64, xg[384:448, :], og[384:448, :], op, o_mate.wait_recv)
    for j in range(N_FC2):
        rows = second(64, j)
        back[j] = rows[BLOCK:]
        start(shared_home(j, False))
        out[4 + cy, :, j * W_FC2:(j + 1) * W_FC2] = rows[0:BLOCK]

    def home_ready():
        for k in range(4):
            o_home(k, 1).wait_recv()

    for k in (1, 2, 3):
        o_home(k, 0).wait_recv()
    finish(128, jnp.concatenate([xg[0:32, :]] + [xs[x_block(chip_at(k), 0), :] for k in (1, 2, 3)], axis=0),
           jnp.concatenate([og[0:32, :], oh[0, 32:128, :]], axis=0), oh.at[1], home_ready)
    for j in range(N_FC2):
        rows = second(128, j)
        for k in range(4):
            out[chip_at(k), :, j * W_FC2:(j + 1) * W_FC2] = rows[k * BLOCK:(k + 1) * BLOCK]

    for j in range(N_FC2):
        shared_home(j, True).wait_recv()
    for c in sends:
        c.wait_send()


def solution(mesh):
    def device_step(images, w_patch, b_patch, pos_embed, ln1_gain, ln1_bias, w_qkv, b_qkv, w_out, b_out, ln2_gain, ln2_bias, w_fc1, b_fc1, w_fc2, b_fc2):
        tile = lambda v: v.reshape(-1, 128)
        args = (
            jnp.transpose(images, (0, 3, 1, 2)),
            jnp.transpose(w_patch, (0, 2, 1, 3)).reshape(768, D),
            tile(b_patch), pos_embed, tile(ln1_gain), tile(ln1_bias),
            jnp.transpose(w_qkv, (1, 2, 3, 0)).reshape(3 * D, D),
            b_qkv, w_out.reshape(D, D), tile(b_out), tile(ln2_gain), tile(ln2_bias),
            w_fc1, tile(b_fc1), w_fc2, tile(b_fc2))
        vm = pltpu.VMEM
        dma = pltpu.SemaphoreType.DMA
        return pl.pallas_call(
            layer_kernel,
            out_shape=pltpu.VMEM((IMAGES, BLOCK, D), BF16),
            in_specs=[pl.BlockSpec(memory_space=pl.ANY)] * len(args),
            out_specs=pl.BlockSpec(memory_space=pltpu.VMEM),
            scratch_shapes=[
                vm((IMAGES, 3, BLOCK, 256), F32), vm((768, D), BF16), vm((BLOCK, D), BF16), vm((7, 8, 128), F32),
                vm((32, 128), F32), vm((3, 8, 64), F32), vm((3, 512, D), BF16), vm((2, 512, D), BF16),
                vm((N_FC1, D, W_FC1), BF16), vm((N_FC2, FF, W_FC2), BF16),
                vm((3 * OWN, 2048), BF16), vm((2048, 256), BF16), vm((OWN, 768), BF16), vm((OWN, D), BF16),
                vm((2 * TOKENS, D), BF16), vm((2 * TOKENS, D), BF16),
                vm((512, 512), BF16), vm((512, 512), BF16), vm((512, 512), BF16), vm((512, 512), BF16),
                vm((64, 512), BF16), vm((2, HALF, 512), BF16),
                vm((HALF, D), F32), vm((HALF, D), BF16), vm((HALF, FF), BF16), vm((N_FC2, BLOCK, W_FC2), BF16),
                vm((N_FC1, 1, W_FC1), F32), vm((2, HALF, W_FC1), F32),
                dma((13,)), dma((3,)), dma((2,)), dma((N_FC1,)), dma((N_FC2,)),
                dma((3, 2)), dma((3, 2)), dma((4, 2)), dma((4, 2)), dma, dma, dma((4, 2)), dma((4, 2)),
                dma((N_FC2,)), dma((N_FC2,)),
            ],
            compiler_params=pltpu.CompilerParams(
                collective_id=0, has_side_effects=True, vmem_limit_bytes=60 * 1024 * 1024),
        )(*args)

    in_specs = (P('dp', 'sp', None, None), P(), P(), P('sp', None), P(), P(), P(), P(), P(), P(), P(), P(), P(), P(), P(), P())
    return jax.shard_map(device_step, mesh=mesh, in_specs=in_specs, out_specs=P('dp', 'sp', None), check_vma=False)
```

```python
import functools
import math
import jax
import jax.numpy as jnp
from jax import lax
from jax.experimental import pallas as pl
from jax.experimental.pallas import tpu as pltpu
from jax.sharding import PartitionSpec as P

LN_EPS = 1e-6
F32 = jnp.float32
BF16 = jnp.bfloat16
D = 1024
FF = 4096
IMAGES = 6
BLOCK = 32
TOKENS = 256
OWN = 192
HALF = 128
N_FC1, W_FC1 = 8, 512
N_FC2, W_FC2 = 2, 512
EXP_SCALE = math.log2(math.e) / 8.0
MESH = pl.DeviceIdType.MESH
NT = (((1,), (1,)), ((), ()))


def as_row(vec):
    return jnp.concatenate([vec[i:i + 1, :] for i in range(vec.shape[0])], axis=1)


def norm_rows(x_in, gain, bias):
    centered = x_in - jnp.mean(x_in, axis=-1, keepdims=True)
    variance = jnp.mean(centered * centered, axis=-1, keepdims=True)
    return centered * lax.rsqrt(variance + LN_EPS) * gain + bias


def layer_kernel(
        img_hbm, wp_hbm, bp_hbm, pos_hbm, g1_hbm, c1_hbm, wqkv_hbm, bqkv_hbm, wo_hbm, bo_hbm, g2_hbm, c2_hbm,
        w1_hbm, b1_hbm, w2_hbm, b2_hbm,
        out,
        img, wp, pos, vecs, b1, bqkv, wqkv, wo, w1, w2,
        lhs, sel, pix, xs, xg, y1, qh, kh, vh, og, op, oh, res, y2, hid, back, b1row, pre,
        in_sem, wqkv_sem, wo_sem, w1_sem, w2_sem,
        xsend, xrecv, fsend, frecv, osend, orecv, hsend, hrecv, rsend, rrecv):
    dp = lax.axis_index("dp")
    me = lax.axis_index("sp")
    chip = me // 2
    core = me % 2
    mate = chip * 2 + (1 - core)
    cx = chip % 2
    cy = chip // 2

    def remote(src, dst, ssem, rsem, dev):
        return pltpu.make_async_remote_copy(
            src_ref=src, dst_ref=dst, send_sem=ssem, recv_sem=rsem, device_id=(dp, dev), device_id_type=MESH)

    def chip_at(k):
        return ((cy + k // 2) % 2) * 2 + (cx + k % 2) % 2

    barrier = pltpu.get_barrier_semaphore()
    for k in range(1, 8):
        pl.semaphore_signal(barrier, inc=1, device_id=(dp, (me + k) % 8), device_id_type=MESH)

    groups = ((4, 2), (0, 4))
    small = [(img_hbm.at[pl.ds(n0, n), :, :, :], img.at[pl.ds(n0, n), :, :, :]) for n0, n in groups] + [(wp_hbm, wp), (pos_hbm, pos)]
    for i, v in enumerate((bp_hbm, g1_hbm, c1_hbm, bo_hbm, g2_hbm, c2_hbm, b2_hbm)):
        small.append((v, vecs.at[i]))
    small.append((b1_hbm, b1))
    small.append((bqkv_hbm.at[:, pl.ds(pl.multiple_of(core * 8, 8), 8), :], bqkv))
    small_copies = [pltpu.make_async_copy(s, d, in_sem.at[i]) for i, (s, d) in enumerate(small)]
    for i in (0, 2, 1) + tuple(range(3, len(small))):
        small_copies[i].start()
    wq_copies = [
        pltpu.make_async_copy(wqkv_hbm.at[pl.ds(pl.multiple_of(t * D + core * 512, 512), 512), :], wqkv.at[t], wqkv_sem.at[t])
        for t in range(3)]
    wo_copies = [
        pltpu.make_async_copy(wo_hbm.at[pl.ds(pl.multiple_of(((core + i) % 2) * 512, 512), 512), :], wo.at[i], wo_sem.at[i])
        for i in range(2)]
    w1_copies = [pltpu.make_async_copy(w1_hbm.at[:, pl.ds(i * W_FC1, W_FC1)], w1.at[i], w1_sem.at[i]) for i in range(N_FC1)]
    w2_copies = [pltpu.make_async_copy(w2_hbm.at[:, pl.ds(i * W_FC2, W_FC2)], w2.at[i], w2_sem.at[i]) for i in range(N_FC2)]

    rows128 = lax.broadcasted_iota(jnp.int32, (128, 256), 0)
    cols256 = lax.broadcasted_iota(jnp.int32, (128, 256), 1)
    diff = cols256 - rows128 % 16

    def build_sel(i, carry):
        sel[pl.ds(pl.multiple_of(i * 128, 128), 128), :] = jnp.where(diff == i * 16, 1.0, 0.0).astype(BF16)
        return carry
    lax.fori_loop(0, 16, build_sel, 0)

    keep = lax.broadcasted_iota(jnp.int32, (8, 128), 1) // 16 == lax.broadcasted_iota(jnp.int32, (8, 128), 0)

    def embed(group):
        n0, count = groups[group]
        m = count * BLOCK
        top = n0 * BLOCK * 3

        def spread(i, carry):
            for g in range(48):
                p, c = g // 3, g % 3
                t, col = g // 16, (g % 16) * 128
                for py in range(2):
                    row = img[n0 + i, c, pl.ds(py * 16 + p, 1), :]
                    halves = [jnp.where(keep, jnp.broadcast_to(row[:, j * 128:(j + 1) * 128], (8, 128)), 0.0) for j in range(2)]
                    at = pl.multiple_of(top + t * m + i * BLOCK + py * 16, 16)
                    lhs[pl.ds(at, 16), pl.ds(col, 128)] = jnp.concatenate(halves, axis=0).astype(BF16)
            return carry
        lax.fori_loop(0, count, spread, 0)
        h = 3 * m // 2
        both = [jnp.dot(lhs[top + i * h:top + (i + 1) * h, :], sel[...], preferred_element_type=F32).astype(BF16) for i in range(2)]
        rows = slice(n0 * BLOCK, n0 * BLOCK + m)
        pix[rows, 0:256] = both[0][0:m]
        pix[rows, 256:512] = jnp.concatenate([both[0][m:], both[1][0:m // 2]], axis=0)
        pix[rows, 512:768] = both[1][m // 2:]
        return rows, count

    def project(rows, count):
        for n in range(2):
            cols = slice(n * 512, (n + 1) * 512)
            emb = jnp.dot(pix[rows, :], wp[:, cols], preferred_element_type=F32) + bp_row[:, cols]
            emb = emb.reshape(count, BLOCK, 512) + pos[:, cols].astype(F32)[None]
            xs[rows, cols] = emb.reshape(count * BLOCK, 512).astype(BF16)

    slot1_first = {3: 8, 1: 10, 0: 12, 2: 13}

    def block(slot, k, other):
        first = 2 * k + other if slot == 0 else slot1_first[k] + other * (2 if k in (0, 2) else 1)
        return pl.ds(first * BLOCK, BLOCK)

    def x_block(chip_to, slot):
        image = chip_to if slot == 0 else 4 + chip_to // 2
        return pl.ds(pl.multiple_of(image * BLOCK, BLOCK), BLOCK)

    sends = []

    def start(copy):
        copy.start()
        sends.append(copy)

    def send_slot(slot):
        for k in (2, 1, 3):
            to = chip_at(k)
            start(remote(xs.at[x_block(to, slot), :], xg.at[block(slot, k, 0), :], xsend.at[k - 1, slot], xrecv.at[k - 1, slot], to * 2 + core))
        start(remote(xs.at[x_block(chip, slot), :], xg.at[block(slot, 0, 1), :], fsend.at[0, slot], frecv.at[0, slot], mate))
        xg[block(slot, 0, 0), :] = xs[x_block(chip, slot), :]

    small_copies[0].wait()
    part = embed(0)
    for c in small_copies[2:]:
        c.wait()
    small_copies[1].wait()
    for c in wq_copies + wo_copies + w1_copies + w2_copies:
        c.start()
    bp_row = as_row(vecs[0])
    project(*part)
    pl.semaphore_wait(barrier, 7)
    send_slot(1)
    project(*embed(1))
    send_slot(0)

    g1_row, c1_row = as_row(vecs[1]), as_row(vecs[2])

    def norm_blocks(blocks):
        for rows in blocks:
            y1[rows, :] = norm_rows(xg[rows, :].astype(F32), g1_row, c1_row).astype(BF16)

    def arrive(slot, k):
        ref = xg.at[block(slot, k, 0), :]
        remote(ref, ref, xsend.at[k - 1, slot], xrecv.at[k - 1, slot], chip_at(k) * 2 + core).wait_recv()
        start(remote(ref, xg.at[block(slot, k, 1), :], fsend.at[k, slot], frecv.at[k, slot], mate))

    def forwarded(slot, k):
        ref = xg.at[block(slot, k, 1), :]
        remote(ref, ref, fsend.at[k, slot], frecv.at[k, slot], mate).wait_recv()

    norm_blocks([block(1, 0, 0), block(0, 0, 0)])
    for slot in (1, 0):
        forwarded(slot, 0)
    norm_blocks([block(1, 0, 1), block(0, 0, 1)])
    for c in wq_copies:
        c.wait()
    brow = [as_row(bqkv[t]) for t in range(3)]

    def heads_of(t, dst, a, b):
        dst[a:b, :] = (lax.dot_general(y1[a:b, :], wqkv[t], NT, preferred_element_type=F32) + brow[t]).astype(BF16)

    def attend(q0, rows, k0):
        low = lax.broadcasted_iota(jnp.int32, (rows, 128), 1) < 64
        for pair in range(4):
            cols = slice(pair * 128, (pair + 1) * 128)
            q_pair = qh[q0:q0 + rows, cols]
            k_pair = kh[k0:k0 + 256, cols]
            v_pair = vh[k0:k0 + 256, cols]
            heads = []
            for h in range(2):
                q_one = jnp.where(low == (h == 0), q_pair, jnp.zeros_like(q_pair))
                s = lax.dot_general(q_one, k_pair, NT, preferred_element_type=F32)
                e = jnp.exp2((s - jnp.max(s, axis=-1, keepdims=True)) * EXP_SCALE)
                w = (e * (1.0 / jnp.sum(e, axis=-1, keepdims=True))).astype(BF16)
                heads.append(jnp.dot(w, v_pair, preferred_element_type=F32))
            og[q0:q0 + rows, cols] = jnp.where(low, heads[0], heads[1]).astype(BF16)

    o_mate = remote(og.at[pl.ds(448, 64), :], op, osend, orecv, mate)

    for k in (2, 1):
        arrive(1, k)
    norm_blocks([block(1, k, 0) for k in (2, 1)])
    for k in (2, 1):
        forwarded(1, k)
    norm_blocks([block(1, k, 1) for k in (2, 1)])
    arrive(1, 3)
    norm_blocks([block(1, 3, 0)])
    for k in (2, 1):
        arrive(0, k)
    norm_blocks([block(0, k, 0) for k in (2, 1)])
    forwarded(1, 3)
    norm_blocks([block(1, 3, 1)])
    heads_of(0, qh, 384, 512)
    heads_of(1, kh, 256, 512)
    heads_of(2, vh, 256, 512)
    for k in (2, 1):
        forwarded(0, k)
    norm_blocks([block(0, k, 1) for k in (2, 1)])
    attend(384, 128, 256)
    start(o_mate)

    arrive(0, 3)
    for t, dst in ((0, qh), (1, kh), (2, vh)):
        heads_of(t, dst, 0, 192)
    norm_blocks([block(0, 3, 0)])
    forwarded(0, 3)
    norm_blocks([block(0, 3, 1)])
    for t, dst in ((0, qh), (1, kh), (2, vh)):
        heads_of(t, dst, 192, 256)

    def o_home(k, other):
        dev = chip_at(k) * 2 + (core if other == 0 else 1 - core)
        return remote(og.at[block(0, k, other), :], oh.at[other, pl.ds(k * BLOCK, BLOCK), :],
                      hsend.at[k, other], hrecv.at[k, other], dev)

    attend(128, 128, 0)
    for k in (3, 2):
        for other in range(2):
            start(o_home(k, other))
    attend(0, 128, 0)
    for k, other in ((1, 0), (1, 1), (0, 1)):
        start(o_home(k, other))

    for c in wo_copies + w1_copies + w2_copies:
        c.wait()
    bo_row, g2_row, c2_row, b2_row = [as_row(vecs[i]) for i in (3, 4, 5, 6)]
    for i in range(N_FC1):
        b1row[i] = as_row(b1[i * 4:(i + 1) * 4, :])

    def finish(m, x_in, near, far, ready):
        res[0:m, :] = x_in.astype(F32) + jnp.dot(near, wo[0], preferred_element_type=F32)
        ready()
        res[0:m, :] = res[0:m, :] + jnp.dot(far[...], wo[1], preferred_element_type=F32) + bo_row
        for i in range(m // BLOCK):
            rows = slice(i * BLOCK, (i + 1) * BLOCK)
            y2[rows, :] = norm_rows(res[rows, :], g2_row, c2_row).astype(BF16)

        def activate(i):
            hid[0:m, i * W_FC1:(i + 1) * W_FC1] = jax.nn.gelu(pre[i % 2, 0:m], approximate=True).astype(BF16)

        for i in range(N_FC1):
            pre[i % 2, 0:m] = jnp.dot(y2[0:m, :], w1[i], preferred_element_type=F32) + b1row[i]
            if i:
                activate(i - 1)
        activate(N_FC1 - 1)

    def second(m, j):
        cols = slice(j * W_FC2, (j + 1) * W_FC2)
        return (jnp.dot(hid[0:m, :], w2[j], preferred_element_type=F32) + (res[0:m, cols] + b2_row[:, cols])).astype(BF16)

    def shared_home(j, recv):
        other = chip_at(2)
        image = 4 + (other if recv else chip) // 2
        return remote(back.at[j], out.at[image, :, pl.ds(j * W_FC2, W_FC2)], rsend.at[j], rrecv.at[j], other * 2 + core)

    finish(64, xg[384:448, :], og[384:448, :], op, o_mate.wait_recv)
    for j in range(N_FC2):
        rows = second(64, j)
        back[j] = rows[BLOCK:]
        start(shared_home(j, False))
        out[4 + cy, :, j * W_FC2:(j + 1) * W_FC2] = rows[0:BLOCK]

    def home_ready():
        for k in range(4):
            o_home(k, 1).wait_recv()

    for k in (1, 2, 3):
        o_home(k, 0).wait_recv()
    finish(128, jnp.concatenate([xg[0:32, :]] + [xs[x_block(chip_at(k), 0), :] for k in (1, 2, 3)], axis=0),
           jnp.concatenate([og[0:32, :], oh[0, 32:128, :]], axis=0), oh.at[1], home_ready)
    for j in range(N_FC2):
        rows = second(128, j)
        for k in range(4):
            out[chip_at(k), :, j * W_FC2:(j + 1) * W_FC2] = rows[k * BLOCK:(k + 1) * BLOCK]

    for j in range(N_FC2):
        shared_home(j, True).wait_recv()
    for c in sends:
        c.wait_send()


def solution(mesh):
    def device_step(images, w_patch, b_patch, pos_embed, ln1_gain, ln1_bias, w_qkv, b_qkv, w_out, b_out, ln2_gain, ln2_bias, w_fc1, b_fc1, w_fc2, b_fc2):
        tile = lambda v: v.reshape(-1, 128)
        args = (
            jnp.transpose(images, (0, 3, 1, 2)),
            jnp.transpose(w_patch, (0, 2, 1, 3)).reshape(768, D),
            tile(b_patch), pos_embed, tile(ln1_gain), tile(ln1_bias),
            jnp.transpose(w_qkv, (1, 2, 3, 0)).reshape(3 * D, D),
            b_qkv, w_out.reshape(D, D), tile(b_out), tile(ln2_gain), tile(ln2_bias),
            w_fc1, tile(b_fc1), w_fc2, tile(b_fc2))
        vm = pltpu.VMEM
        dma = pltpu.SemaphoreType.DMA
        return pl.pallas_call(
            layer_kernel,
            out_shape=pltpu.VMEM((IMAGES, BLOCK, D), BF16),
            in_specs=[pl.BlockSpec(memory_space=pl.ANY)] * len(args),
            out_specs=pl.BlockSpec(memory_space=pltpu.VMEM),
            scratch_shapes=[
                vm((IMAGES, 3, BLOCK, 256), F32), vm((768, D), BF16), vm((BLOCK, D), BF16), vm((7, 8, 128), F32),
                vm((32, 128), F32), vm((3, 8, 64), F32), vm((3, 512, D), BF16), vm((2, 512, D), BF16),
                vm((N_FC1, D, W_FC1), BF16), vm((N_FC2, FF, W_FC2), BF16),
                vm((3 * OWN, 2048), BF16), vm((2048, 256), BF16), vm((OWN, 768), BF16), vm((OWN, D), BF16),
                vm((2 * TOKENS, D), BF16), vm((2 * TOKENS, D), BF16),
                vm((512, 512), BF16), vm((512, 512), BF16), vm((512, 512), BF16), vm((512, 512), BF16),
                vm((64, 512), BF16), vm((2, HALF, 512), BF16),
                vm((HALF, D), F32), vm((HALF, D), BF16), vm((HALF, FF), BF16), vm((N_FC2, BLOCK, W_FC2), BF16),
                vm((N_FC1, 1, W_FC1), F32), vm((2, HALF, W_FC1), F32),
                dma((13,)), dma((3,)), dma((2,)), dma((N_FC1,)), dma((N_FC2,)),
                dma((3, 2)), dma((3, 2)), dma((4, 2)), dma((4, 2)), dma, dma, dma((4, 2)), dma((4, 2)),
                dma((N_FC2,)), dma((N_FC2,)),
            ],
            compiler_params=pltpu.CompilerParams(
                collective_id=0, has_side_effects=True, vmem_limit_bytes=60 * 1024 * 1024),
        )(*args)

    in_specs = (P('dp', 'sp', None, None), P(), P(), P('sp', None), P(), P(), P(), P(), P(), P(), P(), P(), P(), P(), P(), P())
    return jax.shard_map(device_step, mesh=mesh, in_specs=in_specs, out_specs=P('dp', 'sp', None), check_vma=False)
```

```python
import functools
import math
import jax
import jax.numpy as jnp
from jax import lax
from jax.experimental import pallas as pl
from jax.experimental.pallas import tpu as pltpu
from jax.sharding import PartitionSpec as P

LN_EPS = 1e-6
F32 = jnp.float32
BF16 = jnp.bfloat16
D = 1024
FF = 4096
IMAGES = 6
BLOCK = 32
TOKENS = 256
OWN = 192
HALF = 128
N_FC1, W_FC1 = 8, 512
N_FC2, W_FC2 = 2, 512
EXP_SCALE = math.log2(math.e) / 8.0
MESH = pl.DeviceIdType.MESH
NT = (((1,), (1,)), ((), ()))


def as_row(vec):
    return jnp.concatenate([vec[i:i + 1, :] for i in range(vec.shape[0])], axis=1)


def norm_rows(x_in, gain, bias):
    centered = x_in - jnp.mean(x_in, axis=-1, keepdims=True)
    variance = jnp.mean(centered * centered, axis=-1, keepdims=True)
    return centered * lax.rsqrt(variance + LN_EPS) * gain + bias


def layer_kernel(
        img_hbm, wp_hbm, bp_hbm, pos_hbm, g1_hbm, c1_hbm, wqkv_hbm, bqkv_hbm, wo_hbm, bo_hbm, g2_hbm, c2_hbm,
        w1_hbm, b1_hbm, w2_hbm, b2_hbm,
        out,
        img, wp, pos, vecs, b1, bqkv, wqkv, wo, w1, w2,
        lhs, sel, pix, xs, xg, y1, qh, kh, vh, og, op, oh, res, y2, hid, back, b1row, pre,
        in_sem, wqkv_sem, wo_sem, w1_sem, w2_sem,
        xsend, xrecv, fsend, frecv, osend, orecv, hsend, hrecv, rsend, rrecv):
    dp = lax.axis_index("dp")
    me = lax.axis_index("sp")
    chip = me // 2
    core = me % 2
    mate = chip * 2 + (1 - core)
    cx = chip % 2
    cy = chip // 2

    def remote(src, dst, ssem, rsem, dev):
        return pltpu.make_async_remote_copy(
            src_ref=src, dst_ref=dst, send_sem=ssem, recv_sem=rsem, device_id=(dp, dev), device_id_type=MESH)

    def chip_at(k):
        return ((cy + k // 2) % 2) * 2 + (cx + k % 2) % 2

    barrier = pltpu.get_barrier_semaphore()
    for k in range(1, 8):
        pl.semaphore_signal(barrier, inc=1, device_id=(dp, (me + k) % 8), device_id_type=MESH)

    groups = ((4, 2), (0, 4))
    small = [(img_hbm.at[pl.ds(n0, n), :, :, :], img.at[pl.ds(n0, n), :, :, :]) for n0, n in groups] + [(wp_hbm, wp), (pos_hbm, pos)]
    for i, v in enumerate((bp_hbm, g1_hbm, c1_hbm, bo_hbm, g2_hbm, c2_hbm, b2_hbm)):
        small.append((v, vecs.at[i]))
    small.append((b1_hbm, b1))
    small.append((bqkv_hbm.at[:, pl.ds(pl.multiple_of(core * 8, 8), 8), :], bqkv))
    small_copies = [pltpu.make_async_copy(s, d, in_sem.at[i]) for i, (s, d) in enumerate(small)]
    for i in (0, 2, 1) + tuple(range(3, len(small))):
        small_copies[i].start()
    wq_copies = [
        pltpu.make_async_copy(wqkv_hbm.at[pl.ds(pl.multiple_of(t * D + core * 512, 512), 512), :], wqkv.at[t], wqkv_sem.at[t])
        for t in range(3)]
    wo_copies = [
        pltpu.make_async_copy(wo_hbm.at[pl.ds(pl.multiple_of(((core + i) % 2) * 512, 512), 512), :], wo.at[i], wo_sem.at[i])
        for i in range(2)]
    w1_copies = [pltpu.make_async_copy(w1_hbm.at[:, pl.ds(i * W_FC1, W_FC1)], w1.at[i], w1_sem.at[i]) for i in range(N_FC1)]
    w2_copies = [pltpu.make_async_copy(w2_hbm.at[:, pl.ds(i * W_FC2, W_FC2)], w2.at[i], w2_sem.at[i]) for i in range(N_FC2)]

    rows128 = lax.broadcasted_iota(jnp.int32, (128, 256), 0)
    cols256 = lax.broadcasted_iota(jnp.int32, (128, 256), 1)
    diff = cols256 - rows128 % 16

    def build_sel(i, carry):
        sel[pl.ds(pl.multiple_of(i * 128, 128), 128), :] = jnp.where(diff == i * 16, 1.0, 0.0).astype(BF16)
        return carry
    lax.fori_loop(0, 16, build_sel, 0)

    keep = lax.broadcasted_iota(jnp.int32, (8, 128), 1) // 16 == lax.broadcasted_iota(jnp.int32, (8, 128), 0)

    def embed(group):
        n0, count = groups[group]
        m = count * BLOCK
        top = n0 * BLOCK * 3

        def spread(i, carry):
            for g in range(48):
                p, c = g // 3, g % 3
                t, col = g // 16, (g % 16) * 128
                for py in range(2):
                    row = img[n0 + i, c, pl.ds(py * 16 + p, 1), :]
                    halves = [jnp.where(keep, jnp.broadcast_to(row[:, j * 128:(j + 1) * 128], (8, 128)), 0.0) for j in range(2)]
                    at = pl.multiple_of(top + t * m + i * BLOCK + py * 16, 16)
                    lhs[pl.ds(at, 16), pl.ds(col, 128)] = jnp.concatenate(halves, axis=0).astype(BF16)
            return carry
        lax.fori_loop(0, count, spread, 0)
        h = 3 * m // 2
        both = [jnp.dot(lhs[top + i * h:top + (i + 1) * h, :], sel[...], preferred_element_type=F32).astype(BF16) for i in range(2)]
        rows = slice(n0 * BLOCK, n0 * BLOCK + m)
        pix[rows, 0:256] = both[0][0:m]
        pix[rows, 256:512] = jnp.concatenate([both[0][m:], both[1][0:m // 2]], axis=0)
        pix[rows, 512:768] = both[1][m // 2:]
        return rows, count

    def project(rows, count):
        for n in range(2):
            cols = slice(n * 512, (n + 1) * 512)
            emb = jnp.dot(pix[rows, :], wp[:, cols], preferred_element_type=F32) + bp_row[:, cols]
            emb = emb.reshape(count, BLOCK, 512) + pos[:, cols].astype(F32)[None]
            xs[rows, cols] = emb.reshape(count * BLOCK, 512).astype(BF16)

    slot1_first = {3: 8, 1: 10, 0: 12, 2: 13}

    def block(slot, k, other):
        first = 2 * k + other if slot == 0 else slot1_first[k] + other * (2 if k in (0, 2) else 1)
        return pl.ds(first * BLOCK, BLOCK)

    def x_block(chip_to, slot):
        image = chip_to if slot == 0 else 4 + chip_to // 2
        return pl.ds(pl.multiple_of(image * BLOCK, BLOCK), BLOCK)

    sends = []

    def start(copy):
        copy.start()
        sends.append(copy)

    def send_slot(slot):
        for k in (2, 1, 3):
            to = chip_at(k)
            start(remote(xs.at[x_block(to, slot), :], xg.at[block(slot, k, 0), :], xsend.at[k - 1, slot], xrecv.at[k - 1, slot], to * 2 + core))
        start(remote(xs.at[x_block(chip, slot), :], xg.at[block(slot, 0, 1), :], fsend.at[0, slot], frecv.at[0, slot], mate))
        xg[block(slot, 0, 0), :] = xs[x_block(chip, slot), :]

    small_copies[0].wait()
    for c in wq_copies:
        c.start()
    part = embed(0)
    for c in small_copies[2:]:
        c.wait()
    small_copies[1].wait()
    bp_row = as_row(vecs[0])
    project(*part)
    pl.semaphore_wait(barrier, 7)
    send_slot(1)
    project(*embed(1))
    send_slot(0)
    for c in wo_copies + w1_copies + w2_copies:
        c.start()

    g1_row, c1_row = as_row(vecs[1]), as_row(vecs[2])

    def norm_blocks(blocks):
        for rows in blocks:
            y1[rows, :] = norm_rows(xg[rows, :].astype(F32), g1_row, c1_row).astype(BF16)

    def arrive(slot, k):
        ref = xg.at[block(slot, k, 0), :]
        remote(ref, ref, xsend.at[k - 1, slot], xrecv.at[k - 1, slot], chip_at(k) * 2 + core).wait_recv()
        start(remote(ref, xg.at[block(slot, k, 1), :], fsend.at[k, slot], frecv.at[k, slot], mate))

    def forwarded(slot, k):
        ref = xg.at[block(slot, k, 1), :]
        remote(ref, ref, fsend.at[k, slot], frecv.at[k, slot], mate).wait_recv()

    norm_blocks([block(1, 0, 0), block(0, 0, 0)])
    for slot in (1, 0):
        forwarded(slot, 0)
    norm_blocks([block(1, 0, 1), block(0, 0, 1)])
    brow = [as_row(bqkv[t]) for t in range(3)]

    def heads_of(t, dst, a, b):
        dst[a:b, :] = (lax.dot_general(y1[a:b, :], wqkv[t], NT, preferred_element_type=F32) + brow[t]).astype(BF16)

    def attend(q0, rows, k0):
        low = lax.broadcasted_iota(jnp.int32, (rows, 128), 1) < 64
        for pair in range(4):
            cols = slice(pair * 128, (pair + 1) * 128)
            q_pair = qh[q0:q0 + rows, cols]
            k_pair = kh[k0:k0 + 256, cols]
            v_pair = vh[k0:k0 + 256, cols]
            heads = []
            for h in range(2):
                q_one = jnp.where(low == (h == 0), q_pair, jnp.zeros_like(q_pair))
                s = lax.dot_general(q_one, k_pair, NT, preferred_element_type=F32)
                e = jnp.exp2((s - jnp.max(s, axis=-1, keepdims=True)) * EXP_SCALE)
                w = (e * (1.0 / jnp.sum(e, axis=-1, keepdims=True))).astype(BF16)
                heads.append(jnp.dot(w, v_pair, preferred_element_type=F32))
            og[q0:q0 + rows, cols] = jnp.where(low, heads[0], heads[1]).astype(BF16)

    o_mate = remote(og.at[pl.ds(448, 64), :], op, osend, orecv, mate)

    for k in (2, 1):
        arrive(1, k)
    norm_blocks([block(1, k, 0) for k in (2, 1)])
    for k in (2, 1):
        forwarded(1, k)
    norm_blocks([block(1, k, 1) for k in (2, 1)])
    arrive(1, 3)
    norm_blocks([block(1, 3, 0)])
    for k in (2, 1):
        arrive(0, k)
    norm_blocks([block(0, k, 0) for k in (2, 1)])
    forwarded(1, 3)
    norm_blocks([block(1, 3, 1)])
    for c in wq_copies:
        c.wait()
    heads_of(0, qh, 384, 512)
    heads_of(1, kh, 256, 512)
    heads_of(2, vh, 256, 512)
    for k in (2, 1):
        forwarded(0, k)
    norm_blocks([block(0, k, 1) for k in (2, 1)])
    attend(384, 128, 256)
    start(o_mate)

    arrive(0, 3)
    for t, dst in ((0, qh), (1, kh), (2, vh)):
        heads_of(t, dst, 0, 192)
    norm_blocks([block(0, 3, 0)])
    forwarded(0, 3)
    norm_blocks([block(0, 3, 1)])
    for t, dst in ((0, qh), (1, kh), (2, vh)):
        heads_of(t, dst, 192, 256)

    def o_home(k, other):
        dev = chip_at(k) * 2 + (core if other == 0 else 1 - core)
        return remote(og.at[block(0, k, other), :], oh.at[other, pl.ds(k * BLOCK, BLOCK), :],
                      hsend.at[k, other], hrecv.at[k, other], dev)

    attend(128, 128, 0)
    for k in (3, 2):
        for other in range(2):
            start(o_home(k, other))
    attend(0, 128, 0)
    for k, other in ((1, 0), (1, 1), (0, 1)):
        start(o_home(k, other))

    for c in wo_copies + w1_copies + w2_copies:
        c.wait()
    bo_row, g2_row, c2_row, b2_row = [as_row(vecs[i]) for i in (3, 4, 5, 6)]
    for i in range(N_FC1):
        b1row[i] = as_row(b1[i * 4:(i + 1) * 4, :])

    def finish(m, x_in, near, far, ready):
        res[0:m, :] = x_in.astype(F32) + jnp.dot(near, wo[0], preferred_element_type=F32)
        ready()
        res[0:m, :] = res[0:m, :] + jnp.dot(far[...], wo[1], preferred_element_type=F32) + bo_row
        for i in range(m // BLOCK):
            rows = slice(i * BLOCK, (i + 1) * BLOCK)
            y2[rows, :] = norm_rows(res[rows, :], g2_row, c2_row).astype(BF16)

        def activate(i):
            hid[0:m, i * W_FC1:(i + 1) * W_FC1] = jax.nn.gelu(pre[i % 2, 0:m], approximate=True).astype(BF16)

        for i in range(N_FC1):
            pre[i % 2, 0:m] = jnp.dot(y2[0:m, :], w1[i], preferred_element_type=F32) + b1row[i]
            if i:
                activate(i - 1)
        activate(N_FC1 - 1)

    def second(m, j):
        cols = slice(j * W_FC2, (j + 1) * W_FC2)
        return (jnp.dot(hid[0:m, :], w2[j], preferred_element_type=F32) + (res[0:m, cols] + b2_row[:, cols])).astype(BF16)

    def shared_home(j, recv):
        other = chip_at(2)
        image = 4 + (other if recv else chip) // 2
        return remote(back.at[j], out.at[image, :, pl.ds(j * W_FC2, W_FC2)], rsend.at[j], rrecv.at[j], other * 2 + core)

    finish(64, xg[384:448, :], og[384:448, :], op, o_mate.wait_recv)
    for j in range(N_FC2):
        rows = second(64, j)
        back[j] = rows[BLOCK:]
        start(shared_home(j, False))
        out[4 + cy, :, j * W_FC2:(j + 1) * W_FC2] = rows[0:BLOCK]

    def home_ready():
        for k in range(4):
            o_home(k, 1).wait_recv()

    for k in (1, 2, 3):
        o_home(k, 0).wait_recv()
    finish(128, jnp.concatenate([xg[0:32, :]] + [xs[x_block(chip_at(k), 0), :] for k in (1, 2, 3)], axis=0),
           jnp.concatenate([og[0:32, :], oh[0, 32:128, :]], axis=0), oh.at[1], home_ready)
    for j in range(N_FC2):
        rows = second(128, j)
        for k in range(4):
            out[chip_at(k), :, j * W_FC2:(j + 1) * W_FC2] = rows[k * BLOCK:(k + 1) * BLOCK]

    for j in range(N_FC2):
        shared_home(j, True).wait_recv()
    for c in sends:
        c.wait_send()


def solution(mesh):
    def device_step(images, w_patch, b_patch, pos_embed, ln1_gain, ln1_bias, w_qkv, b_qkv, w_out, b_out, ln2_gain, ln2_bias, w_fc1, b_fc1, w_fc2, b_fc2):
        tile = lambda v: v.reshape(-1, 128)
        args = (
            jnp.transpose(images, (0, 3, 1, 2)),
            jnp.transpose(w_patch, (0, 2, 1, 3)).reshape(768, D),
            tile(b_patch), pos_embed, tile(ln1_gain), tile(ln1_bias),
            jnp.transpose(w_qkv, (1, 2, 3, 0)).reshape(3 * D, D),
            b_qkv, w_out.reshape(D, D), tile(b_out), tile(ln2_gain), tile(ln2_bias),
            w_fc1, tile(b_fc1), w_fc2, tile(b_fc2))
        vm = pltpu.VMEM
        dma = pltpu.SemaphoreType.DMA
        return pl.pallas_call(
            layer_kernel,
            out_shape=pltpu.VMEM((IMAGES, BLOCK, D), BF16),
            in_specs=[pl.BlockSpec(memory_space=pl.ANY)] * len(args),
            out_specs=pl.BlockSpec(memory_space=pltpu.VMEM),
            scratch_shapes=[
                vm((IMAGES, 3, BLOCK, 256), F32), vm((768, D), BF16), vm((BLOCK, D), BF16), vm((7, 8, 128), F32),
                vm((32, 128), F32), vm((3, 8, 64), F32), vm((3, 512, D), BF16), vm((2, 512, D), BF16),
                vm((N_FC1, D, W_FC1), BF16), vm((N_FC2, FF, W_FC2), BF16),
                vm((3 * OWN, 2048), BF16), vm((2048, 256), BF16), vm((OWN, 768), BF16), vm((OWN, D), BF16),
                vm((2 * TOKENS, D), BF16), vm((2 * TOKENS, D), BF16),
                vm((512, 512), BF16), vm((512, 512), BF16), vm((512, 512), BF16), vm((512, 512), BF16),
                vm((64, 512), BF16), vm((2, HALF, 512), BF16),
                vm((HALF, D), F32), vm((HALF, D), BF16), vm((HALF, FF), BF16), vm((N_FC2, BLOCK, W_FC2), BF16),
                vm((N_FC1, 1, W_FC1), F32), vm((2, HALF, W_FC1), F32),
                dma((13,)), dma((3,)), dma((2,)), dma((N_FC1,)), dma((N_FC2,)),
                dma((3, 2)), dma((3, 2)), dma((4, 2)), dma((4, 2)), dma, dma, dma((4, 2)), dma((4, 2)),
                dma((N_FC2,)), dma((N_FC2,)),
            ],
            compiler_params=pltpu.CompilerParams(
                collective_id=0, has_side_effects=True, vmem_limit_bytes=60 * 1024 * 1024),
        )(*args)

    in_specs = (P('dp', 'sp', None, None), P(), P(), P('sp', None), P(), P(), P(), P(), P(), P(), P(), P(), P(), P(), P(), P())
    return jax.shard_map(device_step, mesh=mesh, in_specs=in_specs, out_specs=P('dp', 'sp', None), check_vma=False)
```

```python
import functools
import math
import jax
import jax.numpy as jnp
from jax import lax
from jax.experimental import pallas as pl
from jax.experimental.pallas import tpu as pltpu
from jax.sharding import PartitionSpec as P

LN_EPS = 1e-6
F32 = jnp.float32
BF16 = jnp.bfloat16
D = 1024
FF = 4096
IMAGES = 6
BLOCK = 32
TOKENS = 256
OWN = 192
HALF = 128
N_FC1, W_FC1 = 8, 512
N_FC2, W_FC2 = 2, 512
EXP_SCALE = math.log2(math.e) / 8.0
MESH = pl.DeviceIdType.MESH
NT = (((1,), (1,)), ((), ()))


def as_row(vec):
    return jnp.concatenate([vec[i:i + 1, :] for i in range(vec.shape[0])], axis=1)


def norm_rows(x_in, gain, bias):
    centered = x_in - jnp.mean(x_in, axis=-1, keepdims=True)
    variance = jnp.mean(centered * centered, axis=-1, keepdims=True)
    return centered * lax.rsqrt(variance + LN_EPS) * gain + bias


def layer_kernel(
        img_hbm, wp_hbm, bp_hbm, pos_hbm, g1_hbm, c1_hbm, wqkv_hbm, bqkv_hbm, wo_hbm, bo_hbm, g2_hbm, c2_hbm,
        w1_hbm, b1_hbm, w2_hbm, b2_hbm,
        out,
        img, wp, pos, vecs, b1, bqkv, wqkv, wo, w1, w2,
        lhs, sel, pix, xs, xg, y1, qh, kh, vh, og, op, oh, res, y2, hid, back, b1row, pre,
        in_sem, wqkv_sem, wo_sem, w1_sem, w2_sem,
        xsend, xrecv, fsend, frecv, osend, orecv, hsend, hrecv, rsend, rrecv):
    dp = lax.axis_index("dp")
    me = lax.axis_index("sp")
    chip = me // 2
    core = me % 2
    mate = chip * 2 + (1 - core)
    cx = chip % 2
    cy = chip // 2

    def remote(src, dst, ssem, rsem, dev):
        return pltpu.make_async_remote_copy(
            src_ref=src, dst_ref=dst, send_sem=ssem, recv_sem=rsem, device_id=(dp, dev), device_id_type=MESH)

    def chip_at(k):
        return ((cy + k // 2) % 2) * 2 + (cx + k % 2) % 2

    barrier = pltpu.get_barrier_semaphore()
    for k in range(1, 8):
        pl.semaphore_signal(barrier, inc=1, device_id=(dp, (me + k) % 8), device_id_type=MESH)

    groups = ((4, 2), (0, 4))
    small = [(img_hbm.at[pl.ds(n0, n), :, :, :], img.at[pl.ds(n0, n), :, :, :]) for n0, n in groups] + [(wp_hbm, wp), (pos_hbm, pos)]
    for i, v in enumerate((bp_hbm, g1_hbm, c1_hbm, bo_hbm, g2_hbm, c2_hbm, b2_hbm)):
        small.append((v, vecs.at[i]))
    small.append((b1_hbm, b1))
    small.append((bqkv_hbm.at[:, pl.ds(pl.multiple_of(core * 8, 8), 8), :], bqkv))
    small_copies = [pltpu.make_async_copy(s, d, in_sem.at[i]) for i, (s, d) in enumerate(small)]
    for i in (0, 2, 1) + tuple(range(3, len(small))):
        small_copies[i].start()
    wq_copies = [
        pltpu.make_async_copy(wqkv_hbm.at[pl.ds(pl.multiple_of(t * D + core * 512, 512), 512), :], wqkv.at[t], wqkv_sem.at[t])
        for t in range(3)]
    wo_copies = [
        pltpu.make_async_copy(wo_hbm.at[pl.ds(pl.multiple_of(((core + i) % 2) * 512, 512), 512), :], wo.at[i], wo_sem.at[i])
        for i in range(2)]
    w1_copies = [pltpu.make_async_copy(w1_hbm.at[:, pl.ds(i * W_FC1, W_FC1)], w1.at[i], w1_sem.at[i]) for i in range(N_FC1)]
    w2_copies = [pltpu.make_async_copy(w2_hbm.at[:, pl.ds(i * W_FC2, W_FC2)], w2.at[i], w2_sem.at[i]) for i in range(N_FC2)]

    rows128 = lax.broadcasted_iota(jnp.int32, (128, 256), 0)
    cols256 = lax.broadcasted_iota(jnp.int32, (128, 256), 1)
    diff = cols256 - rows128 % 16

    def build_sel(i, carry):
        sel[pl.ds(pl.multiple_of(i * 128, 128), 128), :] = jnp.where(diff == i * 16, 1.0, 0.0).astype(BF16)
        return carry
    lax.fori_loop(0, 16, build_sel, 0)

    keep = lax.broadcasted_iota(jnp.int32, (8, 128), 1) // 16 == lax.broadcasted_iota(jnp.int32, (8, 128), 0)

    def embed(group):
        n0, count = groups[group]
        m = count * BLOCK
        top = n0 * BLOCK * 3

        def spread(i, carry):
            for g in range(48):
                p, c = g // 3, g % 3
                t, col = g // 16, (g % 16) * 128
                for py in range(2):
                    row = img[n0 + i, c, pl.ds(py * 16 + p, 1), :]
                    halves = [jnp.where(keep, jnp.broadcast_to(row[:, j * 128:(j + 1) * 128], (8, 128)), 0.0) for j in range(2)]
                    at = pl.multiple_of(top + t * m + i * BLOCK + py * 16, 16)
                    lhs[pl.ds(at, 16), pl.ds(col, 128)] = jnp.concatenate(halves, axis=0).astype(BF16)
            return carry
        lax.fori_loop(0, count, spread, 0)
        h = 3 * m // 2
        both = [jnp.dot(lhs[top + i * h:top + (i + 1) * h, :], sel[...], preferred_element_type=F32).astype(BF16) for i in range(2)]
        rows = slice(n0 * BLOCK, n0 * BLOCK + m)
        pix[rows, 0:256] = both[0][0:m]
        pix[rows, 256:512] = jnp.concatenate([both[0][m:], both[1][0:m // 2]], axis=0)
        pix[rows, 512:768] = both[1][m // 2:]
        return rows, count

    def project(rows, count):
        for n in range(2):
            cols = slice(n * 512, (n + 1) * 512)
            emb = jnp.dot(pix[rows, :], wp[:, cols], preferred_element_type=F32) + bp_row[:, cols]
            emb = emb.reshape(count, BLOCK, 512) + pos[:, cols].astype(F32)[None]
            xs[rows, cols] = emb.reshape(count * BLOCK, 512).astype(BF16)

    slot1_first = {3: 8, 1: 10, 0: 12, 2: 13}

    def block(slot, k, other):
        first = 2 * k + other if slot == 0 else slot1_first[k] + other * (2 if k in (0, 2) else 1)
        return pl.ds(first * BLOCK, BLOCK)

    def x_block(chip_to, slot):
        image = chip_to if slot == 0 else 4 + chip_to // 2
        return pl.ds(pl.multiple_of(image * BLOCK, BLOCK), BLOCK)

    sends = []

    def start(copy):
        copy.start()
        sends.append(copy)

    def send_slot(slot, where):
        for k in where:
            to = chip_at(k)
            start(remote(xs.at[x_block(to, slot), :], xg.at[block(slot, k, 0), :], xsend.at[k - 1, slot], xrecv.at[k - 1, slot], to * 2 + core))

    def share_own(slot):
        start(remote(xs.at[x_block(chip, slot), :], xg.at[block(slot, 0, 1), :], fsend.at[0, slot], frecv.at[0, slot], mate))
        xg[block(slot, 0, 0), :] = xs[x_block(chip, slot), :]

    small_copies[0].wait()
    part = embed(0)
    for c in small_copies[2:]:
        c.wait()
    small_copies[1].wait()
    for c in wq_copies + wo_copies + w1_copies + w2_copies:
        c.start()
    bp_row = as_row(vecs[0])
    project(*part)
    pl.semaphore_wait(barrier, 7)
    send_slot(1, (2, 1))
    share_own(1)
    project(*embed(1))
    send_slot(0, (2, 1))
    send_slot(1, (3,))
    send_slot(0, (3,))
    share_own(0)

    g1_row, c1_row = as_row(vecs[1]), as_row(vecs[2])

    def norm_blocks(blocks):
        for rows in blocks:
            y1[rows, :] = norm_rows(xg[rows, :].astype(F32), g1_row, c1_row).astype(BF16)

    def arrive(slot, k):
        ref = xg.at[block(slot, k, 0), :]
        remote(ref, ref, xsend.at[k - 1, slot], xrecv.at[k - 1, slot], chip_at(k) * 2 + core).wait_recv()
        start(remote(ref, xg.at[block(slot, k, 1), :], fsend.at[k, slot], frecv.at[k, slot], mate))

    def forwarded(slot, k):
        ref = xg.at[block(slot, k, 1), :]
        remote(ref, ref, fsend.at[k, slot], frecv.at[k, slot], mate).wait_recv()

    norm_blocks([block(1, 0, 0), block(0, 0, 0)])
    for slot in (1, 0):
        forwarded(slot, 0)
    norm_blocks([block(1, 0, 1), block(0, 0, 1)])
    for c in wq_copies:
        c.wait()
    brow = [as_row(bqkv[t]) for t in range(3)]

    def heads_of(t, dst, pieces):
        rows = jnp.concatenate([y1[a:b, :] for a, b in pieces], axis=0)
        got = (lax.dot_general(rows, wqkv[t], NT, preferred_element_type=F32) + brow[t]).astype(BF16)
        at = 0
        for a, b in pieces:
            dst[a:b, :] = got[at:at + b - a]
            at += b - a

    own = ((0, 64), (384, 416), (448, 480))
    heads_of(0, qh, own)
    heads_of(1, kh, own)
    heads_of(2, vh, own)

    for slot in (1, 0):
        for k in (2, 1):
            arrive(slot, k)
        norm_blocks([block(slot, k, 0) for k in (2, 1)])
    for slot in (1, 0):
        for k in (2, 1):
            forwarded(slot, k)
    norm_blocks([block(slot, k, 1) for slot in (1, 0) for k in (2, 1)])
    near_q = ((64, 192), (416, 448), (480, 512))
    near_kv = ((64, 192), (320, 384), (416, 448), (480, 512))
    heads_of(0, qh, near_q)
    heads_of(1, kh, near_kv)
    for slot in (1, 0):
        arrive(slot, 3)
    heads_of(2, vh, near_kv)
    norm_blocks([block(slot, 3, 0) for slot in (1, 0)])
    for slot in (1, 0):
        forwarded(slot, 3)
    norm_blocks([block(slot, 3, 1) for slot in (1, 0)])
    heads_of(0, qh, ((192, 256),))
    heads_of(1, kh, ((192, 320),))
    heads_of(2, vh, ((192, 320),))

    def attend(q0, rows, k0):
        low = lax.broadcasted_iota(jnp.int32, (rows, 128), 1) < 64
        pairs = [slice(pair * 128, (pair + 1) * 128) for pair in range(4)]
        scores = []
        for cols in pairs:
            q_pair = qh[q0:q0 + rows, cols]
            for h in range(2):
                q_one = jnp.where(low == (h == 0), q_pair, jnp.zeros_like(q_pair))
                scores.append(lax.dot_general(q_one, kh[k0:k0 + 256, cols], NT, preferred_element_type=F32))
        weights = []
        for s in scores:
            e = jnp.exp2((s - jnp.max(s, axis=-1, keepdims=True)) * EXP_SCALE)
            weights.append((e * (1.0 / jnp.sum(e, axis=-1, keepdims=True))).astype(BF16))
        for i, cols in enumerate(pairs):
            heads = [jnp.dot(weights[2 * i + h], vh[k0:k0 + 256, cols], preferred_element_type=F32) for h in range(2)]
            og[q0:q0 + rows, cols] = jnp.where(low, heads[0], heads[1]).astype(BF16)

    def o_home(k, other):
        dev = chip_at(k) * 2 + (core if other == 0 else 1 - core)
        return remote(og.at[block(0, k, other), :], oh.at[other, pl.ds(k * BLOCK, BLOCK), :],
                      hsend.at[k, other], hrecv.at[k, other], dev)

    o_mate = remote(og.at[pl.ds(448, 64), :], op, osend, orecv, mate)

    attend(128, 128, 0)
    for k in (3, 2):
        for other in range(2):
            start(o_home(k, other))
    attend(384, 128, 256)
    start(o_mate)
    attend(0, 128, 0)
    for k, other in ((1, 0), (1, 1), (0, 1)):
        start(o_home(k, other))

    for c in wo_copies + w1_copies + w2_copies:
        c.wait()
    bo_row, g2_row, c2_row, b2_row = [as_row(vecs[i]) for i in (3, 4, 5, 6)]
    for i in range(N_FC1):
        b1row[i] = as_row(b1[i * 4:(i + 1) * 4, :])

    def finish(m, x_in, near, far, ready):
        res[0:m, :] = x_in.astype(F32) + jnp.dot(near, wo[0], preferred_element_type=F32)
        ready()
        res[0:m, :] = res[0:m, :] + jnp.dot(far[...], wo[1], preferred_element_type=F32) + bo_row
        for i in range(m // BLOCK):
            rows = slice(i * BLOCK, (i + 1) * BLOCK)
            y2[rows, :] = norm_rows(res[rows, :], g2_row, c2_row).astype(BF16)

        def activate(i):
            hid[0:m, i * W_FC1:(i + 1) * W_FC1] = jax.nn.gelu(pre[i % 2, 0:m], approximate=True).astype(BF16)

        for i in range(N_FC1):
            pre[i % 2, 0:m] = jnp.dot(y2[0:m, :], w1[i], preferred_element_type=F32) + b1row[i]
            if i:
                activate(i - 1)
        activate(N_FC1 - 1)

    def second(m, j):
        cols = slice(j * W_FC2, (j + 1) * W_FC2)
        return (jnp.dot(hid[0:m, :], w2[j], preferred_element_type=F32) + (res[0:m, cols] + b2_row[:, cols])).astype(BF16)

    def shared_home(j, recv):
        other = chip_at(2)
        image = 4 + (other if recv else chip) // 2
        return remote(back.at[j], out.at[image, :, pl.ds(j * W_FC2, W_FC2)], rsend.at[j], rrecv.at[j], other * 2 + core)

    finish(64, xg[384:448, :], og[384:448, :], op, o_mate.wait_recv)
    for j in range(N_FC2):
        rows = second(64, j)
        back[j] = rows[BLOCK:]
        start(shared_home(j, False))
        out[4 + cy, :, j * W_FC2:(j + 1) * W_FC2] = rows[0:BLOCK]

    def home_ready():
        for k in range(4):
            o_home(k, 1).wait_recv()

    for k in (1, 2, 3):
        o_home(k, 0).wait_recv()
    finish(128, jnp.concatenate([xg[0:32, :]] + [xs[x_block(chip_at(k), 0), :] for k in (1, 2, 3)], axis=0),
           jnp.concatenate([og[0:32, :], oh[0, 32:128, :]], axis=0), oh.at[1], home_ready)
    for j in range(N_FC2):
        rows = second(128, j)
        for k in range(4):
            out[chip_at(k), :, j * W_FC2:(j + 1) * W_FC2] = rows[k * BLOCK:(k + 1) * BLOCK]

    for j in range(N_FC2):
        shared_home(j, True).wait_recv()
    for c in sends:
        c.wait_send()


def solution(mesh):
    def device_step(images, w_patch, b_patch, pos_embed, ln1_gain, ln1_bias, w_qkv, b_qkv, w_out, b_out, ln2_gain, ln2_bias, w_fc1, b_fc1, w_fc2, b_fc2):
        tile = lambda v: v.reshape(-1, 128)
        args = (
            jnp.transpose(images, (0, 3, 1, 2)),
            jnp.transpose(w_patch, (0, 2, 1, 3)).reshape(768, D),
            tile(b_patch), pos_embed, tile(ln1_gain), tile(ln1_bias),
            jnp.transpose(w_qkv, (1, 2, 3, 0)).reshape(3 * D, D),
            b_qkv, w_out.reshape(D, D), tile(b_out), tile(ln2_gain), tile(ln2_bias),
            w_fc1, tile(b_fc1), w_fc2, tile(b_fc2))
        vm = pltpu.VMEM
        dma = pltpu.SemaphoreType.DMA
        return pl.pallas_call(
            layer_kernel,
            out_shape=pltpu.VMEM((IMAGES, BLOCK, D), BF16),
            in_specs=[pl.BlockSpec(memory_space=pl.ANY)] * len(args),
            out_specs=pl.BlockSpec(memory_space=pltpu.VMEM),
            scratch_shapes=[
                vm((IMAGES, 3, BLOCK, 256), F32), vm((768, D), BF16), vm((BLOCK, D), BF16), vm((7, 8, 128), F32),
                vm((32, 128), F32), vm((3, 8, 64), F32), vm((3, 512, D), BF16), vm((2, 512, D), BF16),
                vm((N_FC1, D, W_FC1), BF16), vm((N_FC2, FF, W_FC2), BF16),
                vm((3 * OWN, 2048), BF16), vm((2048, 256), BF16), vm((OWN, 768), BF16), vm((OWN, D), BF16),
                vm((2 * TOKENS, D), BF16), vm((2 * TOKENS, D), BF16),
                vm((512, 512), BF16), vm((512, 512), BF16), vm((512, 512), BF16), vm((512, 512), BF16),
                vm((64, 512), BF16), vm((2, HALF, 512), BF16),
                vm((HALF, D), F32), vm((HALF, D), BF16), vm((HALF, FF), BF16), vm((N_FC2, BLOCK, W_FC2), BF16),
                vm((N_FC1, 1, W_FC1), F32), vm((2, HALF, W_FC1), F32),
                dma((13,)), dma((3,)), dma((2,)), dma((N_FC1,)), dma((N_FC2,)),
                dma((3, 2)), dma((3, 2)), dma((4, 2)), dma((4, 2)), dma, dma, dma((4, 2)), dma((4, 2)),
                dma((N_FC2,)), dma((N_FC2,)),
            ],
            compiler_params=pltpu.CompilerParams(
                collective_id=0, has_side_effects=True, vmem_limit_bytes=60 * 1024 * 1024),
        )(*args)

    in_specs = (P('dp', 'sp', None, None), P(), P(), P('sp', None), P(), P(), P(), P(), P(), P(), P(), P(), P(), P(), P(), P())
    return jax.shard_map(device_step, mesh=mesh, in_specs=in_specs, out_specs=P('dp', 'sp', None), check_vma=False)
```

```python
import functools
import math
import jax
import jax.numpy as jnp
from jax import lax
from jax.experimental import pallas as pl
from jax.experimental.pallas import tpu as pltpu
from jax.sharding import PartitionSpec as P

LN_EPS = 1e-6
F32 = jnp.float32
BF16 = jnp.bfloat16
D = 1024
FF = 4096
IMAGES = 6
BLOCK = 32
TOKENS = 256
OWN = 192
HALF = 128
N_FC1, W_FC1 = 8, 512
N_FC2, W_FC2 = 2, 512
EXP_SCALE = math.log2(math.e) / 8.0
MESH = pl.DeviceIdType.MESH
NT = (((1,), (1,)), ((), ()))


def as_row(vec):
    return jnp.concatenate([vec[i:i + 1, :] for i in range(vec.shape[0])], axis=1)


def norm_rows(x_in, gain, bias):
    centered = x_in - jnp.mean(x_in, axis=-1, keepdims=True)
    variance = jnp.mean(centered * centered, axis=-1, keepdims=True)
    return centered * lax.rsqrt(variance + LN_EPS) * gain + bias


def layer_kernel(
        img_hbm, wp_hbm, bp_hbm, pos_hbm, g1_hbm, c1_hbm, wqkv_hbm, bqkv_hbm, wo_hbm, bo_hbm, g2_hbm, c2_hbm,
        w1_hbm, b1_hbm, w2_hbm, b2_hbm,
        out,
        img, wp, pos, vecs, b1, bqkv, wqkv, wo, w1, w2,
        lhs, sel, pix, xs, xg, y1, qh, kh, vh, og, op, oh, res, y2, hid, back, b1row, pre,
        in_sem, wqkv_sem, wo_sem, w1_sem, w2_sem,
        xsend, xrecv, fsend, frecv, osend, orecv, hsend, hrecv, rsend, rrecv):
    dp = lax.axis_index("dp")
    me = lax.axis_index("sp")
    chip = me // 2
    core = me % 2
    mate = chip * 2 + (1 - core)
    cx = chip % 2
    cy = chip // 2

    def remote(src, dst, ssem, rsem, dev):
        return pltpu.make_async_remote_copy(
            src_ref=src, dst_ref=dst, send_sem=ssem, recv_sem=rsem, device_id=(dp, dev), device_id_type=MESH)

    def chip_at(k):
        return ((cy + k // 2) % 2) * 2 + (cx + k % 2) % 2

    barrier = pltpu.get_barrier_semaphore()
    for k in range(1, 8):
        pl.semaphore_signal(barrier, inc=1, device_id=(dp, (me + k) % 8), device_id_type=MESH)

    groups = ((4, 2), (0, 4))
    small = [(img_hbm.at[pl.ds(n0, n), :, :, :], img.at[pl.ds(n0, n), :, :, :]) for n0, n in groups] + [(wp_hbm, wp), (pos_hbm, pos)]
    for i, v in enumerate((bp_hbm, g1_hbm, c1_hbm, bo_hbm, g2_hbm, c2_hbm, b2_hbm)):
        small.append((v, vecs.at[i]))
    small.append((b1_hbm, b1))
    small.append((bqkv_hbm.at[:, pl.ds(pl.multiple_of(core * 8, 8), 8), :], bqkv))
    small_copies = [pltpu.make_async_copy(s, d, in_sem.at[i]) for i, (s, d) in enumerate(small)]
    for i in (0, 2, 1) + tuple(range(3, len(small))):
        small_copies[i].start()
    wq_copies = [
        pltpu.make_async_copy(wqkv_hbm.at[pl.ds(pl.multiple_of(t * D + core * 512, 512), 512), :], wqkv.at[t], wqkv_sem.at[t])
        for t in range(3)]
    wo_copies = [
        pltpu.make_async_copy(wo_hbm.at[pl.ds(pl.multiple_of(((core + i) % 2) * 512, 512), 512), :], wo.at[i], wo_sem.at[i])
        for i in range(2)]
    w1_copies = [pltpu.make_async_copy(w1_hbm.at[:, pl.ds(i * W_FC1, W_FC1)], w1.at[i], w1_sem.at[i]) for i in range(N_FC1)]
    w2_copies = [pltpu.make_async_copy(w2_hbm.at[:, pl.ds(i * W_FC2, W_FC2)], w2.at[i], w2_sem.at[i]) for i in range(N_FC2)]

    rows128 = lax.broadcasted_iota(jnp.int32, (128, 256), 0)
    cols256 = lax.broadcasted_iota(jnp.int32, (128, 256), 1)
    diff = cols256 - rows128 % 16

    def build_sel(i, carry):
        sel[pl.ds(pl.multiple_of(i * 128, 128), 128), :] = jnp.where(diff == i * 16, 1.0, 0.0).astype(BF16)
        return carry
    lax.fori_loop(0, 16, build_sel, 0)

    keep = lax.broadcasted_iota(jnp.int32, (8, 128), 1) // 16 == lax.broadcasted_iota(jnp.int32, (8, 128), 0)

    def embed(group):
        n0, count = groups[group]
        m = count * BLOCK
        top = n0 * BLOCK * 3

        def spread(i, carry):
            for g in range(48):
                p, c = g // 3, g % 3
                t, col = g // 16, (g % 16) * 128
                for py in range(2):
                    row = img[n0 + i, c, pl.ds(py * 16 + p, 1), :]
                    halves = [jnp.where(keep, jnp.broadcast_to(row[:, j * 128:(j + 1) * 128], (8, 128)), 0.0) for j in range(2)]
                    at = pl.multiple_of(top + t * m + i * BLOCK + py * 16, 16)
                    lhs[pl.ds(at, 16), pl.ds(col, 128)] = jnp.concatenate(halves, axis=0).astype(BF16)
            return carry
        lax.fori_loop(0, count, spread, 0)
        h = 3 * m // 2
        both = [jnp.dot(lhs[top + i * h:top + (i + 1) * h, :], sel[...], preferred_element_type=F32).astype(BF16) for i in range(2)]
        rows = slice(n0 * BLOCK, n0 * BLOCK + m)
        pix[rows, 0:256] = both[0][0:m]
        pix[rows, 256:512] = jnp.concatenate([both[0][m:], both[1][0:m // 2]], axis=0)
        pix[rows, 512:768] = both[1][m // 2:]
        return rows, count

    def project(rows, count):
        for n in range(2):
            cols = slice(n * 512, (n + 1) * 512)
            emb = jnp.dot(pix[rows, :], wp[:, cols], preferred_element_type=F32) + bp_row[:, cols]
            emb = emb.reshape(count, BLOCK, 512) + pos[:, cols].astype(F32)[None]
            xs[rows, cols] = emb.reshape(count * BLOCK, 512).astype(BF16)

    slot1_first = {3: 8, 1: 10, 0: 12, 2: 13}

    def block(slot, k, other):
        first = 2 * k + other if slot == 0 else slot1_first[k] + other * (2 if k in (0, 2) else 1)
        return pl.ds(first * BLOCK, BLOCK)

    def x_block(chip_to, slot):
        image = chip_to if slot == 0 else 4 + chip_to // 2
        return pl.ds(pl.multiple_of(image * BLOCK, BLOCK), BLOCK)

    sends = []

    def start(copy):
        copy.start()
        sends.append(copy)

    def send_slot(slot, where):
        for k in where:
            to = chip_at(k)
            start(remote(xs.at[x_block(to, slot), :], xg.at[block(slot, k, 0), :], xsend.at[k - 1, slot], xrecv.at[k - 1, slot], to * 2 + core))

    def share_own(slot):
        start(remote(xs.at[x_block(chip, slot), :], xg.at[block(slot, 0, 1), :], fsend.at[0, slot], frecv.at[0, slot], mate))
        xg[block(slot, 0, 0), :] = xs[x_block(chip, slot), :]

    small_copies[0].wait()
    part = embed(0)
    for c in small_copies[2:]:
        c.wait()
    small_copies[1].wait()
    for c in wq_copies + wo_copies + w1_copies + w2_copies:
        c.start()
    bp_row = as_row(vecs[0])
    project(*part)
    pl.semaphore_wait(barrier, 7)
    send_slot(1, (2, 1))
    share_own(1)
    project(*embed(1))
    send_slot(0, (2, 1))
    send_slot(1, (3,))
    send_slot(0, (3,))
    share_own(0)

    g1_row, c1_row = as_row(vecs[1]), as_row(vecs[2])

    def norm_blocks(blocks):
        for rows in blocks:
            y1[rows, :] = norm_rows(xg[rows, :].astype(F32), g1_row, c1_row).astype(BF16)

    def arrive(slot, k):
        ref = xg.at[block(slot, k, 0), :]
        remote(ref, ref, xsend.at[k - 1, slot], xrecv.at[k - 1, slot], chip_at(k) * 2 + core).wait_recv()
        start(remote(ref, xg.at[block(slot, k, 1), :], fsend.at[k, slot], frecv.at[k, slot], mate))

    def forwarded(slot, k):
        ref = xg.at[block(slot, k, 1), :]
        remote(ref, ref, fsend.at[k, slot], frecv.at[k, slot], mate).wait_recv()

    norm_blocks([block(1, 0, 0), block(0, 0, 0)])
    for slot in (1, 0):
        forwarded(slot, 0)
    norm_blocks([block(1, 0, 1), block(0, 0, 1)])
    for c in wq_copies:
        c.wait()
    brow = [as_row(bqkv[t]) for t in range(3)]

    def heads_of(t, dst, pieces):
        rows = jnp.concatenate([y1[a:b, :] for a, b in pieces], axis=0)
        got = (lax.dot_general(rows, wqkv[t], NT, preferred_element_type=F32) + brow[t]).astype(BF16)
        at = 0
        for a, b in pieces:
            dst[a:b, :] = got[at:at + b - a]
            at += b - a

    pairs = [slice(pair * 128, (pair + 1) * 128) for pair in range(4)]
    low = lax.broadcasted_iota(jnp.int32, (128, 128), 1) < 64

    def score(q0, k0):
        scores = []
        for cols in pairs:
            q_pair = qh[q0:q0 + 128, cols]
            for h in range(2):
                q_one = jnp.where(low == (h == 0), q_pair, jnp.zeros_like(q_pair))
                scores.append(lax.dot_general(q_one, kh[k0:k0 + 256, cols], NT, preferred_element_type=F32))
        return scores

    def soften(scores):
        weights = []
        for s in scores:
            e = jnp.exp2((s - jnp.max(s, axis=-1, keepdims=True)) * EXP_SCALE)
            weights.append((e * (1.0 / jnp.sum(e, axis=-1, keepdims=True))).astype(BF16))
        return weights

    def combine(weights, q0, k0):
        for i, cols in enumerate(pairs):
            heads = [jnp.dot(weights[2 * i + h], vh[k0:k0 + 256, cols], preferred_element_type=F32) for h in range(2)]
            og[q0:q0 + 128, cols] = jnp.where(low, heads[0], heads[1]).astype(BF16)

    o_mate = remote(og.at[pl.ds(448, 64), :], op, osend, orecv, mate)

    own = ((0, 64), (384, 416), (448, 480))
    heads_of(0, qh, own)
    heads_of(1, kh, own)
    heads_of(2, vh, own)

    for slot in (1, 0):
        for k in (2, 1):
            arrive(slot, k)
        norm_blocks([block(slot, k, 0) for k in (2, 1)])
    for slot in (1, 0):
        for k in (2, 1):
            forwarded(slot, k)
    norm_blocks([block(slot, k, 1) for slot in (1, 0) for k in (2, 1)])
    near_q = ((64, 192), (416, 448), (480, 512))
    near_kv = ((64, 192), (320, 384), (416, 448), (480, 512))
    heads_of(0, qh, near_q)
    heads_of(1, kh, near_kv)
    arrive(1, 3)
    heads_of(2, vh, near_kv)
    norm_blocks([block(1, 3, 0)])
    forwarded(1, 3)
    norm_blocks([block(1, 3, 1)])
    heads_of(1, kh, ((256, 320),))
    heads_of(2, vh, ((256, 320),))
    arrive(0, 3)
    combine(soften(score(384, 256)), 384, 256)
    start(o_mate)
    norm_blocks([block(0, 3, 0)])
    forwarded(0, 3)
    norm_blocks([block(0, 3, 1)])
    for t, dst in ((0, qh), (1, kh), (2, vh)):
        heads_of(t, dst, ((192, 256),))

    def o_home(k, other):
        dev = chip_at(k) * 2 + (core if other == 0 else 1 - core)
        return remote(og.at[block(0, k, other), :], oh.at[other, pl.ds(k * BLOCK, BLOCK), :],
                      hsend.at[k, other], hrecv.at[k, other], dev)

    late = soften(score(128, 0))
    scores = score(0, 0)
    combine(late, 128, 0)
    for k in (3, 2):
        for other in range(2):
            start(o_home(k, other))
    combine(soften(scores), 0, 0)
    for k, other in ((1, 0), (1, 1), (0, 1)):
        start(o_home(k, other))

    for c in wo_copies + w1_copies + w2_copies:
        c.wait()
    bo_row, g2_row, c2_row, b2_row = [as_row(vecs[i]) for i in (3, 4, 5, 6)]
    for i in range(N_FC1):
        b1row[i] = as_row(b1[i * 4:(i + 1) * 4, :])

    def finish(m, x_in, near, far, ready):
        res[0:m, :] = x_in.astype(F32) + jnp.dot(near, wo[0], preferred_element_type=F32)
        ready()
        res[0:m, :] = res[0:m, :] + jnp.dot(far[...], wo[1], preferred_element_type=F32) + bo_row
        for i in range(m // BLOCK):
            rows = slice(i * BLOCK, (i + 1) * BLOCK)
            y2[rows, :] = norm_rows(res[rows, :], g2_row, c2_row).astype(BF16)

        def activate(i):
            hid[0:m, i * W_FC1:(i + 1) * W_FC1] = jax.nn.gelu(pre[i % 2, 0:m], approximate=True).astype(BF16)

        for i in range(N_FC1):
            pre[i % 2, 0:m] = jnp.dot(y2[0:m, :], w1[i], preferred_element_type=F32) + b1row[i]
            if i:
                activate(i - 1)
        activate(N_FC1 - 1)

    def second(m, j):
        cols = slice(j * W_FC2, (j + 1) * W_FC2)
        return (jnp.dot(hid[0:m, :], w2[j], preferred_element_type=F32) + (res[0:m, cols] + b2_row[:, cols])).astype(BF16)

    def shared_home(j, recv):
        other = chip_at(2)
        image = 4 + (other if recv else chip) // 2
        return remote(back.at[j], out.at[image, :, pl.ds(j * W_FC2, W_FC2)], rsend.at[j], rrecv.at[j], other * 2 + core)

    finish(64, xg[384:448, :], og[384:448, :], op, o_mate.wait_recv)
    for j in range(N_FC2):
        rows = second(64, j)
        back[j] = rows[BLOCK:]
        start(shared_home(j, False))
        out[4 + cy, :, j * W_FC2:(j + 1) * W_FC2] = rows[0:BLOCK]

    def home_ready():
        for k in range(4):
            o_home(k, 1).wait_recv()

    for k in (1, 2, 3):
        o_home(k, 0).wait_recv()
    finish(128, jnp.concatenate([xg[0:32, :]] + [xs[x_block(chip_at(k), 0), :] for k in (1, 2, 3)], axis=0),
           jnp.concatenate([og[0:32, :], oh[0, 32:128, :]], axis=0), oh.at[1], home_ready)
    for j in range(N_FC2):
        rows = second(128, j)
        for k in range(4):
            out[chip_at(k), :, j * W_FC2:(j + 1) * W_FC2] = rows[k * BLOCK:(k + 1) * BLOCK]

    for j in range(N_FC2):
        shared_home(j, True).wait_recv()
    for c in sends:
        c.wait_send()


def solution(mesh):
    def device_step(images, w_patch, b_patch, pos_embed, ln1_gain, ln1_bias, w_qkv, b_qkv, w_out, b_out, ln2_gain, ln2_bias, w_fc1, b_fc1, w_fc2, b_fc2):
        tile = lambda v: v.reshape(-1, 128)
        args = (
            jnp.transpose(images, (0, 3, 1, 2)),
            jnp.transpose(w_patch, (0, 2, 1, 3)).reshape(768, D),
            tile(b_patch), pos_embed, tile(ln1_gain), tile(ln1_bias),
            jnp.transpose(w_qkv, (1, 2, 3, 0)).reshape(3 * D, D),
            b_qkv, w_out.reshape(D, D), tile(b_out), tile(ln2_gain), tile(ln2_bias),
            w_fc1, tile(b_fc1), w_fc2, tile(b_fc2))
        vm = pltpu.VMEM
        dma = pltpu.SemaphoreType.DMA
        return pl.pallas_call(
            layer_kernel,
            out_shape=pltpu.VMEM((IMAGES, BLOCK, D), BF16),
            in_specs=[pl.BlockSpec(memory_space=pl.ANY)] * len(args),
            out_specs=pl.BlockSpec(memory_space=pltpu.VMEM),
            scratch_shapes=[
                vm((IMAGES, 3, BLOCK, 256), F32), vm((768, D), BF16), vm((BLOCK, D), BF16), vm((7, 8, 128), F32),
                vm((32, 128), F32), vm((3, 8, 64), F32), vm((3, 512, D), BF16), vm((2, 512, D), BF16),
                vm((N_FC1, D, W_FC1), BF16), vm((N_FC2, FF, W_FC2), BF16),
                vm((3 * OWN, 2048), BF16), vm((2048, 256), BF16), vm((OWN, 768), BF16), vm((OWN, D), BF16),
                vm((2 * TOKENS, D), BF16), vm((2 * TOKENS, D), BF16),
                vm((512, 512), BF16), vm((512, 512), BF16), vm((512, 512), BF16), vm((512, 512), BF16),
                vm((64, 512), BF16), vm((2, HALF, 512), BF16),
                vm((HALF, D), F32), vm((HALF, D), BF16), vm((HALF, FF), BF16), vm((N_FC2, BLOCK, W_FC2), BF16),
                vm((N_FC1, 1, W_FC1), F32), vm((2, HALF, W_FC1), F32),
                dma((13,)), dma((3,)), dma((2,)), dma((N_FC1,)), dma((N_FC2,)),
                dma((3, 2)), dma((3, 2)), dma((4, 2)), dma((4, 2)), dma, dma, dma((4, 2)), dma((4, 2)),
                dma((N_FC2,)), dma((N_FC2,)),
            ],
            compiler_params=pltpu.CompilerParams(
                collective_id=0, has_side_effects=True, vmem_limit_bytes=60 * 1024 * 1024),
        )(*args)

    in_specs = (P('dp', 'sp', None, None), P(), P(), P('sp', None), P(), P(), P(), P(), P(), P(), P(), P(), P(), P(), P(), P())
    return jax.shard_map(device_step, mesh=mesh, in_specs=in_specs, out_specs=P('dp', 'sp', None), check_vma=False)
```

```python
import functools
import math
import jax
import jax.numpy as jnp
from jax import lax
from jax.experimental import pallas as pl
from jax.experimental.pallas import tpu as pltpu
from jax.sharding import PartitionSpec as P

LN_EPS = 1e-6
F32 = jnp.float32
BF16 = jnp.bfloat16
D = 1024
FF = 4096
IMAGES = 6
BLOCK = 32
TOKENS = 256
OWN = 192
HALF = 96
N_FC1, W_FC1 = 8, 512
N_FC2, W_FC2 = 2, 512
EXP_SCALE = math.log2(math.e) / 8.0
MESH = pl.DeviceIdType.MESH
NT = (((1,), (1,)), ((), ()))


def as_row(vec):
    return jnp.concatenate([vec[i:i + 1, :] for i in range(vec.shape[0])], axis=1)


def norm_rows(x_in, gain, bias):
    centered = x_in - jnp.mean(x_in, axis=-1, keepdims=True)
    variance = jnp.mean(centered * centered, axis=-1, keepdims=True)
    return centered * lax.rsqrt(variance + LN_EPS) * gain + bias


def layer_kernel(
        img_hbm, wp_hbm, bp_hbm, pos_hbm, g1_hbm, c1_hbm, wqkv_hbm, bqkv_hbm, wo_hbm, bo_hbm, g2_hbm, c2_hbm,
        w1_hbm, b1_hbm, w2_hbm, b2_hbm,
        out,
        img, wp, pos, vecs, b1, bqkv, wqkv, wo, w1, w2,
        lhs, sel, pix, xs, xg, y1, qh, kh, vh, og, op, oh, res, y2, hid, back, b1row, pre,
        in_sem, wqkv_sem, wo_sem, w1_sem, w2_sem,
        xsend, xrecv, fsend, frecv, osend, orecv, hsend, hrecv, rsend, rrecv):
    dp = lax.axis_index("dp")
    me = lax.axis_index("sp")
    chip = me // 2
    core = me % 2
    mate = chip * 2 + (1 - core)
    cx = chip % 2
    cy = chip // 2

    def remote(src, dst, ssem, rsem, dev):
        return pltpu.make_async_remote_copy(
            src_ref=src, dst_ref=dst, send_sem=ssem, recv_sem=rsem, device_id=(dp, dev), device_id_type=MESH)

    def chip_at(k):
        return ((cy + k // 2) % 2) * 2 + (cx + k % 2) % 2

    barrier = pltpu.get_barrier_semaphore()
    for k in range(1, 8):
        pl.semaphore_signal(barrier, inc=1, device_id=(dp, (me + k) % 8), device_id_type=MESH)

    groups = ((4, 2), (0, 4))
    small = [(img_hbm.at[pl.ds(n0, n), :, :, :], img.at[pl.ds(n0, n), :, :, :]) for n0, n in groups] + [(wp_hbm, wp), (pos_hbm, pos)]
    for i, v in enumerate((bp_hbm, g1_hbm, c1_hbm, bo_hbm, g2_hbm, c2_hbm, b2_hbm)):
        small.append((v, vecs.at[i]))
    small.append((b1_hbm, b1))
    small.append((bqkv_hbm.at[:, pl.ds(pl.multiple_of(core * 8, 8), 8), :], bqkv))
    small_copies = [pltpu.make_async_copy(s, d, in_sem.at[i]) for i, (s, d) in enumerate(small)]
    for i in (0, 2, 1) + tuple(range(3, len(small))):
        small_copies[i].start()
    wq_copies = [
        pltpu.make_async_copy(wqkv_hbm.at[pl.ds(pl.multiple_of(t * D + core * 512, 512), 512), :], wqkv.at[t], wqkv_sem.at[t])
        for t in range(3)]
    wo_copies = [
        pltpu.make_async_copy(wo_hbm.at[pl.ds(pl.multiple_of(((core + i) % 2) * 512, 512), 512), :], wo.at[i], wo_sem.at[i])
        for i in range(2)]
    w1_copies = [pltpu.make_async_copy(w1_hbm.at[:, pl.ds(i * W_FC1, W_FC1)], w1.at[i], w1_sem.at[i]) for i in range(N_FC1)]
    w2_copies = [pltpu.make_async_copy(w2_hbm.at[:, pl.ds(i * W_FC2, W_FC2)], w2.at[i], w2_sem.at[i]) for i in range(N_FC2)]

    rows128 = lax.broadcasted_iota(jnp.int32, (128, 256), 0)
    cols256 = lax.broadcasted_iota(jnp.int32, (128, 256), 1)
    diff = cols256 - rows128 % 16

    def build_sel(i, carry):
        sel[pl.ds(pl.multiple_of(i * 128, 128), 128), :] = jnp.where(diff == i * 16, 1.0, 0.0).astype(BF16)
        return carry
    lax.fori_loop(0, 16, build_sel, 0)

    keep = lax.broadcasted_iota(jnp.int32, (8, 128), 1) // 16 == lax.broadcasted_iota(jnp.int32, (8, 128), 0)

    def embed(group):
        n0, count = groups[group]
        m = count * BLOCK
        top = n0 * BLOCK * 3

        def spread(i, carry):
            for g in range(48):
                p, c = g // 3, g % 3
                t, col = g // 16, (g % 16) * 128
                for py in range(2):
                    row = img[n0 + i, c, pl.ds(py * 16 + p, 1), :]
                    halves = [jnp.where(keep, jnp.broadcast_to(row[:, j * 128:(j + 1) * 128], (8, 128)), 0.0) for j in range(2)]
                    at = pl.multiple_of(top + t * m + i * BLOCK + py * 16, 16)
                    lhs[pl.ds(at, 16), pl.ds(col, 128)] = jnp.concatenate(halves, axis=0).astype(BF16)
            return carry
        lax.fori_loop(0, count, spread, 0)
        h = 3 * m // 2
        both = [jnp.dot(lhs[top + i * h:top + (i + 1) * h, :], sel[...], preferred_element_type=F32).astype(BF16) for i in range(2)]
        rows = slice(n0 * BLOCK, n0 * BLOCK + m)
        pix[rows, 0:256] = both[0][0:m]
        pix[rows, 256:512] = jnp.concatenate([both[0][m:], both[1][0:m // 2]], axis=0)
        pix[rows, 512:768] = both[1][m // 2:]
        return rows, count

    def project(rows, count):
        for n in range(2):
            cols = slice(n * 512, (n + 1) * 512)
            emb = jnp.dot(pix[rows, :], wp[:, cols], preferred_element_type=F32) + bp_row[:, cols]
            emb = emb.reshape(count, BLOCK, 512) + pos[:, cols].astype(F32)[None]
            xs[rows, cols] = emb.reshape(count * BLOCK, 512).astype(BF16)

    slot1_first = {3: 8, 1: 10, 0: 12, 2: 13}

    def block(slot, k, other):
        first = 2 * k + other if slot == 0 else slot1_first[k] + other * (2 if k in (0, 2) else 1)
        return pl.ds(first * BLOCK, BLOCK)

    def x_block(chip_to, slot):
        image = chip_to if slot == 0 else 4 + chip_to // 2
        return pl.ds(pl.multiple_of(image * BLOCK, BLOCK), BLOCK)

    sends = []

    def start(copy):
        copy.start()
        sends.append(copy)

    def send_slot(slot, where):
        for k in where:
            to = chip_at(k)
            start(remote(xs.at[x_block(to, slot), :], xg.at[block(slot, k, 0), :], xsend.at[k - 1, slot], xrecv.at[k - 1, slot], to * 2 + core))

    def share_own(slot):
        start(remote(xs.at[x_block(chip, slot), :], xg.at[block(slot, 0, 1), :], fsend.at[0, slot], frecv.at[0, slot], mate))
        xg[block(slot, 0, 0), :] = xs[x_block(chip, slot), :]

    small_copies[0].wait()
    part = embed(0)
    for c in small_copies[2:]:
        c.wait()
    small_copies[1].wait()
    for c in wq_copies + wo_copies + w1_copies + w2_copies:
        c.start()
    bp_row = as_row(vecs[0])
    project(*part)
    pl.semaphore_wait(barrier, 7)
    send_slot(1, (2, 1))
    share_own(1)
    project(*embed(1))
    send_slot(0, (2, 1))
    send_slot(1, (3,))
    send_slot(0, (3,))
    share_own(0)

    g1_row, c1_row = as_row(vecs[1]), as_row(vecs[2])

    def norm_blocks(blocks):
        for rows in blocks:
            y1[rows, :] = norm_rows(xg[rows, :].astype(F32), g1_row, c1_row).astype(BF16)

    def arrive(slot, k):
        ref = xg.at[block(slot, k, 0), :]
        remote(ref, ref, xsend.at[k - 1, slot], xrecv.at[k - 1, slot], chip_at(k) * 2 + core).wait_recv()
        start(remote(ref, xg.at[block(slot, k, 1), :], fsend.at[k, slot], frecv.at[k, slot], mate))

    def forwarded(slot, k):
        ref = xg.at[block(slot, k, 1), :]
        remote(ref, ref, fsend.at[k, slot], frecv.at[k, slot], mate).wait_recv()

    norm_blocks([block(1, 0, 0), block(0, 0, 0)])
    for slot in (1, 0):
        forwarded(slot, 0)
    norm_blocks([block(1, 0, 1), block(0, 0, 1)])
    for c in wq_copies:
        c.wait()
    brow = [as_row(bqkv[t]) for t in range(3)]

    def heads_of(t, dst, pieces):
        rows = jnp.concatenate([y1[a:b, :] for a, b in pieces], axis=0)
        got = (lax.dot_general(rows, wqkv[t], NT, preferred_element_type=F32) + brow[t]).astype(BF16)
        at = 0
        for a, b in pieces:
            dst[a:b, :] = got[at:at + b - a]
            at += b - a

    own = ((0, 64), (384, 416), (448, 480))
    heads_of(0, qh, own)
    heads_of(1, kh, own)
    heads_of(2, vh, own)

    for slot in (1, 0):
        for k in (2, 1):
            arrive(slot, k)
        norm_blocks([block(slot, k, 0) for k in (2, 1)])
    for slot in (1, 0):
        for k in (2, 1):
            forwarded(slot, k)
    norm_blocks([block(slot, k, 1) for slot in (1, 0) for k in (2, 1)])
    near_q = ((64, 192), (416, 448), (480, 512))
    near_kv = ((64, 192), (320, 384), (416, 448), (480, 512))
    heads_of(0, qh, near_q)
    heads_of(1, kh, near_kv)
    for slot in (1, 0):
        arrive(slot, 3)
    heads_of(2, vh, near_kv)
    norm_blocks([block(slot, 3, 0) for slot in (1, 0)])
    for slot in (1, 0):
        forwarded(slot, 3)
    norm_blocks([block(slot, 3, 1) for slot in (1, 0)])
    heads_of(0, qh, ((192, 256),))
    heads_of(1, kh, ((192, 320),))
    heads_of(2, vh, ((192, 320),))

    def attend(q0, rows, k0):
        low = lax.broadcasted_iota(jnp.int32, (rows, 128), 1) < 64
        pairs = [slice(pair * 128, (pair + 1) * 128) for pair in range(4)]
        scores = []
        for cols in pairs:
            q_pair = qh[q0:q0 + rows, cols]
            for h in range(2):
                q_one = jnp.where(low == (h == 0), q_pair, jnp.zeros_like(q_pair))
                scores.append(lax.dot_general(q_one, kh[k0:k0 + 256, cols], NT, preferred_element_type=F32))
        weights = []
        for s in scores:
            e = jnp.exp2((s - jnp.max(s, axis=-1, keepdims=True)) * EXP_SCALE)
            weights.append((e * (1.0 / jnp.sum(e, axis=-1, keepdims=True))).astype(BF16))
        for i, cols in enumerate(pairs):
            heads = [jnp.dot(weights[2 * i + h], vh[k0:k0 + 256, cols], preferred_element_type=F32) for h in range(2)]
            og[q0:q0 + rows, cols] = jnp.where(low, heads[0], heads[1]).astype(BF16)

    def o_home(k, other):
        dev = chip_at(k) * 2 + (core if other == 0 else 1 - core)
        return remote(og.at[block(0, k, other), :], oh.at[other, pl.ds((k + 1) // 2 * BLOCK, BLOCK), :],
                      hsend.at[k, other], hrecv.at[k, other], dev)

    o_mates = [remote(og.at[src, :], op.at[dst, :], osend.at[i], orecv.at[i], mate)
               for i, (src, dst) in enumerate(((block(0, 2, 1), pl.ds(0, 32)), (pl.ds(448, 64), pl.ds(32, 64))))]

    attend(128, 128, 0)
    for other in range(2):
        start(o_home(3, other))
    start(o_mates[0])
    attend(384, 128, 256)
    start(o_mates[1])
    attend(0, 128, 0)
    for k, other in ((1, 0), (1, 1), (0, 1)):
        start(o_home(k, other))

    for c in wo_copies + w1_copies + w2_copies:
        c.wait()
    bo_row, g2_row, c2_row, b2_row = [as_row(vecs[i]) for i in (3, 4, 5, 6)]
    for i in range(N_FC1):
        b1row[i] = as_row(b1[i * 4:(i + 1) * 4, :])

    def finish(m, x_in, near, far, ready):
        res[0:m, :] = x_in.astype(F32) + jnp.dot(near, wo[0], preferred_element_type=F32)
        ready()
        res[0:m, :] = res[0:m, :] + jnp.dot(far[...], wo[1], preferred_element_type=F32) + bo_row
        for i in range(m // BLOCK):
            rows = slice(i * BLOCK, (i + 1) * BLOCK)
            y2[rows, :] = norm_rows(res[rows, :], g2_row, c2_row).astype(BF16)

        def activate(i):
            hid[0:m, i * W_FC1:(i + 1) * W_FC1] = jax.nn.gelu(pre[i % 2, 0:m], approximate=True).astype(BF16)

        for i in range(N_FC1):
            pre[i % 2, 0:m] = jnp.dot(y2[0:m, :], w1[i], preferred_element_type=F32) + b1row[i]
            if i:
                activate(i - 1)
        activate(N_FC1 - 1)

    def second(m, j):
        cols = slice(j * W_FC2, (j + 1) * W_FC2)
        return (jnp.dot(hid[0:m, :], w2[j], preferred_element_type=F32) + (res[0:m, cols] + b2_row[:, cols])).astype(BF16)

    def back_home(i, j, recv):
        other = chip_at(2)
        image = other if recv else chip
        if i == 1:
            image = 4 + image // 2
        return remote(back.at[i, j], out.at[image, :, pl.ds(j * W_FC2, W_FC2)], rsend.at[i, j], rrecv.at[i, j], other * 2 + core)

    def mate_ready():
        for c in o_mates:
            c.wait_recv()

    finish(96, jnp.concatenate([xg[128:160, :], xg[384:448, :]], axis=0), jnp.concatenate([og[128:160, :], og[384:448, :]], axis=0),
           op, mate_ready)
    for j in range(N_FC2):
        rows = second(96, j)
        for i in range(2):
            back[i, j] = rows[64 * i:64 * i + BLOCK]
            start(back_home(i, j, False))
        out[4 + cy, :, j * W_FC2:(j + 1) * W_FC2] = rows[BLOCK:2 * BLOCK]

    def home_ready():
        for k in (0, 1, 3):
            o_home(k, 1).wait_recv()

    for k in (1, 3):
        o_home(k, 0).wait_recv()
    finish(96, jnp.concatenate([xg[0:32, :]] + [xs[x_block(chip_at(k), 0), :] for k in (1, 3)], axis=0),
           jnp.concatenate([og[0:32, :], oh[0, 32:96, :]], axis=0), oh.at[1], home_ready)
    for j in range(N_FC2):
        rows = second(96, j)
        for i, k in enumerate((0, 1, 3)):
            out[chip_at(k), :, j * W_FC2:(j + 1) * W_FC2] = rows[i * BLOCK:(i + 1) * BLOCK]

    for j in range(N_FC2):
        for i in range(2):
            back_home(i, j, True).wait_recv()
    for c in sends:
        c.wait_send()


def solution(mesh):
    def device_step(images, w_patch, b_patch, pos_embed, ln1_gain, ln1_bias, w_qkv, b_qkv, w_out, b_out, ln2_gain, ln2_bias, w_fc1, b_fc1, w_fc2, b_fc2):
        tile = lambda v: v.reshape(-1, 128)
        args = (
            jnp.transpose(images, (0, 3, 1, 2)),
            jnp.transpose(w_patch, (0, 2, 1, 3)).reshape(768, D),
            tile(b_patch), pos_embed, tile(ln1_gain), tile(ln1_bias),
            jnp.transpose(w_qkv, (1, 2, 3, 0)).reshape(3 * D, D),
            b_qkv, w_out.reshape(D, D), tile(b_out), tile(ln2_gain), tile(ln2_bias),
            w_fc1, tile(b_fc1), w_fc2, tile(b_fc2))
        vm = pltpu.VMEM
        dma = pltpu.SemaphoreType.DMA
        return pl.pallas_call(
            layer_kernel,
            out_shape=pltpu.VMEM((IMAGES, BLOCK, D), BF16),
            in_specs=[pl.BlockSpec(memory_space=pl.ANY)] * len(args),
            out_specs=pl.BlockSpec(memory_space=pltpu.VMEM),
            scratch_shapes=[
                vm((IMAGES, 3, BLOCK, 256), F32), vm((768, D), BF16), vm((BLOCK, D), BF16), vm((7, 8, 128), F32),
                vm((32, 128), F32), vm((3, 8, 64), F32), vm((3, 512, D), BF16), vm((2, 512, D), BF16),
                vm((N_FC1, D, W_FC1), BF16), vm((N_FC2, FF, W_FC2), BF16),
                vm((3 * OWN, 2048), BF16), vm((2048, 256), BF16), vm((OWN, 768), BF16), vm((OWN, D), BF16),
                vm((2 * TOKENS, D), BF16), vm((2 * TOKENS, D), BF16),
                vm((512, 512), BF16), vm((512, 512), BF16), vm((512, 512), BF16), vm((512, 512), BF16),
                vm((HALF, 512), BF16), vm((2, HALF, 512), BF16),
                vm((HALF, D), F32), vm((HALF, D), BF16), vm((HALF, FF), BF16), vm((2, N_FC2, BLOCK, W_FC2), BF16),
                vm((N_FC1, 1, W_FC1), F32), vm((2, HALF, W_FC1), F32),
                dma((13,)), dma((3,)), dma((2,)), dma((N_FC1,)), dma((N_FC2,)),
                dma((3, 2)), dma((3, 2)), dma((4, 2)), dma((4, 2)), dma((2,)), dma((2,)), dma((4, 2)), dma((4, 2)),
                dma((2, N_FC2)), dma((2, N_FC2)),
            ],
            compiler_params=pltpu.CompilerParams(
                collective_id=0, has_side_effects=True, vmem_limit_bytes=60 * 1024 * 1024),
        )(*args)

    in_specs = (P('dp', 'sp', None, None), P(), P(), P('sp', None), P(), P(), P(), P(), P(), P(), P(), P(), P(), P(), P(), P())
    return jax.shard_map(device_step, mesh=mesh, in_specs=in_specs, out_specs=P('dp', 'sp', None), check_vma=False)
```

```python
import functools
import math
import jax
import jax.numpy as jnp
from jax import lax
from jax.experimental import pallas as pl
from jax.experimental.pallas import tpu as pltpu
from jax.sharding import PartitionSpec as P

LN_EPS = 1e-6
F32 = jnp.float32
BF16 = jnp.bfloat16
D = 1024
FF = 4096
IMAGES = 6
BLOCK = 32
TOKENS = 256
OWN = 192
HALF = 128
N_FC1, W_FC1 = 8, 512
N_FC2, W_FC2 = 2, 512
EXP_SCALE = math.log2(math.e) / 8.0
MESH = pl.DeviceIdType.MESH
NT = (((1,), (1,)), ((), ()))


def as_row(vec):
    return jnp.concatenate([vec[i:i + 1, :] for i in range(vec.shape[0])], axis=1)


def norm_rows(x_in, gain, bias):
    centered = x_in - jnp.mean(x_in, axis=-1, keepdims=True)
    variance = jnp.mean(centered * centered, axis=-1, keepdims=True)
    return centered * lax.rsqrt(variance + LN_EPS) * gain + bias


def layer_kernel(
        img_hbm, wp_hbm, bp_hbm, pos_hbm, g1_hbm, c1_hbm, wqkv_hbm, bqkv_hbm, wo_hbm, bo_hbm, g2_hbm, c2_hbm,
        w1_hbm, b1_hbm, w2_hbm, b2_hbm,
        out,
        img, wp, pos, vecs, b1, bqkv, wqkv, wo, w1, w2,
        lhs, sel, pix, xs, xg, y1, qh, kh, vh, og, op, oh, res, y2, hid, back, b1row, pre,
        in_sem, wqkv_sem, wo_sem, w1_sem, w2_sem,
        xsend, xrecv, fsend, frecv, osend, orecv, hsend, hrecv, rsend, rrecv):
    dp = lax.axis_index("dp")
    me = lax.axis_index("sp")
    chip = me // 2
    core = me % 2
    mate = chip * 2 + (1 - core)
    cx = chip % 2
    cy = chip // 2

    def remote(src, dst, ssem, rsem, dev):
        return pltpu.make_async_remote_copy(
            src_ref=src, dst_ref=dst, send_sem=ssem, recv_sem=rsem, device_id=(dp, dev), device_id_type=MESH)

    def chip_at(k):
        return ((cy + k // 2) % 2) * 2 + (cx + k % 2) % 2

    barrier = pltpu.get_barrier_semaphore()
    for k in range(1, 8):
        pl.semaphore_signal(barrier, inc=1, device_id=(dp, (me + k) % 8), device_id_type=MESH)

    groups = ((4, 2), (0, 4))
    small = [(img_hbm.at[pl.ds(n0, n), :, :, :], img.at[pl.ds(n0, n), :, :, :]) for n0, n in groups] + [(wp_hbm, wp), (pos_hbm, pos)]
    for i, v in enumerate((bp_hbm, g1_hbm, c1_hbm, bo_hbm, g2_hbm, c2_hbm, b2_hbm)):
        small.append((v, vecs.at[i]))
    small.append((b1_hbm, b1))
    small.append((bqkv_hbm.at[:, pl.ds(pl.multiple_of(core * 8, 8), 8), :], bqkv))
    small_copies = [pltpu.make_async_copy(s, d, in_sem.at[i]) for i, (s, d) in enumerate(small)]
    for i in (0, 2, 1) + tuple(range(3, len(small))):
        small_copies[i].start()
    wq_copies = [
        pltpu.make_async_copy(wqkv_hbm.at[pl.ds(pl.multiple_of(t * D + core * 512, 512), 512), :], wqkv.at[t], wqkv_sem.at[t])
        for t in range(3)]
    wo_copies = [
        pltpu.make_async_copy(wo_hbm.at[pl.ds(pl.multiple_of(((core + i) % 2) * 512, 512), 512), :], wo.at[i], wo_sem.at[i])
        for i in range(2)]
    w1_copies = [pltpu.make_async_copy(w1_hbm.at[:, pl.ds(i * W_FC1, W_FC1)], w1.at[i], w1_sem.at[i]) for i in range(N_FC1)]
    w2_copies = [pltpu.make_async_copy(w2_hbm.at[:, pl.ds(i * W_FC2, W_FC2)], w2.at[i], w2_sem.at[i]) for i in range(N_FC2)]

    rows128 = lax.broadcasted_iota(jnp.int32, (128, 256), 0)
    cols256 = lax.broadcasted_iota(jnp.int32, (128, 256), 1)
    diff = cols256 - rows128 % 16

    def build_sel(i, carry):
        sel[pl.ds(pl.multiple_of(i * 128, 128), 128), :] = jnp.where(diff == i * 16, 1.0, 0.0).astype(BF16)
        return carry
    lax.fori_loop(0, 16, build_sel, 0)

    keep = lax.broadcasted_iota(jnp.int32, (8, 128), 1) // 16 == lax.broadcasted_iota(jnp.int32, (8, 128), 0)

    def embed(group):
        n0, count = groups[group]
        m = count * BLOCK
        top = n0 * BLOCK * 3

        def spread(i, carry):
            for g in range(48):
                p, c = g // 3, g % 3
                t, col = g // 16, (g % 16) * 128
                for py in range(2):
                    row = img[n0 + i, c, pl.ds(py * 16 + p, 1), :]
                    halves = [jnp.where(keep, jnp.broadcast_to(row[:, j * 128:(j + 1) * 128], (8, 128)), 0.0) for j in range(2)]
                    at = pl.multiple_of(top + t * m + i * BLOCK + py * 16, 16)
                    lhs[pl.ds(at, 16), pl.ds(col, 128)] = jnp.concatenate(halves, axis=0).astype(BF16)
            return carry
        lax.fori_loop(0, count, spread, 0)
        h = 3 * m // 2
        both = [jnp.dot(lhs[top + i * h:top + (i + 1) * h, :], sel[...], preferred_element_type=F32).astype(BF16) for i in range(2)]
        rows = slice(n0 * BLOCK, n0 * BLOCK + m)
        pix[rows, 0:256] = both[0][0:m]
        pix[rows, 256:512] = jnp.concatenate([both[0][m:], both[1][0:m // 2]], axis=0)
        pix[rows, 512:768] = both[1][m // 2:]
        return rows, count

    def project(rows, count):
        for n in range(2):
            cols = slice(n * 512, (n + 1) * 512)
            emb = jnp.dot(pix[rows, :], wp[:, cols], preferred_element_type=F32) + bp_row[:, cols]
            emb = emb.reshape(count, BLOCK, 512) + pos[:, cols].astype(F32)[None]
            xs[rows, cols] = emb.reshape(count * BLOCK, 512).astype(BF16)

    slot1_first = {3: 8, 1: 10, 0: 12, 2: 13}

    def block(slot, k, other):
        first = 2 * k + other if slot == 0 else slot1_first[k] + other * (2 if k in (0, 2) else 1)
        return pl.ds(first * BLOCK, BLOCK)

    def x_block(chip_to, slot):
        image = chip_to if slot == 0 else 4 + chip_to // 2
        return pl.ds(pl.multiple_of(image * BLOCK, BLOCK), BLOCK)

    sends = []

    def start(copy):
        copy.start()
        sends.append(copy)

    def send_slot(slot, where):
        for k in where:
            to = chip_at(k)
            start(remote(xs.at[x_block(to, slot), :], xg.at[block(slot, k, 0), :], xsend.at[k - 1, slot], xrecv.at[k - 1, slot], to * 2 + core))

    def share_own(slot):
        start(remote(xs.at[x_block(chip, slot), :], xg.at[block(slot, 0, 1), :], fsend.at[0, slot], frecv.at[0, slot], mate))
        xg[block(slot, 0, 0), :] = xs[x_block(chip, slot), :]

    small_copies[0].wait()
    part = embed(0)
    for c in small_copies[2:]:
        c.wait()
    small_copies[1].wait()
    for c in wq_copies + wo_copies + w1_copies + w2_copies:
        c.start()
    bp_row = as_row(vecs[0])
    project(*part)
    pl.semaphore_wait(barrier, 7)
    send_slot(1, (2, 1))
    share_own(1)
    project(*embed(1))
    send_slot(0, (2, 1))
    send_slot(1, (3,))
    send_slot(0, (3,))
    share_own(0)

    g1_row, c1_row = as_row(vecs[1]), as_row(vecs[2])

    def norm_blocks(blocks):
        for rows in blocks:
            y1[rows, :] = norm_rows(xg[rows, :].astype(F32), g1_row, c1_row).astype(BF16)

    def arrive(slot, k):
        ref = xg.at[block(slot, k, 0), :]
        remote(ref, ref, xsend.at[k - 1, slot], xrecv.at[k - 1, slot], chip_at(k) * 2 + core).wait_recv()
        start(remote(ref, xg.at[block(slot, k, 1), :], fsend.at[k, slot], frecv.at[k, slot], mate))

    def forwarded(slot, k):
        ref = xg.at[block(slot, k, 1), :]
        remote(ref, ref, fsend.at[k, slot], frecv.at[k, slot], mate).wait_recv()

    norm_blocks([block(1, 0, 0), block(0, 0, 0)])
    for slot in (1, 0):
        forwarded(slot, 0)
    norm_blocks([block(1, 0, 1), block(0, 0, 1)])
    for c in wq_copies:
        c.wait()
    brow = [as_row(bqkv[t]) for t in range(3)]

    def heads_of(t, dst, pieces):
        rows = jnp.concatenate([y1[a:b, :] for a, b in pieces], axis=0)
        got = (lax.dot_general(rows, wqkv[t], NT, preferred_element_type=F32) + brow[t]).astype(BF16)
        at = 0
        for a, b in pieces:
            dst[a:b, :] = got[at:at + b - a]
            at += b - a

    own = ((0, 64), (384, 416), (448, 480))
    heads_of(0, qh, own)
    heads_of(1, kh, own)
    heads_of(2, vh, own)

    for slot in (1, 0):
        for k in (2, 1):
            arrive(slot, k)
        norm_blocks([block(slot, k, 0) for k in (2, 1)])
    for slot in (1, 0):
        for k in (2, 1):
            forwarded(slot, k)
    norm_blocks([block(slot, k, 1) for slot in (1, 0) for k in (2, 1)])
    near_q = ((64, 192), (416, 448), (480, 512))
    near_kv = ((64, 192), (320, 384), (416, 448), (480, 512))
    heads_of(0, qh, near_q)
    heads_of(1, kh, near_kv)
    for slot in (1, 0):
        arrive(slot, 3)
    heads_of(2, vh, near_kv)
    norm_blocks([block(slot, 3, 0) for slot in (1, 0)])
    for slot in (1, 0):
        forwarded(slot, 3)
    norm_blocks([block(slot, 3, 1) for slot in (1, 0)])
    heads_of(0, qh, ((192, 256),))
    heads_of(1, kh, ((192, 320),))
    heads_of(2, vh, ((192, 320),))

    pairs = [slice(pair * 128, (pair + 1) * 128) for pair in range(4)]
    low = lax.broadcasted_iota(jnp.int32, (128, 128), 1) < 64

    def score(q0, k0):
        scores = []
        for cols in pairs:
            q_pair = qh[q0:q0 + 128, cols]
            for h in range(2):
                q_one = jnp.where(low == (h == 0), q_pair, jnp.zeros_like(q_pair))
                scores.append(lax.dot_general(q_one, kh[k0:k0 + 256, cols], NT, preferred_element_type=F32))
        return scores

    def soften(scores):
        weights = []
        for s in scores:
            e = jnp.exp2((s - jnp.max(s, axis=-1, keepdims=True)) * EXP_SCALE)
            weights.append((e * (1.0 / jnp.sum(e, axis=-1, keepdims=True))).astype(BF16))
        return weights

    def combine(weights, q0, k0):
        for i, cols in enumerate(pairs):
            heads = [jnp.dot(weights[2 * i + h], vh[k0:k0 + 256, cols], preferred_element_type=F32) for h in range(2)]
            og[q0:q0 + 128, cols] = jnp.where(low, heads[0], heads[1]).astype(BF16)

    def o_home(k, other):
        dev = chip_at(k) * 2 + (core if other == 0 else 1 - core)
        return remote(og.at[block(0, k, other), :], oh.at[other, pl.ds(k * BLOCK, BLOCK), :],
                      hsend.at[k, other], hrecv.at[k, other], dev)

    o_mate = remote(og.at[pl.ds(448, 64), :], op, osend, orecv, mate)

    combine(soften(score(128, 0)), 128, 0)
    for k in (3, 2):
        for other in range(2):
            start(o_home(k, other))
    shared = soften(score(384, 256))
    scores = score(0, 0)
    combine(shared, 384, 256)
    start(o_mate)
    combine(soften(scores), 0, 0)
    for k, other in ((1, 0), (1, 1), (0, 1)):
        start(o_home(k, other))

    for c in wo_copies + w1_copies + w2_copies:
        c.wait()
    bo_row, g2_row, c2_row, b2_row = [as_row(vecs[i]) for i in (3, 4, 5, 6)]
    for i in range(N_FC1):
        b1row[i] = as_row(b1[i * 4:(i + 1) * 4, :])

    def finish(m, x_in, near, far, ready):
        res[0:m, :] = x_in.astype(F32) + jnp.dot(near, wo[0], preferred_element_type=F32)
        ready()
        res[0:m, :] = res[0:m, :] + jnp.dot(far[...], wo[1], preferred_element_type=F32) + bo_row
        for i in range(m // BLOCK):
            rows = slice(i * BLOCK, (i + 1) * BLOCK)
            y2[rows, :] = norm_rows(res[rows, :], g2_row, c2_row).astype(BF16)

        def activate(i):
            hid[0:m, i * W_FC1:(i + 1) * W_FC1] = jax.nn.gelu(pre[i % 2, 0:m], approximate=True).astype(BF16)

        for i in range(N_FC1):
            pre[i % 2, 0:m] = jnp.dot(y2[0:m, :], w1[i], preferred_element_type=F32) + b1row[i]
            if i:
                activate(i - 1)
        activate(N_FC1 - 1)

    def second(m, j):
        cols = slice(j * W_FC2, (j + 1) * W_FC2)
        return (jnp.dot(hid[0:m, :], w2[j], preferred_element_type=F32) + (res[0:m, cols] + b2_row[:, cols])).astype(BF16)

    def shared_home(j, recv):
        other = chip_at(2)
        image = 4 + (other if recv else chip) // 2
        return remote(back.at[j], out.at[image, :, pl.ds(j * W_FC2, W_FC2)], rsend.at[j], rrecv.at[j], other * 2 + core)

    finish(64, xg[384:448, :], og[384:448, :], op, o_mate.wait_recv)
    for j in range(N_FC2):
        rows = second(64, j)
        back[j] = rows[BLOCK:]
        start(shared_home(j, False))
        out[4 + cy, :, j * W_FC2:(j + 1) * W_FC2] = rows[0:BLOCK]

    def home_ready():
        for k in range(4):
            o_home(k, 1).wait_recv()

    for k in (1, 2, 3):
        o_home(k, 0).wait_recv()
    finish(128, jnp.concatenate([xg[0:32, :]] + [xs[x_block(chip_at(k), 0), :] for k in (1, 2, 3)], axis=0),
           jnp.concatenate([og[0:32, :], oh[0, 32:128, :]], axis=0), oh.at[1], home_ready)
    for j in range(N_FC2):
        rows = second(128, j)
        for k in range(4):
            out[chip_at(k), :, j * W_FC2:(j + 1) * W_FC2] = rows[k * BLOCK:(k + 1) * BLOCK]

    for j in range(N_FC2):
        shared_home(j, True).wait_recv()
    for c in sends:
        c.wait_send()


def solution(mesh):
    def device_step(images, w_patch, b_patch, pos_embed, ln1_gain, ln1_bias, w_qkv, b_qkv, w_out, b_out, ln2_gain, ln2_bias, w_fc1, b_fc1, w_fc2, b_fc2):
        tile = lambda v: v.reshape(-1, 128)
        args = (
            jnp.transpose(images, (0, 3, 1, 2)),
            jnp.transpose(w_patch, (0, 2, 1, 3)).reshape(768, D),
            tile(b_patch), pos_embed, tile(ln1_gain), tile(ln1_bias),
            jnp.transpose(w_qkv, (1, 2, 3, 0)).reshape(3 * D, D),
            b_qkv, w_out.reshape(D, D), tile(b_out), tile(ln2_gain), tile(ln2_bias),
            w_fc1, tile(b_fc1), w_fc2, tile(b_fc2))
        vm = pltpu.VMEM
        dma = pltpu.SemaphoreType.DMA
        return pl.pallas_call(
            layer_kernel,
            out_shape=pltpu.VMEM((IMAGES, BLOCK, D), BF16),
            in_specs=[pl.BlockSpec(memory_space=pl.ANY)] * len(args),
            out_specs=pl.BlockSpec(memory_space=pltpu.VMEM),
            scratch_shapes=[
                vm((IMAGES, 3, BLOCK, 256), F32), vm((768, D), BF16), vm((BLOCK, D), BF16), vm((7, 8, 128), F32),
                vm((32, 128), F32), vm((3, 8, 64), F32), vm((3, 512, D), BF16), vm((2, 512, D), BF16),
                vm((N_FC1, D, W_FC1), BF16), vm((N_FC2, FF, W_FC2), BF16),
                vm((3 * OWN, 2048), BF16), vm((2048, 256), BF16), vm((OWN, 768), BF16), vm((OWN, D), BF16),
                vm((2 * TOKENS, D), BF16), vm((2 * TOKENS, D), BF16),
                vm((512, 512), BF16), vm((512, 512), BF16), vm((512, 512), BF16), vm((512, 512), BF16),
                vm((64, 512), BF16), vm((2, HALF, 512), BF16),
                vm((HALF, D), F32), vm((HALF, D), BF16), vm((HALF, FF), BF16), vm((N_FC2, BLOCK, W_FC2), BF16),
                vm((N_FC1, 1, W_FC1), F32), vm((2, HALF, W_FC1), F32),
                dma((13,)), dma((3,)), dma((2,)), dma((N_FC1,)), dma((N_FC2,)),
                dma((3, 2)), dma((3, 2)), dma((4, 2)), dma((4, 2)), dma, dma, dma((4, 2)), dma((4, 2)),
                dma((N_FC2,)), dma((N_FC2,)),
            ],
            compiler_params=pltpu.CompilerParams(
                collective_id=0, has_side_effects=True, vmem_limit_bytes=60 * 1024 * 1024),
        )(*args)

    in_specs = (P('dp', 'sp', None, None), P(), P(), P('sp', None), P(), P(), P(), P(), P(), P(), P(), P(), P(), P(), P(), P())
    return jax.shard_map(device_step, mesh=mesh, in_specs=in_specs, out_specs=P('dp', 'sp', None), check_vma=False)
```

```python
import functools
import math
import jax
import jax.numpy as jnp
from jax import lax
from jax.experimental import pallas as pl
from jax.experimental.pallas import tpu as pltpu
from jax.sharding import PartitionSpec as P

LN_EPS = 1e-6
F32 = jnp.float32
BF16 = jnp.bfloat16
D = 1024
FF = 4096
IMAGES = 6
BLOCK = 32
TOKENS = 256
OWN = 192
HALF = 128
N_FC1, W_FC1 = 8, 512
N_FC2, W_FC2 = 2, 512
EXP_SCALE = math.log2(math.e) / 8.0
MESH = pl.DeviceIdType.MESH
NT = (((1,), (1,)), ((), ()))


def as_row(vec):
    return jnp.concatenate([vec[i:i + 1, :] for i in range(vec.shape[0])], axis=1)


def norm_rows(x_in, gain, bias):
    centered = x_in - jnp.mean(x_in, axis=-1, keepdims=True)
    variance = jnp.mean(centered * centered, axis=-1, keepdims=True)
    return centered * lax.rsqrt(variance + LN_EPS) * gain + bias


def layer_kernel(
        img_hbm, wp_hbm, bp_hbm, pos_hbm, g1_hbm, c1_hbm, wqkv_hbm, bqkv_hbm, wo_hbm, bo_hbm, g2_hbm, c2_hbm,
        w1_hbm, b1_hbm, w2_hbm, b2_hbm,
        out,
        img, wp, pos, vecs, b1, bqkv, wqkv, wo, w1, w2,
        lhs, sel, pix, xs, xg, y1, qh, kh, vh, og, op, oh, res, y2, hid, back, b1row, pre,
        in_sem, wqkv_sem, wo_sem, w1_sem, w2_sem,
        xsend, xrecv, fsend, frecv, osend, orecv, hsend, hrecv, rsend, rrecv):
    dp = lax.axis_index("dp")
    me = lax.axis_index("sp")
    chip = me // 2
    core = me % 2
    mate = chip * 2 + (1 - core)
    cx = chip % 2
    cy = chip // 2

    def remote(src, dst, ssem, rsem, dev):
        return pltpu.make_async_remote_copy(
            src_ref=src, dst_ref=dst, send_sem=ssem, recv_sem=rsem, device_id=(dp, dev), device_id_type=MESH)

    def chip_at(k):
        return ((cy + k // 2) % 2) * 2 + (cx + k % 2) % 2

    barrier = pltpu.get_barrier_semaphore()
    for k in range(1, 8):
        pl.semaphore_signal(barrier, inc=1, device_id=(dp, (me + k) % 8), device_id_type=MESH)

    groups = ((4, 2), (0, 4))
    small = [(img_hbm.at[pl.ds(n0, n), :, :, :], img.at[pl.ds(n0, n), :, :, :]) for n0, n in groups] + [(wp_hbm, wp), (pos_hbm, pos)]
    for i, v in enumerate((bp_hbm, g1_hbm, c1_hbm, bo_hbm, g2_hbm, c2_hbm, b2_hbm)):
        small.append((v, vecs.at[i]))
    small.append((b1_hbm, b1))
    small.append((bqkv_hbm.at[:, pl.ds(pl.multiple_of(core * 8, 8), 8), :], bqkv))
    small_copies = [pltpu.make_async_copy(s, d, in_sem.at[i]) for i, (s, d) in enumerate(small)]
    for i in (0, 2, 1) + tuple(range(3, len(small))):
        small_copies[i].start()
    wq_copies = [
        pltpu.make_async_copy(wqkv_hbm.at[pl.ds(pl.multiple_of(t * D + core * 512, 512), 512), :], wqkv.at[t], wqkv_sem.at[t])
        for t in range(3)]
    wo_copies = [
        pltpu.make_async_copy(wo_hbm.at[pl.ds(pl.multiple_of(((core + i) % 2) * 512, 512), 512), :], wo.at[i], wo_sem.at[i])
        for i in range(2)]
    w1_copies = [pltpu.make_async_copy(w1_hbm.at[:, pl.ds(i * W_FC1, W_FC1)], w1.at[i], w1_sem.at[i]) for i in range(N_FC1)]
    w2_copies = [pltpu.make_async_copy(w2_hbm.at[:, pl.ds(i * W_FC2, W_FC2)], w2.at[i], w2_sem.at[i]) for i in range(N_FC2)]

    rows128 = lax.broadcasted_iota(jnp.int32, (128, 256), 0)
    cols256 = lax.broadcasted_iota(jnp.int32, (128, 256), 1)
    diff = cols256 - rows128 % 16

    def build_sel(i, carry):
        sel[pl.ds(pl.multiple_of(i * 128, 128), 128), :] = jnp.where(diff == i * 16, 1.0, 0.0).astype(BF16)
        return carry
    lax.fori_loop(0, 16, build_sel, 0)

    keep = lax.broadcasted_iota(jnp.int32, (8, 128), 1) // 16 == lax.broadcasted_iota(jnp.int32, (8, 128), 0)

    def embed(group):
        n0, count = groups[group]
        m = count * BLOCK
        top = n0 * BLOCK * 3

        def spread(i, carry):
            for g in range(48):
                p, c = g // 3, g % 3
                t, col = g // 16, (g % 16) * 128
                for py in range(2):
                    row = img[n0 + i, c, pl.ds(py * 16 + p, 1), :]
                    halves = [jnp.where(keep, jnp.broadcast_to(row[:, j * 128:(j + 1) * 128], (8, 128)), 0.0) for j in range(2)]
                    at = pl.multiple_of(top + t * m + i * BLOCK + py * 16, 16)
                    lhs[pl.ds(at, 16), pl.ds(col, 128)] = jnp.concatenate(halves, axis=0).astype(BF16)
            return carry
        lax.fori_loop(0, count, spread, 0)
        h = 3 * m // 2
        both = [jnp.dot(lhs[top + i * h:top + (i + 1) * h, :], sel[...], preferred_element_type=F32).astype(BF16) for i in range(2)]
        rows = slice(n0 * BLOCK, n0 * BLOCK + m)
        pix[rows, 0:256] = both[0][0:m]
        pix[rows, 256:512] = jnp.concatenate([both[0][m:], both[1][0:m // 2]], axis=0)
        pix[rows, 512:768] = both[1][m // 2:]
        return rows, count

    def project(rows, count):
        for n in range(2):
            cols = slice(n * 512, (n + 1) * 512)
            emb = jnp.dot(pix[rows, :], wp[:, cols], preferred_element_type=F32) + bp_row[:, cols]
            emb = emb.reshape(count, BLOCK, 512) + pos[:, cols].astype(F32)[None]
            xs[rows, cols] = emb.reshape(count * BLOCK, 512).astype(BF16)

    slot1_first = {3: 8, 1: 10, 0: 12, 2: 13}

    def block(slot, k, other):
        first = 2 * k + other if slot == 0 else slot1_first[k] + other * (2 if k in (0, 2) else 1)
        return pl.ds(first * BLOCK, BLOCK)

    def x_block(chip_to, slot):
        image = chip_to if slot == 0 else 4 + chip_to // 2
        return pl.ds(pl.multiple_of(image * BLOCK, BLOCK), BLOCK)

    sends = []

    def start(copy):
        copy.start()
        sends.append(copy)

    def send_slot(slot, where):
        for k in where:
            to = chip_at(k)
            start(remote(xs.at[x_block(to, slot), :], xg.at[block(slot, k, 0), :], xsend.at[k - 1, slot], xrecv.at[k - 1, slot], to * 2 + core))

    def share_own(slot):
        start(remote(xs.at[x_block(chip, slot), :], xg.at[block(slot, 0, 1), :], fsend.at[0, slot], frecv.at[0, slot], mate))
        xg[block(slot, 0, 0), :] = xs[x_block(chip, slot), :]

    small_copies[0].wait()
    part = embed(0)
    for c in small_copies[2:]:
        c.wait()
    small_copies[1].wait()
    for c in wq_copies + wo_copies + w1_copies + w2_copies:
        c.start()
    bp_row = as_row(vecs[0])
    project(*part)
    pl.semaphore_wait(barrier, 7)
    send_slot(1, (2, 1))
    share_own(1)
    project(*embed(1))
    send_slot(0, (2, 1))
    send_slot(0, (3,))
    send_slot(1, (3,))
    share_own(0)

    g1_row, c1_row = as_row(vecs[1]), as_row(vecs[2])

    def norm_blocks(blocks):
        for rows in blocks:
            y1[rows, :] = norm_rows(xg[rows, :].astype(F32), g1_row, c1_row).astype(BF16)

    def arrive(slot, k):
        ref = xg.at[block(slot, k, 0), :]
        remote(ref, ref, xsend.at[k - 1, slot], xrecv.at[k - 1, slot], chip_at(k) * 2 + core).wait_recv()
        start(remote(ref, xg.at[block(slot, k, 1), :], fsend.at[k, slot], frecv.at[k, slot], mate))

    def forwarded(slot, k):
        ref = xg.at[block(slot, k, 1), :]
        remote(ref, ref, fsend.at[k, slot], frecv.at[k, slot], mate).wait_recv()

    norm_blocks([block(1, 0, 0), block(0, 0, 0)])
    for slot in (1, 0):
        forwarded(slot, 0)
    norm_blocks([block(1, 0, 1), block(0, 0, 1)])
    for c in wq_copies:
        c.wait()
    brow = [as_row(bqkv[t]) for t in range(3)]

    def heads_of(t, dst, pieces):
        rows = jnp.concatenate([y1[a:b, :] for a, b in pieces], axis=0)
        got = (lax.dot_general(rows, wqkv[t], NT, preferred_element_type=F32) + brow[t]).astype(BF16)
        at = 0
        for a, b in pieces:
            dst[a:b, :] = got[at:at + b - a]
            at += b - a

    own = ((0, 64), (384, 416), (448, 480))
    heads_of(0, qh, own)
    heads_of(1, kh, own)
    heads_of(2, vh, own)

    for slot in (1, 0):
        for k in (2, 1):
            arrive(slot, k)
        norm_blocks([block(slot, k, 0) for k in (2, 1)])
    for slot in (1, 0):
        for k in (2, 1):
            forwarded(slot, k)
    norm_blocks([block(slot, k, 1) for slot in (1, 0) for k in (2, 1)])
    near_q = ((64, 192), (416, 448), (480, 512))
    near_kv = ((64, 192), (320, 384), (416, 448), (480, 512))
    heads_of(0, qh, near_q)
    heads_of(1, kh, near_kv)
    arrive(0, 3)
    heads_of(2, vh, near_kv)
    norm_blocks([block(0, 3, 0)])
    forwarded(0, 3)
    norm_blocks([block(0, 3, 1)])
    for t, dst in ((0, qh), (1, kh), (2, vh)):
        heads_of(t, dst, ((192, 256),))
    arrive(1, 3)

    pairs = [slice(pair * 128, (pair + 1) * 128) for pair in range(4)]
    low = lax.broadcasted_iota(jnp.int32, (128, 128), 1) < 64

    def score(q0, k0):
        scores = []
        for cols in pairs:
            q_pair = qh[q0:q0 + 128, cols]
            for h in range(2):
                q_one = jnp.where(low == (h == 0), q_pair, jnp.zeros_like(q_pair))
                scores.append(lax.dot_general(q_one, kh[k0:k0 + 256, cols], NT, preferred_element_type=F32))
        return scores

    def soften(scores):
        weights = []
        for s in scores:
            e = jnp.exp2((s - jnp.max(s, axis=-1, keepdims=True)) * EXP_SCALE)
            weights.append((e * (1.0 / jnp.sum(e, axis=-1, keepdims=True))).astype(BF16))
        return weights

    def combine(weights, q0, k0):
        for i, cols in enumerate(pairs):
            heads = [jnp.dot(weights[2 * i + h], vh[k0:k0 + 256, cols], preferred_element_type=F32) for h in range(2)]
            og[q0:q0 + 128, cols] = jnp.where(low, heads[0], heads[1]).astype(BF16)

    def o_home(k, other):
        dev = chip_at(k) * 2 + (core if other == 0 else 1 - core)
        return remote(og.at[block(0, k, other), :], oh.at[other, pl.ds(k * BLOCK, BLOCK), :],
                      hsend.at[k, other], hrecv.at[k, other], dev)

    o_mate = remote(og.at[pl.ds(448, 64), :], op, osend, orecv, mate)

    combine(soften(score(128, 0)), 128, 0)
    for k in (3, 2):
        for other in range(2):
            start(o_home(k, other))
    norm_blocks([block(1, 3, 0)])
    forwarded(1, 3)
    norm_blocks([block(1, 3, 1)])
    heads_of(1, kh, ((256, 320),))
    heads_of(2, vh, ((256, 320),))
    shared = soften(score(384, 256))
    scores = score(0, 0)
    combine(shared, 384, 256)
    start(o_mate)
    combine(soften(scores), 0, 0)
    for k, other in ((1, 0), (1, 1), (0, 1)):
        start(o_home(k, other))

    for c in wo_copies + w1_copies + w2_copies:
        c.wait()
    bo_row, g2_row, c2_row, b2_row = [as_row(vecs[i]) for i in (3, 4, 5, 6)]
    for i in range(N_FC1):
        b1row[i] = as_row(b1[i * 4:(i + 1) * 4, :])

    def finish(m, x_in, near, far, ready):
        res[0:m, :] = x_in.astype(F32) + jnp.dot(near, wo[0], preferred_element_type=F32)
        ready()
        res[0:m, :] = res[0:m, :] + jnp.dot(far[...], wo[1], preferred_element_type=F32) + bo_row
        for i in range(m // BLOCK):
            rows = slice(i * BLOCK, (i + 1) * BLOCK)
            y2[rows, :] = norm_rows(res[rows, :], g2_row, c2_row).astype(BF16)

        def activate(i):
            hid[0:m, i * W_FC1:(i + 1) * W_FC1] = jax.nn.gelu(pre[i % 2, 0:m], approximate=True).astype(BF16)

        for i in range(N_FC1):
            pre[i % 2, 0:m] = jnp.dot(y2[0:m, :], w1[i], preferred_element_type=F32) + b1row[i]
            if i:
                activate(i - 1)
        activate(N_FC1 - 1)

    def second(m, j):
        cols = slice(j * W_FC2, (j + 1) * W_FC2)
        return (jnp.dot(hid[0:m, :], w2[j], preferred_element_type=F32) + (res[0:m, cols] + b2_row[:, cols])).astype(BF16)

    def shared_home(j, recv):
        other = chip_at(2)
        image = 4 + (other if recv else chip) // 2
        return remote(back.at[j], out.at[image, :, pl.ds(j * W_FC2, W_FC2)], rsend.at[j], rrecv.at[j], other * 2 + core)

    finish(64, xg[384:448, :], og[384:448, :], op, o_mate.wait_recv)
    for j in range(N_FC2):
        rows = second(64, j)
        back[j] = rows[BLOCK:]
        start(shared_home(j, False))
        out[4 + cy, :, j * W_FC2:(j + 1) * W_FC2] = rows[0:BLOCK]

    def home_ready():
        for k in range(4):
            o_home(k, 1).wait_recv()

    for k in (1, 2, 3):
        o_home(k, 0).wait_recv()
    finish(128, jnp.concatenate([xg[0:32, :]] + [xs[x_block(chip_at(k), 0), :] for k in (1, 2, 3)], axis=0),
           jnp.concatenate([og[0:32, :], oh[0, 32:128, :]], axis=0), oh.at[1], home_ready)
    for j in range(N_FC2):
        rows = second(128, j)
        for k in range(4):
            out[chip_at(k), :, j * W_FC2:(j + 1) * W_FC2] = rows[k * BLOCK:(k + 1) * BLOCK]

    for j in range(N_FC2):
        shared_home(j, True).wait_recv()
    for c in sends:
        c.wait_send()


def solution(mesh):
    def device_step(images, w_patch, b_patch, pos_embed, ln1_gain, ln1_bias, w_qkv, b_qkv, w_out, b_out, ln2_gain, ln2_bias, w_fc1, b_fc1, w_fc2, b_fc2):
        tile = lambda v: v.reshape(-1, 128)
        args = (
            jnp.transpose(images, (0, 3, 1, 2)),
            jnp.transpose(w_patch, (0, 2, 1, 3)).reshape(768, D),
            tile(b_patch), pos_embed, tile(ln1_gain), tile(ln1_bias),
            jnp.transpose(w_qkv, (1, 2, 3, 0)).reshape(3 * D, D),
            b_qkv, w_out.reshape(D, D), tile(b_out), tile(ln2_gain), tile(ln2_bias),
            w_fc1, tile(b_fc1), w_fc2, tile(b_fc2))
        vm = pltpu.VMEM
        dma = pltpu.SemaphoreType.DMA
        return pl.pallas_call(
            layer_kernel,
            out_shape=pltpu.VMEM((IMAGES, BLOCK, D), BF16),
            in_specs=[pl.BlockSpec(memory_space=pl.ANY)] * len(args),
            out_specs=pl.BlockSpec(memory_space=pltpu.VMEM),
            scratch_shapes=[
                vm((IMAGES, 3, BLOCK, 256), F32), vm((768, D), BF16), vm((BLOCK, D), BF16), vm((7, 8, 128), F32),
                vm((32, 128), F32), vm((3, 8, 64), F32), vm((3, 512, D), BF16), vm((2, 512, D), BF16),
                vm((N_FC1, D, W_FC1), BF16), vm((N_FC2, FF, W_FC2), BF16),
                vm((3 * OWN, 2048), BF16), vm((2048, 256), BF16), vm((OWN, 768), BF16), vm((OWN, D), BF16),
                vm((2 * TOKENS, D), BF16), vm((2 * TOKENS, D), BF16),
                vm((512, 512), BF16), vm((512, 512), BF16), vm((512, 512), BF16), vm((512, 512), BF16),
                vm((64, 512), BF16), vm((2, HALF, 512), BF16),
                vm((HALF, D), F32), vm((HALF, D), BF16), vm((HALF, FF), BF16), vm((N_FC2, BLOCK, W_FC2), BF16),
                vm((N_FC1, 1, W_FC1), F32), vm((2, HALF, W_FC1), F32),
                dma((13,)), dma((3,)), dma((2,)), dma((N_FC1,)), dma((N_FC2,)),
                dma((3, 2)), dma((3, 2)), dma((4, 2)), dma((4, 2)), dma, dma, dma((4, 2)), dma((4, 2)),
                dma((N_FC2,)), dma((N_FC2,)),
            ],
            compiler_params=pltpu.CompilerParams(
                collective_id=0, has_side_effects=True, vmem_limit_bytes=60 * 1024 * 1024),
        )(*args)

    in_specs = (P('dp', 'sp', None, None), P(), P(), P('sp', None), P(), P(), P(), P(), P(), P(), P(), P(), P(), P(), P(), P())
    return jax.shard_map(device_step, mesh=mesh, in_specs=in_specs, out_specs=P('dp', 'sp', None), check_vma=False)
```
